32 devices in a mesh: dp: 16 (over z, y, x), tensor: 2 (over core).
Axes of the slice: x: 2, y: 2, z: 4, core: 2. Of those that a mesh axis runs over, the one named last changes fastest.
Arguments:
- inputs: bfloat16 [4, 8192, 768], P(None, ('dp', 'tensor')), may hold values from -6 to 6
- lengths: int32 [4, 16], P(None, 'dp'), may hold values from 128 to 512, as said below
- bounds: int32 [4, 16], P(None, 'dp'), may hold values from 32 to 384, as said below
- query_matrix: bfloat16 [768, 768], P('dp', 'tensor'), may hold values from -0.21875 to 0.21875
- key_matrix: bfloat16 [768, 768], P('dp', 'tensor'), may hold values from -0.21875 to 0.21875
- value_matrix: bfloat16 [768, 768], P('dp', 'tensor'), may hold values from -0.21875 to 0.21875
- query_value_bias: float32 [2, 768], P(None, 'tensor'), may hold values from -3 to 3
- adapter_down_weight: bfloat16 [2, 768, 8], P(None, 'dp'), may hold values from -0.21875 to 0.21875
- adapter_up_weight: bfloat16 [2, 8, 768], P(None, None, 'tensor'), may hold values from -1 to 1
- attention_output_weight: bfloat16 [768, 768], P('tensor', 'dp'), may hold values from -1.75 to 1.75
- feedforward_input_weight: bfloat16 [768, 3072], P('dp', 'tensor'), may hold values from -0.21875 to 0.21875
- feedforward_input_bias: float32 [3072], P('tensor'), may hold values from -3 to 3
- feedforward_output_weight: bfloat16 [3072, 768], P('tensor', 'dp'), may hold values from -0.109375 to 0.109375
- output_bias: float32 [2, 768], replicated, may hold values from -3 to 3
- layernorm_scale: float32 [2, 768], replicated, may hold values from 0.5 to 1.5
- layernorm_bias: float32 [2, 768], replicated, may hold values from -2 to 2
- output_gradient: bfloat16 [4, 8192, 768], P(None, ('dp', 'tensor')), may hold values from -6 to 6
Outputs:
- outputs: bfloat16 [4, 8192, 768], P(None, ('dp', 'tensor'))
- input_grad: float32 [4, 8192, 768], P(None, ('dp', 'tensor'))
- lora_up_grad: float32 [2, 8, 768], P(None, None, 'tensor')
The draws below stay inside these ranges and needn't reach their ends.
Inputs may be any that keep to these rules, and one draw needn't show every extreme that they name: Item i of micro-batch m has live positions 0 to lengths[m, i] - 1 of its 512; the others are padding. An item's first segment is positions 0 to bounds - 1, its second bounds to 511; bounds lies between lengths // 4 and 3 * lengths // 4.
All inputs are finite; a program needn't handle non-finite values.
Results may differ from the reference program's by a relative error of at most 0.015.
The reference program's roundings to bfloat16 on the way count: a program that leaves them out, or rounds other values in their place, can miss the bound.
Values may be sent and summed in bfloat16 or wider, within the bound.
No kernel may reach another device: no remote copies, remote signals or barrier semaphores. Data moves between devices by JAX's collectives and lax.ppermute only.
A program may use at most 192 MiB of HBM per device.

```python
import jax
import jax.numpy as jnp
from jax import lax

MODEL_WIDTH = 768
HEADS = 12
HEAD_DIM = 64
FF = 3072
UPDATE_RANK = 8
SLOT = 512
MB = 4
ITEMS = 16
ROWS = 8192


def item_lengths(key):
    first = jax.random.fold_in(key, 11)
    drawn = jax.random.randint(first, (MB, ITEMS), SLOT // 4, SLOT + 1)
    drawn = drawn.at[0, 0].set(SLOT)
    drawn = drawn.at[MB - 1, ITEMS - 1].set(SLOT // 4)
    return drawn.astype(jnp.int32)


def draw_lengths(key, part):
    return item_lengths(key)


def draw_bounds(key, part):
    drawn = item_lengths(key)
    second = jax.random.fold_in(key, 23)
    result = jax.random.randint(second, (MB, ITEMS), drawn // 4, 3 * drawn // 4 + 1)
    result = result.at[0, 0].set(3 * SLOT // 4)
    result = result.at[MB - 1, ITEMS - 1].set(SLOT // 16)
    return result.astype(jnp.int32)


def shard_levels(stream_key, dims, shards, least, top_value):
    def one(position, blocks):
        draws = jax.random.uniform(jax.random.fold_in(jax.random.fold_in(stream_key, 6), position), (blocks,), jnp.float32, least / len(shards), top_value / len(shards))
        return jnp.repeat(jnp.exp(draws), dims[position] // blocks).reshape((-1,) + (1,) * (len(dims) - position - 1))

    level = one(*shards[0])
    for cut in shards[1:]:
        level = level * one(*cut)
    return level


def scatter_about(stream_key, shape, scale, most, cuts=(), held_as=jnp.bfloat16):
    values = scale * jax.random.normal(stream_key, shape, jnp.float32)
    if cuts:
        values = values * shard_levels(stream_key, shape, cuts, -0.22, 0.18)
    return jnp.clip(values, -most, most).astype(held_as)


def setup_inputs(seed: int = 0) -> dict:
    splits = jax.random.split(jax.random.key(seed), 18)
    return {
        "inputs": scatter_about(splits[0], (MB, ROWS, MODEL_WIDTH), 1.0, 6.0, ((1, 32),)),
        "lengths": draw_lengths(jax.random.fold_in(splits[17], 71), 0),
        "bounds": draw_bounds(jax.random.fold_in(splits[17], 71), 0),
        "query_matrix": scatter_about(splits[3], (MODEL_WIDTH, MODEL_WIDTH), MODEL_WIDTH ** -0.5, 0.21875, ((0, 16), (1, 2))),
        "key_matrix": scatter_about(splits[4], (MODEL_WIDTH, MODEL_WIDTH), MODEL_WIDTH ** -0.5, 0.21875, ((0, 16), (1, 2))),
        "value_matrix": scatter_about(splits[5], (MODEL_WIDTH, MODEL_WIDTH), MODEL_WIDTH ** -0.5, 0.21875, ((0, 16), (1, 2))),
        "query_value_bias": scatter_about(splits[6], (2, MODEL_WIDTH), 0.5, 3.0, ((1, 2),), jnp.float32),
        "adapter_down_weight": scatter_about(splits[7], (2, MODEL_WIDTH, UPDATE_RANK), MODEL_WIDTH ** -0.5, 0.21875, ((1, 16),)),
        "adapter_up_weight": scatter_about(splits[8], (2, UPDATE_RANK, MODEL_WIDTH), 0.15, 1.0, ((2, 2),)),
        "attention_output_weight": scatter_about(splits[9], (MODEL_WIDTH, MODEL_WIDTH), (MODEL_WIDTH // 64) ** -0.5, 1.75, ((0, 2), (1, 16))),
        "feedforward_input_weight": scatter_about(splits[10], (MODEL_WIDTH, FF), MODEL_WIDTH ** -0.5, 0.21875, ((0, 16), (1, 2))),
        "feedforward_input_bias": scatter_about(splits[11], (FF,), 0.5, 3.0, ((0, 2),), jnp.float32),
        "feedforward_output_weight": scatter_about(splits[12], (FF, MODEL_WIDTH), FF ** -0.5, 0.109375, ((0, 2), (1, 16))),
        "output_bias": scatter_about(splits[13], (2, MODEL_WIDTH), 0.5, 3.0, (), jnp.float32),
        "layernorm_scale": jnp.clip(1.0 + 0.1 * jax.random.normal(splits[14], (2, MODEL_WIDTH), jnp.float32), 0.5, 1.5),
        "layernorm_bias": scatter_about(splits[15], (2, MODEL_WIDTH), 0.3, 2.0, (), jnp.float32),
        "output_gradient": scatter_about(splits[16], (MB, ROWS, MODEL_WIDTH), 1.0, 6.0, ((1, 32),)),
    }


adapter_scale = 2.0
masked_value = -1000000000.0
norm_eps = 1e-05
highest_precision = lax.Precision.HIGHEST

@jax.custom_vjp
def low(v):
    return lax.optimization_barrier(v.astype(jnp.bfloat16)).astype(jnp.float32)

@jax.custom_vjp
def low_back(v):
    return v

def low_keep(v):
    return (low(v), None)

def low_pass(kept, grad):
    return (grad,)

def back_keep(v):
    return (v, None)

def back_low(kept, grad):
    return (low(grad),)
low.defvjp(low_keep, low_pass)
low_back.defvjp(back_keep, back_low)

def layer_norm(value_rows, gain, shift):
    centre = value_rows - lax.optimization_barrier(jnp.mean(value_rows, axis=-1, keepdims=True))
    spread = lax.optimization_barrier(jnp.mean(centre * centre, axis=-1, keepdims=True))
    return centre * lax.rsqrt(spread + norm_eps) * gain + shift

def item_mask(length, bound):
    places = jnp.arange(SLOT)
    segment = places >= bound
    return (places < length)[None, :] & (segment[:, None] == segment[None, :])

def attend(pieces):
    query_rows, keys, value_rows, length, bound = pieces
    scores = jnp.einsum('qhd,khd->hqk', query_rows, keys, precision=highest_precision) * 0.125
    scores = jnp.where(item_mask(length, bound)[None], scores, masked_value)
    scores = low_back(scores)
    probs = low(jax.nn.softmax(scores, axis=-1))
    return jnp.einsum('hqk,khd->qhd', probs, value_rows, precision=highest_precision)

def encoder_layer(input_rows, adapter_up_weight, lengths, bounds, frozen_params):
    query_matrix, key_matrix, value_matrix, query_value_bias, adapter_down_weight, attention_output_weight, feedforward_input_weight, feedforward_input_bias, feedforward_output_weight, output_bias, layernorm_scale, layernorm_bias = frozen_params
    count = input_rows.shape[0]
    flattened = input_rows.reshape(count * SLOT, MODEL_WIDTH)
    query_lowrank = jnp.dot(flattened, adapter_down_weight[0], precision=highest_precision)
    value_lowrank = jnp.dot(flattened, adapter_down_weight[1], precision=highest_precision)
    query_rows = jnp.dot(flattened, query_matrix, precision=highest_precision) + query_value_bias[0] + adapter_scale * jnp.dot(query_lowrank, adapter_up_weight[0], precision=highest_precision)
    keys = jnp.dot(flattened, key_matrix, precision=highest_precision)
    value_rows = jnp.dot(flattened, value_matrix, precision=highest_precision) + query_value_bias[1] + adapter_scale * jnp.dot(value_lowrank, adapter_up_weight[1], precision=highest_precision)
    query_rows = low(low_back(query_rows))
    keys = low(low_back(keys))
    value_rows = low(low_back(value_rows))
    array_shape = (count, SLOT, HEADS, HEAD_DIM)
    mixed = lax.map(jax.checkpoint(attend), (query_rows.reshape(array_shape), keys.reshape(array_shape), value_rows.reshape(array_shape), lengths, bounds))
    mixed = low(low_back(mixed.reshape(count * SLOT, MODEL_WIDTH)))
    hidden_sum = flattened + low_back(jnp.dot(mixed, attention_output_weight, precision=highest_precision) + output_bias[0])
    normed = layer_norm(hidden_sum, layernorm_scale[0], layernorm_bias[0])
    pre_act = low_back(jnp.dot(low(normed), feedforward_input_weight, precision=highest_precision) + feedforward_input_bias)
    activated = low(jax.nn.gelu(pre_act, approximate=False))
    ffn_sum = normed + low_back(jnp.dot(activated, feedforward_output_weight, precision=highest_precision) + output_bias[1])
    return layer_norm(ffn_sum, layernorm_scale[1], layernorm_bias[1]).reshape(count, SLOT, MODEL_WIDTH)

def reference(inputs, lengths, bounds, query_matrix, key_matrix, value_matrix, query_value_bias, adapter_down_weight, adapter_up_weight, attention_output_weight, feedforward_input_weight, feedforward_input_bias, feedforward_output_weight, output_bias, layernorm_scale, layernorm_bias, output_gradient):
    frozen_params = tuple((input_array.astype(jnp.float32) for input_array in (query_matrix, key_matrix, value_matrix, query_value_bias, adapter_down_weight, attention_output_weight, feedforward_input_weight, feedforward_input_bias, feedforward_output_weight, output_bias, layernorm_scale, layernorm_bias)))
    group = 8
    blocks = MB * ITEMS // group
    input_rows = inputs.astype(jnp.float32).reshape(blocks, group, SLOT, MODEL_WIDTH)
    cotangent = output_gradient.astype(jnp.float32).reshape(blocks, group, SLOT, MODEL_WIDTH)
    length_blocks = lengths.reshape(blocks, group)
    bound_blocks = bounds.reshape(blocks, group)
    up_weight_float = adapter_up_weight.astype(jnp.float32)

    def advance(total, pieces):
        block_rows, block_cot, block_lengths, block_bounds = pieces
        result, pull = jax.vjp(lambda value_rows, weights: encoder_layer(value_rows, weights, block_lengths, block_bounds, frozen_params), block_rows, up_weight_float)
        row_gradient, grad_up = pull(block_cot)
        return (total + grad_up, (result, row_gradient))
    total, (result_list, row_gradient) = lax.scan(advance, jnp.zeros((2, UPDATE_RANK, MODEL_WIDTH), jnp.float32), (input_rows, cotangent, length_blocks, bound_blocks))
    return (result_list.reshape(MB, ROWS, MODEL_WIDTH).astype(jnp.bfloat16), row_gradient.reshape(MB, ROWS, MODEL_WIDTH), total)
```

```python
import functools

import jax
import jax.numpy as jnp
from jax import lax
from jax.experimental import pallas as pl
from jax.experimental.pallas import tpu as pltpu
from jax.sharding import PartitionSpec as P

F32 = jnp.float32
BF16 = jnp.bfloat16
HEAD_DIM = 64
RANK = 8
LANES = 128
EPS = 1e-05
MASKED = -float(2**30)
SEG = 64
TILE = 256
VMEM_LIMIT = 60 * 2**20

NT = (((1,), (1,)), ((), ()))
TN = (((0,), (0,)), ((), ()))


def mm(a, b):
    return jnp.dot(a, b, preferred_element_type=F32)


def mm_nt(a, b):
    return lax.dot_general(a, b, NT, preferred_element_type=F32)


def mm_tn(a, b):
    return lax.dot_general(a, b, TN, preferred_element_type=F32)


def lane_iota(shape):
    return lax.broadcasted_iota(jnp.int32, shape, len(shape) - 1)


def three_parts(value, lane):
    high = value.astype(BF16).astype(F32)
    rest = value - high
    middle = rest.astype(BF16).astype(F32)
    low = rest - middle
    parts = jnp.where(lane < 16, high, jnp.where(lane < 32, middle, jnp.where(lane < 48, low, 0.0)))
    return parts.astype(BF16)


def two_parts(value):
    high = value.astype(BF16)
    low = (value - high.astype(F32)).astype(BF16)
    return jnp.concatenate([high, low], axis=1)


def load_weights(layout, offsets, pieces, target, sems, columns):
    copies = []
    for group, (first, width) in enumerate(columns):
        for half in range(2):
            for piece, (ref, blocks) in enumerate(zip(pieces[half], layout, strict=True)):
                rows = ref.shape[0] // len(blocks)
                for place, block in enumerate(blocks):
                    start = offsets[block]
                    if rows % 16 == 0:
                        start = pl.multiple_of(start, 16)
                    copies.append(
                        (
                            group,
                            pltpu.make_async_copy(
                                ref.at[pl.ds(place * rows, rows), pl.ds(first, width)],
                                target.at[half, pl.ds(start, rows), pl.ds(first, width)],
                                sems.at[group],
                            ),
                        )
                    )
    return copies


def project_attend_kernel(layout, offsets, lengths, bounds, *refs):
    n = len(layout)
    pieces = (refs[:n], refs[n : 2 * n])
    (
        x_ref,
        bias_ref,
        up_query_ref,
        up_value_ref,
        query_ref,
        key_ref,
        value_ref,
        mixed_ref,
        spare_ref,
        low_ref,
        weights,
        sems,
    ) = refs[2 * n :]
    item = pl.program_id(0)
    half_width = query_ref.shape[2] // 2

    @pl.when(item == 0)
    def _():
        copies = load_weights(layout, offsets, pieces, weights, sems, ((0, weights.shape[2]),))
        for _, copy in copies:
            copy.start()
        for _, copy in copies:
            copy.wait()

    slot = x_ref.shape[1]
    x = x_ref[0]
    low = two_parts(mm(x, weights[0, :, 3 * half_width :]))
    low_ref[0] = low
    for half in range(2):
        at = slice(half * half_width, (half + 1) * half_width)
        query = (
            mm(x, weights[half, :, :half_width])
            + bias_ref[0:1, at]
            + mm(low, up_query_ref[:, at])
        )
        query_ref[0, :, at] = query.astype(BF16) * 0.125
        key_ref[0, :, at] = mm(x, weights[half, :, half_width : 2 * half_width]).astype(BF16)
        value = (
            mm(x, weights[half, :, 2 * half_width : 3 * half_width])
            + bias_ref[1:2, at]
            + mm(low, up_value_ref[:, at])
        )
        value_ref[0, :, at] = value.astype(BF16)

    length = lengths[item]
    bound = bounds[item]
    lane = lane_iota((slot, LANES))
    place = lax.broadcasted_iota(jnp.int32, (slot, LANES), 0)
    second = place >= bound
    flags = jnp.where(
        lane == SEG,
        jnp.where(second, 1.0, 0.0),
        jnp.where(lane == SEG + 1, jnp.where(second, 0.0, 1.0), jnp.where(lane == SEG + 2, 1.0, 0.0)),
    )
    key_flags = jnp.where(
        lane == SEG,
        jnp.where(second, 0.0, MASKED),
        jnp.where(
            lane == SEG + 1,
            jnp.where(second, MASKED, 0.0),
            jnp.where((lane == SEG + 2) & (place >= length), MASKED, 0.0),
        ),
    ).astype(BF16)
    ones = jnp.where(lane == 0, 1.0, 0.0).astype(BF16)
    query_flags = flags.astype(BF16)
    tile_lane = lane_iota((TILE, LANES))
    zero = jnp.zeros((TILE, LANES), BF16)
    logs = [jnp.zeros((TILE, LANES), F32) for _ in range(slot // TILE)]
    for pair in range(2 * half_width // LANES):
        at = slice(pair * LANES, (pair + 1) * LANES)
        keys = jnp.concatenate([key_ref[0, :, at], key_flags], axis=1)
        values = jnp.concatenate([value_ref[0, :, at], ones], axis=1)
        for tile in range(slot // TILE):
            rows = slice(tile * TILE, (tile + 1) * TILE)
            query = query_ref[0, rows, at]
            outs = []
            for side in range(2):
                inside = (tile_lane < HEAD_DIM) if side == 0 else (tile_lane >= HEAD_DIM)
                scores = mm_nt(
                    jnp.concatenate([jnp.where(inside, query, zero), query_flags[rows]], axis=1), keys
                )
                peak = jnp.max(scores, axis=-1, keepdims=True)
                probs = jnp.exp(scores - peak).astype(BF16)
                out = mm(probs, values)
                total = out[:, LANES : LANES + 1]
                outs.append(out[:, :LANES] * (1.0 / total))
                head = 2 * pair + side
                logs[tile] = jnp.where((tile_lane & 15) == head, peak + jnp.log(total), logs[tile])
            mixed_ref[0, rows, at] = jnp.where(tile_lane < HEAD_DIM, outs[0], outs[1]).astype(BF16)
    for tile in range(slot // TILE):
        rows = slice(tile * TILE, (tile + 1) * TILE)
        spare_ref[0, rows] = (
            three_parts(logs[tile], tile_lane).astype(F32) + flags[rows]
        ).astype(BF16)


def row_mean(value):
    return jnp.mean(value, axis=-1, keepdims=True)


def normalize(value):
    centre = value - row_mean(value)
    scale = lax.rsqrt(row_mean(centre * centre) + EPS)
    return centre * scale, scale


def normalize_back(grad, gain, normal, scale):
    grad = grad * gain
    return scale * (grad - row_mean(grad) - normal * row_mean(grad * normal))


def feed_kernel(layout, offsets, *refs):
    n = len(layout)
    pieces = (refs[:n], refs[n : 2 * n])
    (
        x_ref,
        mixed_ref,
        grad_ref,
        hidden_bias_ref,
        output_bias_ref,
        gain_ref,
        shift_ref,
        out_ref,
        grad_hidden_ref,
        grad_mixed_ref,
        weights,
        slope,
        sems,
    ) = refs[2 * n :]
    width = x_ref.shape[1]
    heads = width // 2
    hidden = hidden_bias_ref.shape[1] // 2
    chunk = 512
    first_in = heads
    first_out = heads + hidden

    @pl.when(pl.program_id(0) == 0)
    def _():
        columns = ((0, heads), (first_in, hidden), (first_out, hidden))
        copies = load_weights(layout, offsets, pieces, weights, sems, columns)
        for _, copy in copies:
            copy.start()
        for _, copy in copies:
            copy.wait()

    x = x_ref[...].astype(F32)
    summed = x + output_bias_ref[0:1]
    for half in range(2):
        summed += mm_nt(mixed_ref[:, half * heads : (half + 1) * heads], weights[half, :, :heads])
    normal_in, scale_in = normalize(summed)
    normed = normal_in * gain_ref[0:1] + shift_ref[0:1]
    normed_low = normed.astype(BF16)
    total = normed + output_bias_ref[1:2]
    for half in range(2):
        for part in range(hidden // chunk):
            at = part * chunk
            wide = half * hidden + at
            pre = mm(normed_low, weights[half, :, first_in + at : first_in + at + chunk])
            pre = pre + hidden_bias_ref[:, wide : wide + chunk]
            share = 0.5 * (1.0 + lax.erf(pre * 0.7071067811865476))
            slope[:, wide : wide + chunk] = share + pre * jnp.exp(-0.5 * pre * pre) * 0.3989422804014327
            active = (pre * share).astype(BF16)
            total += mm_nt(active, weights[half, :, first_out + at : first_out + at + chunk])
    normal_out, scale_out = normalize(total)
    out_ref[...] = (normal_out * gain_ref[1:2] + shift_ref[1:2]).astype(BF16)
    grad_total = normalize_back(grad_ref[...].astype(F32), gain_ref[1:2], normal_out, scale_out)
    grad_low = grad_total.astype(BF16)
    grad_normed = grad_total
    for half in range(2):
        for part in range(hidden // chunk):
            at = part * chunk
            wide = half * hidden + at
            grad_active = mm(grad_low, weights[half, :, first_out + at : first_out + at + chunk])
            grad_pre = (grad_active * slope[:, wide : wide + chunk]).astype(BF16)
            grad_normed += mm_nt(grad_pre, weights[half, :, first_in + at : first_in + at + chunk])
    grad_hidden = normalize_back(grad_normed, gain_ref[0:1], normal_in, scale_in)
    grad_hidden_ref[...] = grad_hidden
    grad_hidden_low = grad_hidden.astype(BF16)
    for half in range(2):
        grad_mixed_ref[:, half * heads : (half + 1) * heads] = mm(
            grad_hidden_low, weights[half, :, :heads]
        ).astype(BF16)


def attend_back_kernel(layout, offsets, lengths, bounds, *refs):
    n = len(layout)
    pieces = (refs[:n], refs[n : 2 * n])
    (
        query_ref,
        key_ref,
        value_ref,
        mixed_ref,
        spare_ref,
        low_ref,
        grad_mixed_ref,
        grad_hidden_ref,
        up_query_ref,
        up_value_ref,
        out_ref,
        adapter_ref,
        weights,
        grad_query,
        grad_key,
        grad_value,
        sems,
    ) = refs[2 * n :]
    item = pl.program_id(0)
    slot, width = query_ref.shape[1:]
    half_width = width // 2

    @pl.when(item == 0)
    def _():
        copies = load_weights(layout, offsets, pieces, weights, sems, ((0, weights.shape[2]),))
        for _, copy in copies:
            copy.start()
        for _, copy in copies:
            copy.wait()

    length = lengths[item]
    bound = bounds[item]
    lane = lane_iota((slot, LANES))
    place = lax.broadcasted_iota(jnp.int32, (slot, LANES), 0)
    second = place >= bound
    key_flags = jnp.where(
        lane == SEG,
        jnp.where(second, 0.0, MASKED),
        jnp.where(
            lane == SEG + 1,
            jnp.where(second, MASKED, 0.0),
            jnp.where((lane == SEG + 2) & (place >= length), MASKED, 0.0),
        ),
    )
    row = lax.broadcasted_iota(jnp.int32, (width, LANES), 0)
    column = lane_iota((width, LANES))
    pick = jnp.where((row // HEAD_DIM == (column & 15)) & (column < 48), 1.0, 0.0).astype(BF16)
    product = grad_mixed_ref[0].astype(F32) * mixed_ref[0].astype(F32)
    high = product.astype(BF16)
    rest = (product - high.astype(F32)).astype(BF16)
    inner = three_parts(mm(high, pick) + mm(rest, pick), lane)
    spare = spare_ref[0]
    low_side = lane < HEAD_DIM
    zero = jnp.zeros((slot, LANES), BF16)
    for pair in range(width // LANES):
        at = slice(pair * LANES, (pair + 1) * LANES)
        query = query_ref[0, :, at]
        keys = key_ref[0, :, at]
        values = value_ref[0, :, at]
        grad = grad_mixed_ref[0, :, at]
        total_query = jnp.zeros((slot, LANES), F32)
        total_key = jnp.zeros((slot, LANES), F32)
        total_value = jnp.zeros((slot, LANES), F32)
        for side in range(2):
            head = 2 * pair + side
            inside = low_side if side == 0 else lane >= HEAD_DIM
            mine = ((lane & 15) == head) & (lane < 48)
            query_side = jnp.where(inside, query, zero)
            key_side = jnp.where(inside, keys, zero)
            grad_side = jnp.where(inside, grad, zero)
            key_wide = jnp.concatenate([keys, jnp.where(mine, -1.0, key_flags).astype(BF16)], axis=1)
            value_wide = jnp.concatenate([values, jnp.where(mine, -1.0, 0.0).astype(BF16)], axis=1)
            probs = jnp.exp(mm_nt(key_wide, jnp.concatenate([query_side, spare], axis=1)))
            grad_probs = mm_nt(value_wide, jnp.concatenate([grad_side, inner], axis=1))
            grad_scores = (probs * grad_probs).astype(BF16)
            total_value += mm(probs.astype(BF16), grad_side)
            total_key += mm(grad_scores, query_side)
            total_query += mm_tn(grad_scores, key_side)
        grad_query[:, at] = (total_query * 0.125).astype(BF16)
        grad_key[:, at] = total_key.astype(BF16)
        grad_value[:, at] = total_value.astype(BF16)

    small = mm_nt(grad_query[...], up_query_ref[:LANES]) + mm_nt(grad_value[...], up_value_ref[:LANES])
    down = weights[0, :, 3 * half_width :]
    total = grad_hidden_ref[0] + mm_nt(two_parts(small), jnp.concatenate([down, down], axis=1))
    for half in range(2):
        at = slice(half * half_width, (half + 1) * half_width)
        for index, grads in enumerate((grad_query, grad_key, grad_value)):
            total += mm_nt(
                grads[:, at], weights[half, :, index * half_width : (index + 1) * half_width]
            )
    out_ref[0] = total
    low = low_ref[0]
    by_query = mm_tn(low, grad_query[...])
    by_value = mm_tn(low, grad_value[...])
    update = 2.0 * jnp.concatenate(
        [
            by_query[:RANK] + by_query[LANES : LANES + RANK],
            by_value[RANK : 2 * RANK] + by_value[LANES + RANK : LANES + 2 * RANK],
        ],
        axis=0,
    )

    @pl.when(item == 0)
    def _():
        adapter_ref[...] = update

    @pl.when(item > 0)
    def _():
        adapter_ref[...] += update


def any_spec():
    return pl.BlockSpec(memory_space=pl.ANY)


def whole_spec(array):
    return pl.BlockSpec(array.shape, lambda i, *_: (0,) * array.ndim)


def item_spec(shape):
    return pl.BlockSpec((1, *shape[1:]), lambda i, *_: (i, 0, 0))


def shape_of(shape, dtype):
    return jax.ShapeDtypeStruct(shape, dtype)


def project_attend(layout, offsets, lengths, bounds, pieces, x, bias, up_query, up_value):
    items, slot, width = x.shape
    flat = [*pieces[0], *pieces[1]]
    columns = pieces[0][0].shape[1]
    outs = [shape_of(x.shape, BF16)] * 4 + [
        shape_of((items, slot, LANES), BF16),
        shape_of((items, slot, 2 * LANES), BF16),
    ]
    flops = 2 * items * slot * width * (3 * width + 4 * slot)
    return pl.pallas_call(
        functools.partial(project_attend_kernel, layout),
        grid_spec=pltpu.PrefetchScalarGridSpec(
            num_scalar_prefetch=3,
            grid=(items,),
            in_specs=[any_spec()] * len(flat)
            + [item_spec(x.shape), whole_spec(bias), whole_spec(up_query), whole_spec(up_value)],
            out_specs=[item_spec(out.shape) for out in outs],
            scratch_shapes=[
                pltpu.VMEM((2, width, columns), BF16),
                pltpu.SemaphoreType.DMA((1,)),
            ],
        ),
        out_shape=outs,
        compiler_params=pltpu.CompilerParams(vmem_limit_bytes=VMEM_LIMIT),
        cost_estimate=pl.CostEstimate(
            flops=flops, bytes_accessed=12 * items * slot * width, transcendentals=items * slot * slot * 12
        ),
        name="project_attend",
    )(offsets, lengths, bounds, *flat, x, bias, up_query, up_value)


def feed(layout, offsets, pieces, x, mixed, grad, hidden_bias, output_bias, gain, shift):
    rows, width = x.shape
    flat = [*pieces[0], *pieces[1]]
    columns = pieces[0][0].shape[1]
    tile = pl.BlockSpec((TILE, width), lambda i, *_: (i, 0))
    outs = [shape_of(x.shape, BF16), shape_of(x.shape, F32), shape_of(x.shape, BF16)]
    smalls = (hidden_bias, output_bias, gain, shift)
    return pl.pallas_call(
        functools.partial(feed_kernel, layout),
        grid_spec=pltpu.PrefetchScalarGridSpec(
            num_scalar_prefetch=1,
            grid=(rows // TILE,),
            in_specs=[any_spec()] * len(flat) + [tile] * 3 + [whole_spec(a) for a in smalls],
            out_specs=[tile] * 3,
            scratch_shapes=[
                pltpu.VMEM((2, width, columns), BF16),
                pltpu.VMEM((TILE, hidden_bias.shape[1]), F32),
                pltpu.SemaphoreType.DMA((3,)),
            ],
        ),
        out_shape=outs,
        compiler_params=pltpu.CompilerParams(vmem_limit_bytes=VMEM_LIMIT),
        cost_estimate=pl.CostEstimate(
            flops=8 * rows * width * columns, bytes_accessed=4 * width * columns, transcendentals=0
        ),
        name="feed",
    )(offsets, *flat, x, mixed, grad, *smalls)


def attend_back(layout, offsets, lengths, bounds, pieces, query, key, value, mixed, spare, low, grad_mixed, grad_hidden, up_query, up_value):
    items, slot, width = query.shape
    flat = [*pieces[0], *pieces[1]]
    columns = pieces[0][0].shape[1]
    blocks = (query, key, value, mixed, spare, low, grad_mixed, grad_hidden)
    adapter = (2 * RANK, width)
    return pl.pallas_call(
        functools.partial(attend_back_kernel, layout),
        grid_spec=pltpu.PrefetchScalarGridSpec(
            num_scalar_prefetch=3,
            grid=(items,),
            in_specs=[any_spec()] * len(flat)
            + [item_spec(a.shape) for a in blocks]
            + [whole_spec(up_query), whole_spec(up_value)],
            out_specs=[item_spec(query.shape), pl.BlockSpec(adapter, lambda i, *_: (0, 0))],
            scratch_shapes=[
                pltpu.VMEM((2, width, columns), BF16),
                pltpu.VMEM((slot, width), BF16),
                pltpu.VMEM((slot, width), BF16),
                pltpu.VMEM((slot, width), BF16),
                pltpu.SemaphoreType.DMA((1,)),
            ],
        ),
        out_shape=[shape_of(query.shape, F32), shape_of(adapter, F32)],
        compiler_params=pltpu.CompilerParams(vmem_limit_bytes=VMEM_LIMIT),
        cost_estimate=pl.CostEstimate(
            flops=2 * items * slot * width * (3 * width + 10 * slot),
            bytes_accessed=16 * items * slot * width,
            transcendentals=items * slot * slot * 12,
        ),
        name="attend_back",
    )(offsets, lengths, bounds, *flat, *blocks, up_query, up_value)


def swap(array):
    return lax.ppermute(array, "tensor", [(0, 1), (1, 0)])


def ring_gather(shard, count):
    def moved(array, target):
        return lax.ppermute(array, "dp", [(i, target(i)) for i in range(count)])

    plane = [shard] + [moved(shard, lambda i, d=d: (i + 4 * d) % count) for d in (1, 2, 3)]
    line = jnp.concatenate(plane, axis=0)
    half = line.shape[0] // 2
    by_x = moved(line, lambda i: i ^ 1)
    by_y = moved(line, lambda i: i ^ 2)
    far_low = moved(by_x[:half], lambda i: i ^ 2)
    far_high = moved(by_y[half:], lambda i: i ^ 1)
    return [line, by_x, by_y, far_low, far_high]


RING_LAYOUT = ((0, 1, 2, 3), (4, 5, 6, 7), (8, 9, 10, 11), (12, 13), (14, 15))


def ring_offsets(index, rows):
    table = []
    for flip in (0, 1, 2, 3):
        for back in range(4):
            table.append((((index ^ flip) - 4 * back) % 16) * rows)
    return jnp.stack(table).astype(jnp.int32)


def local(
    inputs,
    lengths,
    bounds,
    query_matrix,
    key_matrix,
    value_matrix,
    query_value_bias,
    adapter_down_weight,
    adapter_up_weight,
    attention_output_weight,
    feedforward_input_weight,
    feedforward_input_bias,
    feedforward_output_weight,
    output_bias,
    layernorm_scale,
    layernorm_bias,
    output_gradient,
    *,
    count,
):
    micro, rows, width = inputs.shape
    mine = micro // 2
    core = lax.axis_index("tensor")
    shard_rows = query_matrix.shape[0]

    down = jnp.transpose(adapter_down_weight, (1, 0, 2)).reshape(shard_rows, 2 * RANK)
    down = jnp.pad(down, ((0, 0), (0, LANES - 2 * RANK)))
    shard = jnp.concatenate([query_matrix, key_matrix, value_matrix, down], axis=1)
    shard_feed = jnp.concatenate(
        [attention_output_weight.T, feedforward_input_weight, feedforward_output_weight.T], axis=1
    )
    zero = jnp.zeros((1,), jnp.int32)
    if count == 16:
        offsets = ring_offsets(lax.axis_index("dp"), shard_rows)
        layout = RING_LAYOUT
        own = ring_gather(shard, count)
    else:
        offsets = zero
        layout = ((0,),)
        own = [lax.all_gather(shard, "dp", axis=0, tiled=True)]
    pieces = (own, [swap(piece) for piece in own])
    own_feed = [lax.all_gather(shard_feed, "dp", axis=0, tiled=True)]
    pieces_feed = (own_feed, [swap(piece) for piece in own_feed])

    first = core * mine
    other_first = (1 - core) * mine

    def take_items(array):
        kept = lax.dynamic_slice_in_dim(array, first, mine, 0)
        given = lax.dynamic_slice_in_dim(array, other_first, mine, 0)
        got = swap(given)
        return jnp.where(
            core == 0,
            jnp.concatenate([kept, got], axis=1),
            jnp.concatenate([got, kept], axis=1),
        )

    def give_items(array):
        kept = lax.dynamic_slice_in_dim(array, core * rows, rows, 1)
        given = lax.dynamic_slice_in_dim(array, (1 - core) * rows, rows, 1)
        got = swap(given)
        return jnp.where(
            core == 0,
            jnp.concatenate([kept, got], axis=0),
            jnp.concatenate([got, kept], axis=0),
        )

    x = take_items(inputs)
    grad = take_items(output_gradient)
    my_lengths = lax.dynamic_slice_in_dim(lengths[:, 0], first, mine, 0)
    my_bounds = lax.dynamic_slice_in_dim(bounds[:, 0], first, mine, 0)

    bias = jnp.concatenate([query_value_bias, swap(query_value_bias)], axis=1)
    hidden_bias = feedforward_input_bias[None]
    hidden_bias = jnp.concatenate([hidden_bias, swap(hidden_bias)], axis=1)
    up = jnp.concatenate([adapter_up_weight, swap(adapter_up_weight)], axis=2) * 2
    up_query = jnp.pad(up[0], ((0, LANES - RANK), (0, 0)))
    up_value = jnp.pad(up[1], ((RANK, LANES - 2 * RANK), (0, 0)))
    up_query = jnp.concatenate([up_query, up_query], axis=0)
    up_value = jnp.concatenate([up_value, up_value], axis=0)

    query, key, value, mixed, spare, low = project_attend(
        layout, offsets, my_lengths, my_bounds, pieces, x, bias, up_query, up_value
    )
    flat = (mine * 2 * rows, width)
    out, grad_hidden, grad_mixed = feed(
        ((0,),),
        zero,
        pieces_feed,
        x.reshape(flat),
        mixed.reshape(flat),
        grad.reshape(flat),
        hidden_bias,
        output_bias,
        layernorm_scale,
        layernorm_bias,
    )
    input_grad, adapter = attend_back(
        layout,
        offsets,
        my_lengths,
        my_bounds,
        pieces,
        query,
        key,
        value,
        mixed,
        spare,
        low,
        grad_mixed.reshape(x.shape),
        grad_hidden.reshape(x.shape),
        up_query,
        up_value,
    )
    half = width // 2
    adapter = adapter[:, :half] + swap(adapter[:, half:])
    adapter = lax.psum(adapter, "dp").reshape(2, RANK, half)
    return give_items(out.reshape(x.shape)), give_items(input_grad), adapter


def solution(mesh):
    return jax.shard_map(
        functools.partial(local, count=mesh.shape["dp"]),
        mesh=mesh,
        in_specs=(
            P(None, ("dp", "tensor"), None),
            P(None, "dp"),
            P(None, "dp"),
            P("dp", "tensor"),
            P("dp", "tensor"),
            P("dp", "tensor"),
            P(None, "tensor"),
            P(None, "dp", None),
            P(None, None, "tensor"),
            P("tensor", "dp"),
            P("dp", "tensor"),
            P("tensor"),
            P("tensor", "dp"),
            P(),
            P(),
            P(),
            P(None, ("dp", "tensor"), None),
        ),
        out_specs=(
            P(None, ("dp", "tensor"), None),
            P(None, ("dp", "tensor"), None),
            P(None, None, "tensor"),
        ),
        check_vma=False,
    )
```

```python
import functools

import jax
import jax.numpy as jnp
from jax import lax
from jax.experimental import pallas as pl
from jax.experimental.pallas import tpu as pltpu
from jax.sharding import PartitionSpec as P

F32 = jnp.float32
BF16 = jnp.bfloat16
HEAD_DIM = 64
RANK = 8
LANES = 128
EPS = 1e-05
MASKED = -float(2**30)
SEG = 64
VMEM_LIMIT = 60 * 2**20

NT = (((1,), (1,)), ((), ()))
TN = (((0,), (0,)), ((), ()))


def mm(a, b):
    return jnp.dot(a, b, preferred_element_type=F32)


def mm_nt(a, b):
    return lax.dot_general(a, b, NT, preferred_element_type=F32)


def mm_tn(a, b):
    return lax.dot_general(a, b, TN, preferred_element_type=F32)


def iota(shape, dimension):
    return lax.broadcasted_iota(jnp.int32, shape, dimension)


def three_parts(value, lane):
    high = value.astype(BF16).astype(F32)
    rest = value - high
    middle = rest.astype(BF16).astype(F32)
    return jnp.where(lane < 16, high, jnp.where(lane < 32, middle, jnp.where(lane < 48, rest - middle, 0.0)))


def two_parts(value):
    high = value.astype(BF16)
    return jnp.concatenate([high, (value - high.astype(F32)).astype(BF16)], axis=1)


def weight_copies(layout, offsets, pieces, target, sem, columns):
    copies = []
    for half, first, width, to in columns:
        for ref, blocks in zip(pieces[half], layout, strict=True):
            rows = ref.shape[0] // len(blocks)
            for place, block in enumerate(blocks):
                start = offsets[block]
                if rows % 16 == 0:
                    start = pl.multiple_of(start, 16)
                copies.append(
                    pltpu.make_async_copy(
                        ref.at[pl.ds(place * rows, rows), pl.ds(first, width)],
                        target.at[pl.ds(start, rows), pl.ds(to, width)],
                        sem,
                    )
                )
    return copies


def start_all(copies):
    for copy in copies:
        copy.start()


def wait_all(copies):
    for copy in copies:
        copy.wait()


def places(core, shape, half_slot):
    row = iota(shape, 0)
    return jnp.where(row < half_slot, row + core * half_slot, row - core * half_slot)


def flags_of(core, length, bound, slot):
    lane = iota((slot, LANES), 1)
    place = places(core, (slot, LANES), slot // 2)
    second = place >= bound
    query = jnp.where(
        lane == SEG,
        jnp.where(second, 1.0, 0.0),
        jnp.where(lane == SEG + 1, jnp.where(second, 0.0, 1.0), jnp.where(lane == SEG + 2, 1.0, 0.0)),
    )
    key = jnp.where(
        lane == SEG,
        jnp.where(second, 0.0, MASKED),
        jnp.where(
            lane == SEG + 1,
            jnp.where(second, MASKED, 0.0),
            jnp.where((lane == SEG + 2) & (place >= length), MASKED, 0.0),
        ),
    )
    return lane, query, key


def pair_columns(pair, heads):
    per_half = heads // LANES
    base = (pair // per_half) * 3 * heads + (pair % per_half) * LANES
    return base, base + heads, base + 2 * heads


def load_projections(layout, offsets, pieces, weights, sem, heads, downs):
    wide = 3 * heads
    columns = [(0, 0, wide, 0), (1, 0, wide, wide)]
    columns += [(0, wide, LANES, to) for to in downs]
    return weight_copies(layout, offsets, pieces, weights, sem, columns)


def ups(up_refs, heads):
    blank = jnp.zeros((RANK, heads), BF16)
    parts = []
    for ref in up_refs:
        parts += [
            jnp.concatenate([ref[0] * 2, blank], axis=0),
            jnp.concatenate([blank, blank], axis=0),
            jnp.concatenate([blank, ref[1] * 2], axis=0),
        ]
    return jnp.concatenate(parts, axis=1)


def project_attend_kernel(layout, offsets, lengths, bounds, core_ref, *refs):
    n = len(layout)
    pieces = (refs[:n], refs[n : 2 * n])
    (
        x_own_ref,
        x_got_ref,
        bias_ref,
        up_own_ref,
        up_got_ref,
        qkv_ref,
        mixed_ref,
        spare_ref,
        low_ref,
        weights,
        down,
        sems,
    ) = refs[2 * n :]
    item = pl.program_id(0)
    core = core_ref[0]
    slot, width = mixed_ref.shape[1:]
    heads = width // 2

    @pl.when(item == 0)
    def _():
        wide = 3 * heads
        copies = weight_copies(layout, offsets, pieces, weights, sems.at[0], [(0, 0, wide, 0), (1, 0, wide, wide)])
        downs = weight_copies(layout, offsets, pieces, down, sems.at[1], [(0, wide, LANES, 0)])
        start_all(downs)
        start_all(copies)
        weights[width:] = jnp.zeros((2 * LANES, 6 * heads), BF16)
        up = ups((up_own_ref, up_got_ref), heads)
        weights[width : width + 2 * RANK] = up
        weights[width + LANES : width + LANES + 2 * RANK] = up
        wait_all(downs)
        wait_all(copies)

    x = jnp.concatenate([x_own_ref[0], x_got_ref[0]], axis=0)
    low = two_parts(mm(x, down[...]))
    low_ref[0] = low
    wide_x = jnp.concatenate([x, low], axis=1)
    for part in range(3):
        at = slice(part * width, (part + 1) * width)
        out = (mm(wide_x, weights[:, at]) + bias_ref[0:1, at]) * bias_ref[1:2, at]
        qkv_ref[0, :, at] = out.astype(BF16)

    lane, query_flags, key_flags = flags_of(core, lengths[item], bounds[item], slot)
    query_low = query_flags.astype(BF16)
    key_low = key_flags.astype(BF16)
    ones = jnp.where(lane == 0, 1.0, 0.0).astype(BF16)
    zero = jnp.zeros((slot, LANES), BF16)
    totals = jnp.ones((slot, LANES), F32)
    peaks = []
    for pair in range(width // LANES):
        at_query, at_key, at_value = pair_columns(pair, heads)
        query = qkv_ref[0, :, at_query : at_query + LANES]
        keys = jnp.concatenate([qkv_ref[0, :, at_key : at_key + LANES], key_low], axis=1)
        values = jnp.concatenate([qkv_ref[0, :, at_value : at_value + LANES], ones], axis=1)
        outs = []
        for side in range(2):
            inside = (lane < HEAD_DIM) if side == 0 else (lane >= HEAD_DIM)
            query_side = jnp.concatenate([jnp.where(inside, query, zero), query_low], axis=1)
            scores = mm_nt(keys, query_side)
            peak = jnp.max(scores, axis=0, keepdims=True)
            probs = jnp.exp(scores - peak).astype(BF16)
            out = mm_tn(probs, values)
            total = out[:, LANES : LANES + 1]
            outs.append(out[:, :LANES] * (1.0 / total))
            totals = jnp.where((lane & 15) == 2 * pair + side, total, totals)
            peaks.append(peak)
        mixed_ref[0, :, pair * LANES : (pair + 1) * LANES] = jnp.where(
            lane < HEAD_DIM, outs[0], outs[1]
        ).astype(BF16)
    peaks += [jnp.zeros((1, slot), F32)] * (16 - len(peaks))
    peaks = jnp.concatenate(peaks, axis=0)
    peaks = jnp.concatenate([peaks] * (LANES // 16), axis=0).T
    spare_ref[0] = (three_parts(peaks + jnp.log(totals), lane) + query_flags).astype(BF16)


def row_mean(value):
    return jnp.mean(value, axis=-1, keepdims=True)


def normalize(value):
    centre = value - row_mean(value)
    scale = lax.rsqrt(row_mean(centre * centre) + EPS)
    return centre * scale, scale


def normalize_back(grad, gain, normal, scale):
    grad = grad * gain
    return scale * (grad - row_mean(grad) - normal * row_mean(grad * normal))


def feed_kernel(layouts, chunks, offsets, core_ref, *refs):
    n, m = map(len, layouts)
    pieces = (refs[:n], refs[n : 2 * n])
    pieces_last = (refs[2 * n : 2 * n + m], refs[2 * n + m : 2 * n + 2 * m])
    (
        x_own_ref,
        x_got_ref,
        mixed_ref,
        grad_own_ref,
        grad_got_ref,
        hidden_bias_ref,
        output_bias_ref,
        gain_ref,
        shift_ref,
        out_own_ref,
        out_got_ref,
        grad_hidden_ref,
        grad_mixed_ref,
        out_weights,
        in_weights,
        back_weights,
        slope,
        sems,
    ) = refs[2 * (n + m) :]
    slot, width = mixed_ref.shape[1:]
    half_slot = slot // 2
    heads = width // 2
    first, last = chunks
    parts = [(0, first), (first, first), (2 * first, last), (2 * first + last, last)]

    @pl.when(pl.program_id(0) == 0)
    def _():
        o = heads
        copies = weight_copies(layouts[0], offsets, pieces, out_weights, sems.at[0], [(0, 0, o, 0), (1, 0, o, o)])
        copies += weight_copies(
            layouts[0], offsets, pieces, in_weights, sems.at[0], [(0, o, first, 0), (1, o, first, first)]
        )
        copies += weight_copies(
            layouts[0], offsets, pieces, back_weights, sems.at[0], [(0, o + first, first, 0), (1, o + first, first, first)]
        )
        at = 2 * first
        copies += weight_copies(
            layouts[1], offsets, pieces_last, in_weights, sems.at[0], [(0, 0, last, at), (1, 0, last, at + last)]
        )
        copies += weight_copies(
            layouts[1], offsets, pieces_last, back_weights, sems.at[0], [(0, last, last, at), (1, last, last, at + last)]
        )
        start_all(copies)
        wait_all(copies)

    x = jnp.concatenate([x_own_ref[0], x_got_ref[0]], axis=0).astype(F32)
    summed = x + output_bias_ref[0:1] + mm_nt(mixed_ref[0], out_weights[...])
    normal_in, scale_in = normalize(summed)
    normed = normal_in * gain_ref[0:1] + shift_ref[0:1]
    normed_low = normed.astype(BF16)
    total = normed + output_bias_ref[1:2]
    for at, size in parts:
        pre = mm(normed_low, in_weights[:, at : at + size]) + hidden_bias_ref[:, at : at + size]
        share = 0.5 * (1.0 + lax.erf(pre * 0.7071067811865476))
        slope[:, at : at + size] = share + pre * jnp.exp(-0.5 * pre * pre) * 0.3989422804014327
        total += mm_nt((pre * share).astype(BF16), back_weights[:, at : at + size])
    normal_out, scale_out = normalize(total)
    out = (normal_out * gain_ref[1:2] + shift_ref[1:2]).astype(BF16)
    out_own_ref[0] = out[:half_slot]
    out_got_ref[0] = out[half_slot:]
    grad = jnp.concatenate([grad_own_ref[0], grad_got_ref[0]], axis=0).astype(F32)
    grad_total = normalize_back(grad, gain_ref[1:2], normal_out, scale_out)
    grad_low = grad_total.astype(BF16)
    grad_normed = grad_total
    for at, size in parts:
        grad_pre = (mm(grad_low, back_weights[:, at : at + size]) * slope[:, at : at + size]).astype(BF16)
        grad_normed += mm_nt(grad_pre, in_weights[:, at : at + size])
    grad_hidden = normalize_back(grad_normed, gain_ref[0:1], normal_in, scale_in)
    grad_hidden_ref[0] = grad_hidden
    grad_mixed_ref[0] = mm(grad_hidden.astype(BF16), out_weights[...]).astype(BF16)


def attend_back_kernel(lengths, bounds, core_ref, *refs):
    (
        qkv_ref,
        mixed_ref,
        spare_ref,
        low_ref,
        grad_mixed_ref,
        grads_ref,
        adapter_own_ref,
        adapter_got_ref,
    ) = refs
    item = pl.program_id(0)
    core = core_ref[0]
    slot, width = mixed_ref.shape[1:]
    heads = width // 2

    lane, _, key_flags = flags_of(core, lengths[item], bounds[item], slot)
    row = iota((width, LANES), 0)
    column = iota((width, LANES), 1)
    pick = jnp.where((row // HEAD_DIM == (column & 15)) & (column < 48), 1.0, 0.0).astype(BF16)
    product = grad_mixed_ref[0].astype(F32) * mixed_ref[0].astype(F32)
    high = product.astype(BF16)
    rest = (product - high.astype(F32)).astype(BF16)
    inner = three_parts(mm(high, pick) + mm(rest, pick), lane).astype(BF16)
    spare = spare_ref[0]
    zero = jnp.zeros((slot, LANES), BF16)
    for pair in range(width // LANES):
        at_query, at_key, at_value = pair_columns(pair, heads)
        query = qkv_ref[0, :, at_query : at_query + LANES]
        keys = qkv_ref[0, :, at_key : at_key + LANES]
        values = qkv_ref[0, :, at_value : at_value + LANES]
        grad = grad_mixed_ref[0, :, pair * LANES : (pair + 1) * LANES]
        total_query = jnp.zeros((slot, LANES), F32)
        total_key = jnp.zeros((slot, LANES), F32)
        total_value = jnp.zeros((slot, LANES), F32)
        for side in range(2):
            head = 2 * pair + side
            inside = (lane < HEAD_DIM) if side == 0 else (lane >= HEAD_DIM)
            mine = ((lane & 15) == head) & (lane < 48)
            query_side = jnp.where(inside, query, zero)
            key_side = jnp.where(inside, keys, zero)
            grad_side = jnp.where(inside, grad, zero)
            key_wide = jnp.concatenate([keys, jnp.where(mine, -1.0, key_flags).astype(BF16)], axis=1)
            value_wide = jnp.concatenate([values, jnp.where(mine, -1.0, 0.0).astype(BF16)], axis=1)
            probs = jnp.exp(mm_nt(key_wide, jnp.concatenate([query_side, spare], axis=1)))
            grad_probs = mm_nt(value_wide, jnp.concatenate([grad_side, inner], axis=1))
            grad_scores = (probs * grad_probs).astype(BF16)
            total_value += mm(probs.astype(BF16), grad_side)
            total_key += mm(grad_scores, query_side)
            total_query += mm_tn(grad_scores, key_side)
        grads_ref[0, :, at_query : at_query + LANES] = (total_query * 0.125).astype(BF16)
        grads_ref[0, :, at_key : at_key + LANES] = total_key.astype(BF16)
        grads_ref[0, :, at_value : at_value + LANES] = total_value.astype(BF16)

    update = 2.0 * mm_tn(low_ref[0], grads_ref[0])
    for half, ref in enumerate((adapter_own_ref, adapter_got_ref)):
        at = half * 3 * heads
        of_query = update[:, at : at + heads]
        of_value = update[:, at + 2 * heads : at + 3 * heads]
        part = jnp.concatenate(
            [
                of_query[:RANK] + of_query[LANES : LANES + RANK],
                of_value[RANK : 2 * RANK] + of_value[LANES + RANK : LANES + 2 * RANK],
            ],
            axis=0,
        )

        @pl.when(item == 0)
        def _(ref=ref, part=part):
            ref[...] = part

        @pl.when(item > 0)
        def _(ref=ref, part=part):
            ref[...] += part


def input_grad_kernel(layout, offsets, core_ref, *refs):
    n = len(layout)
    pieces = (refs[:n], refs[n : 2 * n])
    (
        grads_ref,
        grad_hidden_ref,
        up_own_ref,
        up_got_ref,
        own_ref,
        got_ref,
        weights,
        up,
        sems,
    ) = refs[2 * n :]
    slot, width = grad_hidden_ref.shape[1:]
    heads = width // 2

    @pl.when(pl.program_id(0) == 0)
    def _():
        copies = load_projections(layout, offsets, pieces, weights, sems.at[0], heads, (6 * heads, 6 * heads + LANES))
        start_all(copies)
        up[...] = jnp.zeros_like(up)
        up[: 2 * RANK] = ups((up_own_ref, up_got_ref), heads)
        wait_all(copies)

    grads = grads_ref[0]
    small = two_parts(mm_nt(grads, up[...]))
    total = grad_hidden_ref[0] + mm_nt(jnp.concatenate([grads, small], axis=1), weights[...])
    own_ref[0] = total[: slot // 2]
    got_ref[0] = total[slot // 2 :]


def any_spec():
    return pl.BlockSpec(memory_space=pl.ANY)


def whole_spec(array):
    return pl.BlockSpec(array.shape, lambda i, *_: (0,) * array.ndim)


def item_spec(shape):
    return pl.BlockSpec((1, *shape[1:]), lambda i, *_: (i, 0, 0))


def shape_of(shape, dtype):
    return jax.ShapeDtypeStruct(shape, dtype)


def call(kernel, name, scalars, flat, args, outs, scratch, items, flops, moved):
    return pl.pallas_call(
        kernel,
        grid_spec=pltpu.PrefetchScalarGridSpec(
            num_scalar_prefetch=len(scalars),
            grid=(items,),
            in_specs=[any_spec()] * len(flat) + [spec for _, spec in args],
            out_specs=[spec for _, spec in outs],
            scratch_shapes=scratch,
        ),
        out_shape=[shape for shape, _ in outs],
        compiler_params=pltpu.CompilerParams(vmem_limit_bytes=VMEM_LIMIT),
        cost_estimate=pl.CostEstimate(flops=flops, bytes_accessed=moved, transcendentals=0),
        name=name,
    )(*scalars, *flat, *[array for array, _ in args])


def swap(array):
    return lax.ppermute(array, "tensor", [(0, 1), (1, 0)])


def after(value, *deps):
    return lax.optimization_barrier((value, *deps))[0]


def over_dp(count, array, target):
    return lax.ppermute(array, "dp", [(i, target(i)) for i in range(count)])


LINE_FIRST = ((0, 1, 2, 3), (4, 5, 6, 7), (8, 9, 10, 11), (12, 13), (14, 15))
PLANE_FIRST = ((0, 4, 8, 12), (1, 5, 9, 13), (2, 6, 10, 14), (3, 7, 11, 15))


def ring_offsets(index, rows):
    flip = jnp.arange(16) // 4
    back = jnp.arange(16) % 4
    return (((index ^ flip) - 4 * back) % 16 * rows).astype(jnp.int32)


def local(
    inputs,
    lengths,
    bounds,
    query_matrix,
    key_matrix,
    value_matrix,
    query_value_bias,
    adapter_down_weight,
    adapter_up_weight,
    attention_output_weight,
    feedforward_input_weight,
    feedforward_input_bias,
    feedforward_output_weight,
    output_bias,
    layernorm_scale,
    layernorm_bias,
    output_gradient,
    *,
    count,
):
    micro, rows, width = inputs.shape
    mine = micro // 2
    slot = 2 * rows
    heads = width // 2
    core = lax.axis_index("tensor")
    shard_rows = query_matrix.shape[0]
    hidden = feedforward_input_weight.shape[1]
    last = hidden // 3
    first = hidden - last

    down = jnp.transpose(adapter_down_weight, (1, 0, 2)).reshape(shard_rows, 2 * RANK)
    down = jnp.pad(down, ((0, 0), (0, LANES - 2 * RANK)))
    shard = jnp.concatenate([query_matrix, key_matrix, value_matrix, down], axis=1)
    back = feedforward_output_weight.T
    shard_first = jnp.concatenate(
        [attention_output_weight.T, feedforward_input_weight[:, :first], back[:, :first]], axis=1
    )
    shard_last = jnp.concatenate([feedforward_input_weight[:, first:], back[:, first:]], axis=1)

    others = (1 - core) * mine
    x_got = swap(lax.dynamic_slice_in_dim(inputs, others, mine, 0))
    grad_got = swap(lax.dynamic_slice_in_dim(output_gradient, others, mine, 0))
    bias_got, hidden_bias_got, up_got = swap(query_value_bias), swap(feedforward_input_bias), swap(adapter_up_weight)

    if count == 16:
        offsets = ring_offsets(lax.axis_index("dp"), shard_rows)
        move = functools.partial(over_dp, count)

        def to_x(array):
            return move(array, lambda i: i ^ 1)

        def to_y(array):
            return move(array, lambda i: i ^ 2)

        def along_z(array):
            return [array] + [move(array, lambda i, d=d: (i + 4 * d) % 16) for d in (1, 2, 3)]

        def far(by_x, by_y):
            half = by_x.shape[0] // 2
            return [to_y(by_x[:half]), to_x(by_y[half:])]

        plane = [shard_last, to_x(shard_last), to_y(shard_last), move(shard_last, lambda i: i ^ 3)]
        line = jnp.concatenate(along_z(shard), axis=0)
        plane = jnp.concatenate(plane, axis=0)
        shard_first, plane = lax.optimization_barrier((shard_first, plane, line))[:2]
        near = [to_x(line), to_y(line)]
        line_first = jnp.concatenate(along_z(shard_first), axis=0)
        own = [line, *near, *far(*near)]
        line_first, plane = lax.optimization_barrier((line_first, plane, own[3], own[4]))[:2]
        own_last = along_z(plane)
        near_first = [to_x(line_first), to_y(line_first)]
        own_first = [line_first, *near_first, *far(*near_first)]
        layout, layout_last = LINE_FIRST, PLANE_FIRST
    else:
        offsets = jnp.zeros((2,), jnp.int32)
        layout = layout_last = ((0,),)
        own, own_first, own_last = (
            [lax.all_gather(s, "dp", axis=0, tiled=True)] for s in (shard, shard_first, shard_last)
        )
    pieces = (*own, *map(swap, own))
    pieces_feed = (*own_first, *map(swap, own_first), *own_last, *map(swap, own_last))

    first_item = core * mine
    my_lengths = lax.dynamic_slice_in_dim(lengths[:, 0], first_item, mine, 0)
    my_bounds = lax.dynamic_slice_in_dim(bounds[:, 0], first_item, mine, 0)
    core = core[None].astype(jnp.int32)

    blank = jnp.zeros((heads,), F32)
    ones = blank + 1
    both = [query_value_bias[0], blank, query_value_bias[1], bias_got[0], blank, bias_got[1]]
    scale = [ones * 0.125, ones, ones] * 2
    bias = jnp.stack([jnp.concatenate(both), jnp.concatenate(scale)])
    hidden_bias = jnp.concatenate(
        [
            feedforward_input_bias[:first],
            hidden_bias_got[:first],
            feedforward_input_bias[first:],
            hidden_bias_got[first:],
        ]
    )[None]

    own_block = pl.BlockSpec((1, rows, width), lambda i, *s: (s[-1][0] * mine + i, 0, 0))
    got_block = pl.BlockSpec((1, rows, width), lambda i, *_: (i, 0, 0))
    item = (mine, slot, width)
    wide = (mine, slot, 3 * width)

    def out_item(shape, dtype):
        return shape_of(shape, dtype), item_spec(shape)

    def in_item(array):
        return array, item_spec(array.shape)

    def in_whole(array):
        return array, whole_spec(array)

    split_out = lambda dtype: [(shape_of(inputs.shape, dtype), own_block), (shape_of((mine, rows, width), dtype), got_block)]

    tokens = mine * slot
    qkv, mixed, spare, low = call(
        functools.partial(project_attend_kernel, layout),
        "project_attend",
        (offsets, my_lengths, my_bounds, core),
        pieces,
        [(inputs, own_block), (x_got, got_block), in_whole(bias), in_whole(adapter_up_weight), in_whole(up_got)],
        [
            out_item(wide, BF16),
            out_item(item, BF16),
            out_item((mine, slot, LANES), BF16),
            out_item((mine, slot, 2 * LANES), BF16),
        ],
        [
            pltpu.VMEM((width + 2 * LANES, 3 * width), BF16),
            pltpu.VMEM((width, LANES), BF16),
            pltpu.SemaphoreType.DMA((2,)),
        ],
        mine,
        2 * tokens * width * (4 * width + 8 * slot),
        12 * tokens * width,
    )
    out, out_send, grad_hidden, grad_mixed = call(
        functools.partial(feed_kernel, (layout, layout_last), (first, last)),
        "feed",
        (offsets, core),
        pieces_feed,
        [
            (inputs, own_block),
            (x_got, got_block),
            in_item(mixed),
            (output_gradient, own_block),
            (grad_got, got_block),
            *map(in_whole, (hidden_bias, output_bias, layernorm_scale, layernorm_bias)),
        ],
        [*split_out(BF16), out_item(item, F32), out_item(item, BF16)],
        [
            pltpu.VMEM((width, width), BF16),
            pltpu.VMEM((width, 2 * hidden), BF16),
            pltpu.VMEM((width, 2 * hidden), BF16),
            pltpu.VMEM((slot, 2 * hidden), F32),
            pltpu.SemaphoreType.DMA((1,)),
        ],
        mine,
        4 * tokens * width * (width + 4 * hidden),
        8 * width * hidden,
    )
    adapter = (2 * RANK, heads)
    grads, adapter_own, adapter_got = call(
        attend_back_kernel,
        "attend_back",
        (my_lengths, my_bounds, core),
        (),
        [*map(in_item, (qkv, mixed, spare, low, grad_mixed))],
        [out_item(wide, BF16)] + [(shape_of(adapter, F32), pl.BlockSpec(adapter, lambda i, *_: (0, 0)))] * 2,
        [],
        mine,
        2 * tokens * width * 20 * slot,
        16 * tokens * width,
    )
    total, total_send = call(
        functools.partial(input_grad_kernel, layout),
        "input_grad",
        (offsets, core),
        pieces,
        [in_item(grads), in_item(grad_hidden), in_whole(adapter_up_weight), in_whole(up_got)],
        split_out(F32),
        [
            pltpu.VMEM((width, 3 * width + 2 * LANES), BF16),
            pltpu.VMEM((LANES, 3 * width), BF16),
            pltpu.SemaphoreType.DMA((1,)),
        ],
        mine,
        2 * tokens * width * 3 * width,
        12 * tokens * width,
    )
    adapter = adapter_own + swap(adapter_got)
    if count == 16:
        for step in (1, 2, 4, 8):
            adapter = adapter + over_dp(count, adapter, lambda i, step=step: i ^ step)
    else:
        adapter = lax.psum(adapter, "dp")
    result = lax.dynamic_update_slice_in_dim(out, swap(out_send), others, 0)
    input_grad = lax.dynamic_update_slice_in_dim(total, swap(total_send), others, 0)
    return result, input_grad, adapter.reshape(2, RANK, heads)


def solution(mesh):
    return jax.shard_map(
        functools.partial(local, count=mesh.shape["dp"]),
        mesh=mesh,
        in_specs=(
            P(None, ("dp", "tensor"), None),
            P(None, "dp"),
            P(None, "dp"),
            P("dp", "tensor"),
            P("dp", "tensor"),
            P("dp", "tensor"),
            P(None, "tensor"),
            P(None, "dp", None),
            P(None, None, "tensor"),
            P("tensor", "dp"),
            P("dp", "tensor"),
            P("tensor"),
            P("tensor", "dp"),
            P(),
            P(),
            P(),
            P(None, ("dp", "tensor"), None),
        ),
        out_specs=(
            P(None, ("dp", "tensor"), None),
            P(None, ("dp", "tensor"), None),
            P(None, None, "tensor"),
        ),
        check_vma=False,
    )
```

```python
import functools

import jax
import jax.numpy as jnp
from jax import lax
from jax.experimental import pallas as pl
from jax.experimental.pallas import tpu as pltpu
from jax.sharding import PartitionSpec as P

F32 = jnp.float32
BF16 = jnp.bfloat16
HEAD_DIM = 64
RANK = 8
LANES = 128
EPS = 1e-05
MASKED = -float(2**30)
SEG = 64
VMEM_LIMIT = 60 * 2**20

NT = (((1,), (1,)), ((), ()))
TN = (((0,), (0,)), ((), ()))


def mm(a, b):
    return jnp.dot(a, b, preferred_element_type=F32)


def mm_nt(a, b):
    return lax.dot_general(a, b, NT, preferred_element_type=F32)


def mm_tn(a, b):
    return lax.dot_general(a, b, TN, preferred_element_type=F32)


def iota(shape, dimension):
    return lax.broadcasted_iota(jnp.int32, shape, dimension)


def three_parts(value, lane):
    high = value.astype(BF16).astype(F32)
    rest = value - high
    middle = rest.astype(BF16).astype(F32)
    return jnp.where(lane < 16, high, jnp.where(lane < 32, middle, jnp.where(lane < 48, rest - middle, 0.0)))


def two_parts(value):
    high = value.astype(BF16)
    return jnp.concatenate([high, (value - high.astype(F32)).astype(BF16)], axis=1)


def weight_copies(layout, offsets, pieces, target, sem, columns):
    copies = []
    for half, first, width, to in columns:
        for ref, blocks in zip(pieces[half], layout, strict=True):
            rows = ref.shape[0] // len(blocks)
            for place, block in enumerate(blocks):
                start = offsets[block]
                if rows % 16 == 0:
                    start = pl.multiple_of(start, 16)
                copies.append(
                    pltpu.make_async_copy(
                        ref.at[pl.ds(place * rows, rows), pl.ds(first, width)],
                        target.at[pl.ds(start, rows), pl.ds(to, width)],
                        sem,
                    )
                )
    return copies


def start_all(copies):
    for copy in copies:
        copy.start()


def wait_all(copies):
    for copy in copies:
        copy.wait()


def places(core, shape, half_slot):
    row = iota(shape, 0)
    return jnp.where(row < half_slot, row + core * half_slot, row - core * half_slot)


def flags_of(core, length, bound, slot):
    lane = iota((slot, LANES), 1)
    place = places(core, (slot, LANES), slot // 2)
    second = place >= bound
    query = jnp.where(
        lane == SEG,
        jnp.where(second, 1.0, 0.0),
        jnp.where(lane == SEG + 1, jnp.where(second, 0.0, 1.0), jnp.where(lane == SEG + 2, 1.0, 0.0)),
    )
    key = jnp.where(
        lane == SEG,
        jnp.where(second, 0.0, MASKED),
        jnp.where(
            lane == SEG + 1,
            jnp.where(second, MASKED, 0.0),
            jnp.where((lane == SEG + 2) & (place >= length), MASKED, 0.0),
        ),
    )
    return lane, query, key


def pair_columns(pair, heads):
    per_half = heads // LANES
    base = (pair // per_half) * 3 * heads + (pair % per_half) * LANES
    return base, base + heads, base + 2 * heads


def load_projections(layout, offsets, pieces, weights, sem, heads, downs):
    wide = 3 * heads
    columns = [(0, 0, wide, 0), (1, 0, wide, wide)]
    columns += [(0, wide, LANES, to) for to in downs]
    return weight_copies(layout, offsets, pieces, weights, sem, columns)


def ups(up_refs, heads):
    blank = jnp.zeros((RANK, heads), BF16)
    parts = []
    for ref in up_refs:
        parts += [
            jnp.concatenate([ref[0] * 2, blank], axis=0),
            jnp.concatenate([blank, blank], axis=0),
            jnp.concatenate([blank, ref[1] * 2], axis=0),
        ]
    return jnp.concatenate(parts, axis=1)


def project_attend_kernel(layout, offsets, lengths, bounds, core_ref, *refs):
    n = len(layout)
    pieces = (refs[:n], refs[n : 2 * n])
    (
        x_own_ref,
        x_got_ref,
        bias_ref,
        up_own_ref,
        up_got_ref,
        qkv_ref,
        mixed_ref,
        spare_ref,
        low_ref,
        weights,
        down,
        sems,
    ) = refs[2 * n :]
    item = pl.program_id(0)
    core = core_ref[0]
    slot, width = mixed_ref.shape[1:]
    heads = width // 2

    @pl.when(item == 0)
    def _():
        wide = 3 * heads
        copies = weight_copies(layout, offsets, pieces, weights, sems.at[0], [(0, 0, wide, 0), (1, 0, wide, wide)])
        downs = weight_copies(layout, offsets, pieces, down, sems.at[1], [(0, wide, LANES, 0)])
        start_all(downs)
        start_all(copies)
        weights[width:] = jnp.zeros((2 * LANES, 6 * heads), BF16)
        up = ups((up_own_ref, up_got_ref), heads)
        weights[width : width + 2 * RANK] = up
        weights[width + LANES : width + LANES + 2 * RANK] = up
        wait_all(downs)
        wait_all(copies)

    x = jnp.concatenate([x_own_ref[0], x_got_ref[0]], axis=0)
    low = two_parts(mm(x, down[...]))
    low_ref[0] = low
    wide_x = jnp.concatenate([x, low], axis=1)
    for part in range(3):
        at = slice(part * width, (part + 1) * width)
        out = (mm(wide_x, weights[:, at]) + bias_ref[0:1, at]) * bias_ref[1:2, at]
        qkv_ref[0, :, at] = out.astype(BF16)

    lane, query_flags, key_flags = flags_of(core, lengths[item], bounds[item], slot)
    query_low = query_flags.astype(BF16)
    key_low = key_flags.astype(BF16)
    ones = jnp.where(lane == 0, 1.0, 0.0).astype(BF16)
    zero = jnp.zeros((slot, LANES), BF16)
    totals = jnp.ones((slot, LANES), F32)
    peaks = []
    for pair in range(width // LANES):
        at_query, at_key, at_value = pair_columns(pair, heads)
        query = qkv_ref[0, :, at_query : at_query + LANES]
        keys = jnp.concatenate([qkv_ref[0, :, at_key : at_key + LANES], key_low], axis=1)
        values = jnp.concatenate([qkv_ref[0, :, at_value : at_value + LANES], ones], axis=1)
        outs = []
        for side in range(2):
            inside = (lane < HEAD_DIM) if side == 0 else (lane >= HEAD_DIM)
            query_side = jnp.concatenate([jnp.where(inside, query, zero), query_low], axis=1)
            scores = mm_nt(keys, query_side)
            peak = jnp.max(scores, axis=0, keepdims=True)
            probs = jnp.exp(scores - peak).astype(BF16)
            out = mm_tn(probs, values)
            total = out[:, LANES : LANES + 1]
            outs.append(out[:, :LANES] * (1.0 / total))
            totals = jnp.where((lane & 15) == 2 * pair + side, total, totals)
            peaks.append(peak)
        mixed_ref[0, :, pair * LANES : (pair + 1) * LANES] = jnp.where(
            lane < HEAD_DIM, outs[0], outs[1]
        ).astype(BF16)
    peaks += [jnp.zeros((1, slot), F32)] * (16 - len(peaks))
    peaks = jnp.concatenate(peaks, axis=0)
    peaks = jnp.concatenate([peaks] * (LANES // 16), axis=0).T
    spare_ref[0] = (three_parts(peaks + jnp.log(totals), lane) + query_flags).astype(BF16)


def row_mean(value):
    return jnp.mean(value, axis=-1, keepdims=True)


def normalize(value):
    centre = value - row_mean(value)
    scale = lax.rsqrt(row_mean(centre * centre) + EPS)
    return centre * scale, scale


def normalize_back(grad, gain, normal, scale):
    grad = grad * gain
    return scale * (grad - row_mean(grad) - normal * row_mean(grad * normal))


def feed_kernel(layouts, chunks, offsets, core_ref, *refs):
    n, m = map(len, layouts)
    pieces = (refs[:n], refs[n : 2 * n])
    pieces_last = (refs[2 * n : 2 * n + m], refs[2 * n + m : 2 * n + 2 * m])
    (
        x_own_ref,
        x_got_ref,
        mixed_ref,
        grad_own_ref,
        grad_got_ref,
        hidden_bias_ref,
        output_bias_ref,
        gain_ref,
        shift_ref,
        out_own_ref,
        out_got_ref,
        grad_hidden_ref,
        grad_mixed_ref,
        out_weights,
        in_weights,
        back_weights,
        slope,
        sems,
    ) = refs[2 * (n + m) :]
    slot, width = mixed_ref.shape[1:]
    half_slot = slot // 2
    heads = width // 2
    first, last = chunks
    size = width
    parts = list(range(0, 2 * (first + last), size))

    o = heads
    tail = 2 * first
    groups = [
        weight_copies(layouts[0], offsets, pieces, out_weights, sems.at[0], [(0, 0, o, 0), (1, 0, o, o)]),
        weight_copies(layouts[0], offsets, pieces, in_weights, sems.at[1], [(0, o, first, 0), (1, o, first, first)]),
        weight_copies(
            layouts[0], offsets, pieces, back_weights, sems.at[2], [(0, o + first, first, 0), (1, o + first, first, first)]
        ),
        weight_copies(
            layouts[1], offsets, pieces_last, in_weights, sems.at[3], [(0, 0, last, tail), (1, 0, last, tail + last)]
        ),
        weight_copies(
            layouts[1], offsets, pieces_last, back_weights, sems.at[4], [(0, last, last, tail), (1, last, last, tail + last)]
        ),
    ]

    @pl.when(pl.program_id(0) == 0)
    def _():
        for group in groups:
            start_all(group)

    def arrived(*which):
        @pl.when(pl.program_id(0) == 0)
        def _():
            for index in which:
                wait_all(groups[index])

    arrived(0)
    x = jnp.concatenate([x_own_ref[0], x_got_ref[0]], axis=0).astype(F32)
    summed = x + output_bias_ref[0:1] + mm_nt(mixed_ref[0], out_weights[...])
    normal_in, scale_in = normalize(summed)
    normed = normal_in * gain_ref[0:1] + shift_ref[0:1]
    normed_low = normed.astype(BF16)
    total = normed + output_bias_ref[1:2]
    for at in parts:
        if at == 0:
            arrived(1)
        if at < tail < at + size or at == tail:
            arrived(3)
        pre = mm(normed_low, in_weights[:, at : at + size]) + hidden_bias_ref[:, at : at + size]
        share = 0.5 * (1.0 + lax.erf(pre * 0.7071067811865476))
        slope[:, at : at + size] = share + pre * jnp.exp(-0.5 * pre * pre) * 0.3989422804014327
        if at == 0:
            arrived(2)
        if at < tail < at + size or at == tail:
            arrived(4)
        total += mm_nt((pre * share).astype(BF16), back_weights[:, at : at + size])
    normal_out, scale_out = normalize(total)
    out = (normal_out * gain_ref[1:2] + shift_ref[1:2]).astype(BF16)
    out_own_ref[0] = out[:half_slot]
    out_got_ref[0] = out[half_slot:]
    grad = jnp.concatenate([grad_own_ref[0], grad_got_ref[0]], axis=0).astype(F32)
    grad_total = normalize_back(grad, gain_ref[1:2], normal_out, scale_out)
    grad_low = grad_total.astype(BF16)
    grad_normed = grad_total
    for at in parts:
        grad_pre = (mm(grad_low, back_weights[:, at : at + size]) * slope[:, at : at + size]).astype(BF16)
        grad_normed += mm_nt(grad_pre, in_weights[:, at : at + size])
    grad_hidden = normalize_back(grad_normed, gain_ref[0:1], normal_in, scale_in)
    grad_hidden_ref[0] = grad_hidden
    grad_mixed_ref[0] = mm(grad_hidden.astype(BF16), out_weights[...]).astype(BF16)


def attend_back_kernel(lengths, bounds, core_ref, *refs):
    (
        qkv_ref,
        mixed_ref,
        spare_ref,
        low_ref,
        grad_mixed_ref,
        grads_ref,
        adapter_own_ref,
        adapter_got_ref,
    ) = refs
    item = pl.program_id(0)
    core = core_ref[0]
    slot, width = mixed_ref.shape[1:]
    heads = width // 2

    lane, _, key_flags = flags_of(core, lengths[item], bounds[item], slot)
    row = iota((width, LANES), 0)
    column = iota((width, LANES), 1)
    pick = jnp.where((row // HEAD_DIM == (column & 15)) & (column < 48), 1.0, 0.0).astype(BF16)
    product = grad_mixed_ref[0].astype(F32) * mixed_ref[0].astype(F32)
    high = product.astype(BF16)
    rest = (product - high.astype(F32)).astype(BF16)
    inner = three_parts(mm(high, pick) + mm(rest, pick), lane).astype(BF16)
    spare = spare_ref[0]
    zero = jnp.zeros((slot, LANES), BF16)
    for pair in range(width // LANES):
        at_query, at_key, at_value = pair_columns(pair, heads)
        query = qkv_ref[0, :, at_query : at_query + LANES]
        keys = qkv_ref[0, :, at_key : at_key + LANES]
        values = qkv_ref[0, :, at_value : at_value + LANES]
        grad = grad_mixed_ref[0, :, pair * LANES : (pair + 1) * LANES]
        total_query = jnp.zeros((slot, LANES), F32)
        total_key = jnp.zeros((slot, LANES), F32)
        total_value = jnp.zeros((slot, LANES), F32)
        for side in range(2):
            head = 2 * pair + side
            inside = (lane < HEAD_DIM) if side == 0 else (lane >= HEAD_DIM)
            mine = ((lane & 15) == head) & (lane < 48)
            query_side = jnp.where(inside, query, zero)
            key_side = jnp.where(inside, keys, zero)
            grad_side = jnp.where(inside, grad, zero)
            key_wide = jnp.concatenate([keys, jnp.where(mine, -1.0, key_flags).astype(BF16)], axis=1)
            value_wide = jnp.concatenate([values, jnp.where(mine, -1.0, 0.0).astype(BF16)], axis=1)
            probs = jnp.exp(mm_nt(key_wide, jnp.concatenate([query_side, spare], axis=1)))
            grad_probs = mm_nt(value_wide, jnp.concatenate([grad_side, inner], axis=1))
            grad_scores = (probs * grad_probs).astype(BF16)
            total_value += mm(probs.astype(BF16), grad_side)
            total_key += mm(grad_scores, query_side)
            total_query += mm_tn(grad_scores, key_side)
        grads_ref[0, :, at_query : at_query + LANES] = (total_query * 0.125).astype(BF16)
        grads_ref[0, :, at_key : at_key + LANES] = total_key.astype(BF16)
        grads_ref[0, :, at_value : at_value + LANES] = total_value.astype(BF16)

    update = 2.0 * mm_tn(low_ref[0], grads_ref[0])
    for half, ref in enumerate((adapter_own_ref, adapter_got_ref)):
        at = half * 3 * heads
        of_query = update[:, at : at + heads]
        of_value = update[:, at + 2 * heads : at + 3 * heads]
        part = jnp.concatenate(
            [
                of_query[:RANK] + of_query[LANES : LANES + RANK],
                of_value[RANK : 2 * RANK] + of_value[LANES + RANK : LANES + 2 * RANK],
            ],
            axis=0,
        )

        @pl.when(item == 0)
        def _(ref=ref, part=part):
            ref[...] = part

        @pl.when(item > 0)
        def _(ref=ref, part=part):
            ref[...] += part


def input_grad_kernel(layout, offsets, core_ref, *refs):
    n = len(layout)
    pieces = (refs[:n], refs[n : 2 * n])
    (
        grads_ref,
        grad_hidden_ref,
        up_own_ref,
        up_got_ref,
        _,
        own_ref,
        got_ref,
        weights,
        up,
        sems,
    ) = refs[2 * n :]
    slot, width = grad_hidden_ref.shape[1:]
    heads = width // 2
    copies = load_projections(layout, offsets, pieces, weights, sems.at[0], heads, (6 * heads, 6 * heads + LANES))
    start_all(copies)
    up[...] = jnp.zeros_like(up)
    up[: 2 * RANK] = ups((up_own_ref, up_got_ref), heads)
    grads = grads_ref[0]
    small = two_parts(mm_nt(grads, up[...]))
    wait_all(copies)
    total = grad_hidden_ref[0] + mm_nt(jnp.concatenate([grads, small], axis=1), weights[...])
    own_ref[0] = total[: slot // 2]
    got_ref[0] = total[slot // 2 :]


def any_spec():
    return pl.BlockSpec(memory_space=pl.ANY)


def whole_spec(array):
    return pl.BlockSpec(array.shape, lambda i, *_: (0,) * array.ndim)


def item_spec(shape):
    return pl.BlockSpec((1, *shape[1:]), lambda i, *_: (i, 0, 0))


def shape_of(shape, dtype):
    return jax.ShapeDtypeStruct(shape, dtype)


def call(kernel, name, scalars, flat, args, outs, scratch, items, flops, moved, aliases=None):
    return pl.pallas_call(
        kernel,
        grid_spec=pltpu.PrefetchScalarGridSpec(
            num_scalar_prefetch=len(scalars),
            grid=(items,),
            in_specs=[any_spec()] * len(flat) + [spec for _, spec in args],
            out_specs=[spec for _, spec in outs],
            scratch_shapes=scratch,
        ),
        out_shape=[shape for shape, _ in outs],
        compiler_params=pltpu.CompilerParams(vmem_limit_bytes=VMEM_LIMIT),
        cost_estimate=pl.CostEstimate(flops=flops, bytes_accessed=moved, transcendentals=0),
        name=name,
        input_output_aliases=aliases or {},
    )(*scalars, *flat, *[array for array, _ in args])


def swap(array):
    return lax.ppermute(array, "tensor", [(0, 1), (1, 0)])


def after(value, *deps):
    return lax.optimization_barrier((value, *deps))[0]


def over_dp(count, array, target):
    return lax.ppermute(array, "dp", [(i, target(i)) for i in range(count)])


LINE_FIRST = ((0, 1, 2, 3), (4, 5, 6, 7), (8, 9, 10, 11), (12, 13), (14, 15))
PLANE_FIRST = ((0, 4, 8, 12), (1, 5, 9, 13), (2, 6, 10, 14), (3, 7, 11, 15))


def ring_offsets(index, rows):
    flip = jnp.arange(16) // 4
    back = jnp.arange(16) % 4
    return (((index ^ flip) - 4 * back) % 16 * rows).astype(jnp.int32)


def local(
    inputs,
    lengths,
    bounds,
    query_matrix,
    key_matrix,
    value_matrix,
    query_value_bias,
    adapter_down_weight,
    adapter_up_weight,
    attention_output_weight,
    feedforward_input_weight,
    feedforward_input_bias,
    feedforward_output_weight,
    output_bias,
    layernorm_scale,
    layernorm_bias,
    output_gradient,
    *,
    count,
):
    micro, rows, width = inputs.shape
    mine = micro // 2
    slot = 2 * rows
    heads = width // 2
    core = lax.axis_index("tensor")
    shard_rows = query_matrix.shape[0]
    hidden = feedforward_input_weight.shape[1]
    last = hidden // 3
    first = hidden - last

    down = jnp.transpose(adapter_down_weight, (1, 0, 2)).reshape(shard_rows, 2 * RANK)
    down = jnp.pad(down, ((0, 0), (0, LANES - 2 * RANK)))
    shard = jnp.concatenate([query_matrix, key_matrix, value_matrix, down], axis=1)
    back = feedforward_output_weight.T
    shard_first = jnp.concatenate(
        [attention_output_weight.T, feedforward_input_weight[:, :first], back[:, :first]], axis=1
    )
    shard_last = jnp.concatenate([feedforward_input_weight[:, first:], back[:, first:]], axis=1)

    others = (1 - core) * mine
    x_got = swap(lax.dynamic_slice_in_dim(inputs, others, mine, 0))
    bias_got, up_got = swap(query_value_bias), swap(adapter_up_weight)

    if count == 16:
        offsets = ring_offsets(lax.axis_index("dp"), shard_rows)
        move = functools.partial(over_dp, count)

        def to_x(array):
            return move(array, lambda i: i ^ 1)

        def to_y(array):
            return move(array, lambda i: i ^ 2)

        def z_move(array, planes):
            return move(array, lambda i: (i + 4 * planes) % 16)

        def along_z(array):
            return [array] + [z_move(array, planes) for planes in (1, 2, 3)]

        def far_halves(by_x, by_y):
            half = by_x.shape[0] // 2
            return by_x[:half], by_y[half:]

        def far_moves(low, high):
            return [to_y(low), to_x(high)]

        plane = [shard_last, to_x(shard_last), to_y(shard_last), move(shard_last, lambda i: i ^ 3)]
        line = jnp.concatenate(along_z(shard), axis=0)
        line, x_got, bias_got, up_got = lax.optimization_barrier((line, x_got, bias_got, up_got))
        plane = jnp.concatenate(plane, axis=0)
        shard_first, plane = lax.optimization_barrier((shard_first, plane, line))[:2]
        by = [to_x(line), to_y(line)]
        own = [line, *by, *far_moves(*far_halves(*by))]
        swapped = [swap(piece) for piece in own]
        ahead, behind = z_move(shard_first, 1), z_move(shard_first, 3)
        across = z_move(after(shard_first, *by), 2)
        line_first = jnp.concatenate([shard_first, ahead, across, behind], axis=0)
        line_first = after(line_first, *own[3:])
        own_last = along_z(after(plane, line_first, *swapped))
        by_first = [to_x(line_first), to_y(line_first)]
        own_first = [line_first, *by_first]
        layout, layout_last = LINE_FIRST, PLANE_FIRST
    else:
        offsets = jnp.zeros((2,), jnp.int32)
        layout = layout_last = ((0,),)
        own, own_first, own_last = (
            [lax.all_gather(s, "dp", axis=0, tiled=True)] for s in (shard, shard_first, shard_last)
        )
        swapped = [swap(piece) for piece in own]
    pieces = (*own, *swapped)

    first_item = core * mine
    my_lengths = lax.dynamic_slice_in_dim(lengths[:, 0], first_item, mine, 0)
    my_bounds = lax.dynamic_slice_in_dim(bounds[:, 0], first_item, mine, 0)
    core = core[None].astype(jnp.int32)

    blank = jnp.zeros((heads,), F32)
    ones = blank + 1
    both = [query_value_bias[0], blank, query_value_bias[1], bias_got[0], blank, bias_got[1]]
    scale = [ones * 0.125, ones, ones] * 2
    bias = jnp.stack([jnp.concatenate(both), jnp.concatenate(scale)])
    own_block = pl.BlockSpec((1, rows, width), lambda i, *s: (s[-1][0] * mine + i, 0, 0))
    got_block = pl.BlockSpec((1, rows, width), lambda i, *_: (i, 0, 0))
    item = (mine, slot, width)
    wide = (mine, slot, 3 * width)

    def out_item(shape, dtype):
        return shape_of(shape, dtype), item_spec(shape)

    def in_item(array):
        return array, item_spec(array.shape)

    def in_whole(array):
        return array, whole_spec(array)

    split_out = lambda dtype: [(shape_of(inputs.shape, dtype), own_block), (shape_of((mine, rows, width), dtype), got_block)]

    tokens = mine * slot
    qkv, mixed, spare, low = call(
        functools.partial(project_attend_kernel, layout),
        "project_attend",
        (offsets, my_lengths, my_bounds, core),
        pieces,
        [(inputs, own_block), (x_got, got_block), in_whole(bias), in_whole(adapter_up_weight), in_whole(up_got)],
        [
            out_item(wide, BF16),
            out_item(item, BF16),
            out_item((mine, slot, LANES), BF16),
            out_item((mine, slot, 2 * LANES), BF16),
        ],
        [
            pltpu.VMEM((width + 2 * LANES, 3 * width), BF16),
            pltpu.VMEM((width, LANES), BF16),
            pltpu.SemaphoreType.DMA((2,)),
        ],
        mine,
        2 * tokens * width * (4 * width + 8 * slot),
        12 * tokens * width,
    )
    own_first, own_last, grad, hidden_bias_own = lax.optimization_barrier(
        (own_first, own_last, output_gradient, feedforward_input_bias, mixed)
    )[:4]
    if count == 16:
        ends = far_halves(*own_first[1:])
        own_first, own_last, ends, grad, hidden_bias_own = lax.optimization_barrier(
            (own_first, own_last, ends, grad, hidden_bias_own)
        )
        own_first += far_moves(*ends)
    grad_got = swap(lax.dynamic_slice_in_dim(grad, others, mine, 0))
    hidden_bias_got = swap(hidden_bias_own)
    hidden_bias = jnp.concatenate(
        [
            feedforward_input_bias[:first],
            hidden_bias_got[:first],
            feedforward_input_bias[first:],
            hidden_bias_got[first:],
        ]
    )[None]
    pieces_feed = (*own_first, *map(swap, own_first), *own_last, *map(swap, own_last))
    out, out_send, grad_hidden, grad_mixed = call(
        functools.partial(feed_kernel, (layout, layout_last), (first, last)),
        "feed",
        (offsets, core),
        pieces_feed,
        [
            (inputs, own_block),
            (x_got, got_block),
            in_item(mixed),
            (output_gradient, own_block),
            (grad_got, got_block),
            *map(in_whole, (hidden_bias, output_bias, layernorm_scale, layernorm_bias)),
        ],
        [*split_out(BF16), out_item(item, F32), out_item(item, BF16)],
        [
            pltpu.VMEM((width, width), BF16),
            pltpu.VMEM((width, 2 * hidden), BF16),
            pltpu.VMEM((width, 2 * hidden), BF16),
            pltpu.VMEM((slot, 2 * hidden), F32),
            pltpu.SemaphoreType.DMA((5,)),
        ],
        mine,
        4 * tokens * width * (width + 4 * hidden),
        8 * width * hidden,
    )
    adapter = (2 * RANK, heads)
    grads, adapter_own, adapter_got = call(
        attend_back_kernel,
        "attend_back",
        (my_lengths, my_bounds, core),
        (),
        [*map(in_item, (qkv, mixed, spare, low, grad_mixed))],
        [out_item(wide, BF16)] + [(shape_of(adapter, F32), pl.BlockSpec(adapter, lambda i, *_: (0, 0)))] * 2,
        [],
        mine,
        2 * tokens * width * 20 * slot,
        16 * tokens * width,
    )
    def input_grad_of(index, total, grads):
        at = pl.BlockSpec((1, slot, width), lambda i, *_: (index, 0, 0))
        at_wide = pl.BlockSpec((1, slot, 3 * width), lambda i, *_: (index, 0, 0))
        own_at = pl.BlockSpec((1, rows, width), lambda i, *r: (r[-1][0] * mine + index, 0, 0))
        args = [
            (grads, at_wide),
            (grad_hidden, at),
            in_whole(adapter_up_weight),
            in_whole(up_got),
            (total, any_spec()),
        ]
        return call(
            functools.partial(input_grad_kernel, layout),
            "input_grad",
            (offsets, core),
            pieces,
            args,
            [(shape_of(inputs.shape, F32), own_at), (shape_of((1, rows, width), F32), got_block)],
            [
                pltpu.VMEM((width, 3 * width + 2 * LANES), BF16),
                pltpu.VMEM((LANES, 3 * width), BF16),
                pltpu.SemaphoreType.DMA((1,)),
            ],
            1,
            2 * slot * width * 3 * width,
            12 * slot * width,
            {2 + len(pieces) + 4: 0},
        )

    total = jnp.zeros(inputs.shape, F32)
    sends = []
    adapter = adapter_own + swap(adapter_got)
    if count == 16:
        total, send = input_grad_of(0, total, grads)
        sends.append(swap(send))
        adapter = after(adapter, total)
        adapter = (adapter + to_x(adapter)) + (to_y(adapter) + move(adapter, lambda i: i ^ 3))
        grads_last = after(grads, total)
        total, send = input_grad_of(1, total, grads_last)
        sends.append(swap(send))
        adapter = after(adapter, total)
        ways = along_z(adapter)
        adapter = (ways[0] + ways[1]) + (ways[2] + ways[3])
    else:
        adapter = lax.psum(adapter, "dp")
        for index in range(mine):
            total, send = input_grad_of(index, total, grads)
            sends.append(swap(send))
    result = lax.dynamic_update_slice_in_dim(out, swap(out_send), others, 0)
    input_grad = total
    for index, send in enumerate(sends):
        input_grad = lax.dynamic_update_slice_in_dim(input_grad, send, others + index, 0)
    return result, input_grad, adapter.reshape(2, RANK, heads)


def solution(mesh):
    return jax.shard_map(
        functools.partial(local, count=mesh.shape["dp"]),
        mesh=mesh,
        in_specs=(
            P(None, ("dp", "tensor"), None),
            P(None, "dp"),
            P(None, "dp"),
            P("dp", "tensor"),
            P("dp", "tensor"),
            P("dp", "tensor"),
            P(None, "tensor"),
            P(None, "dp", None),
            P(None, None, "tensor"),
            P("tensor", "dp"),
            P("dp", "tensor"),
            P("tensor"),
            P("tensor", "dp"),
            P(),
            P(),
            P(),
            P(None, ("dp", "tensor"), None),
        ),
        out_specs=(
            P(None, ("dp", "tensor"), None),
            P(None, ("dp", "tensor"), None),
            P(None, None, "tensor"),
        ),
        check_vma=False,
    )
```

```python
import functools

import jax
import jax.numpy as jnp
from jax import lax
from jax.experimental import pallas as pl
from jax.experimental.pallas import tpu as pltpu
from jax.sharding import PartitionSpec as P

F32 = jnp.float32
BF16 = jnp.bfloat16
HEAD_DIM = 64
RANK = 8
LANES = 128
EPS = 1e-05
MASKED = -float(2**30)
SEG = 64
VMEM_LIMIT = 60 * 2**20

NT = (((1,), (1,)), ((), ()))
TN = (((0,), (0,)), ((), ()))


def mm(a, b):
    return jnp.dot(a, b, preferred_element_type=F32)


def mm_nt(a, b):
    return lax.dot_general(a, b, NT, preferred_element_type=F32)


def mm_tn(a, b):
    return lax.dot_general(a, b, TN, preferred_element_type=F32)


def iota(shape, dimension):
    return lax.broadcasted_iota(jnp.int32, shape, dimension)


def three_parts(value, lane):
    high = value.astype(BF16).astype(F32)
    rest = value - high
    middle = rest.astype(BF16).astype(F32)
    return jnp.where(lane < 16, high, jnp.where(lane < 32, middle, jnp.where(lane < 48, rest - middle, 0.0)))


def two_parts(value):
    high = value.astype(BF16)
    return jnp.concatenate([high, (value - high.astype(F32)).astype(BF16)], axis=1)


def weight_copies(order, offsets, pieces, target, sem, columns):
    firsts, blocks = order
    copies, waits = [], []
    for half, first, width, to in columns:
        for index, ref in enumerate(pieces[half]):
            rows = ref.shape[0] // blocks
            for place in range(blocks):
                start = offsets[firsts[half] + index * blocks + place]
                if rows % 16 == 0:
                    start = pl.multiple_of(start, 16)
                copies.append(
                    pltpu.make_async_copy(
                        ref.at[pl.ds(place * rows, rows), pl.ds(first, width)],
                        target.at[pl.ds(start, rows), pl.ds(to, width)],
                        sem,
                    )
                )
        filled = target.at[pl.ds(0, sum(ref.shape[0] for ref in pieces[half])), pl.ds(to, width)]
        waits.append(pltpu.make_async_copy(filled, filled, sem))
    return copies, waits


def start_all(group):
    for copy in group[0]:
        copy.start()


def wait_all(group):
    for copy in group[1]:
        copy.wait()


def places(core, shape, half_slot):
    row = iota(shape, 0)
    return jnp.where(row < half_slot, row + core * half_slot, row - core * half_slot)


def flags_of(core, length, bound, slot):
    lane = iota((slot, LANES), 1)
    place = places(core, (slot, LANES), slot // 2)
    second = place >= bound
    query = jnp.where(
        lane == SEG,
        jnp.where(second, 1.0, 0.0),
        jnp.where(lane == SEG + 1, jnp.where(second, 0.0, 1.0), jnp.where(lane == SEG + 2, 1.0, 0.0)),
    )
    key = jnp.where(
        lane == SEG,
        jnp.where(second, 0.0, MASKED),
        jnp.where(
            lane == SEG + 1,
            jnp.where(second, MASKED, 0.0),
            jnp.where((lane == SEG + 2) & (place >= length), MASKED, 0.0),
        ),
    )
    return lane, query, key


def pair_columns(pair, heads):
    per_half = heads // LANES
    base = (pair // per_half) * 3 * heads + (pair % per_half) * LANES
    return base, base + heads, base + 2 * heads


def load_projections(order, offsets, pieces, weights, sem, heads, downs):
    wide = 3 * heads
    columns = [(0, 0, wide, 0), (1, 0, wide, wide)]
    columns += [(0, wide, LANES, to) for to in downs]
    return weight_copies(order, offsets, pieces, weights, sem, columns)


def ups(up_refs, heads):
    blank = jnp.zeros((RANK, heads), BF16)
    parts = []
    for ref in up_refs:
        parts += [
            jnp.concatenate([ref[0] * 2, blank], axis=0),
            jnp.concatenate([blank, blank], axis=0),
            jnp.concatenate([blank, ref[1] * 2], axis=0),
        ]
    return jnp.concatenate(parts, axis=1)


def project_attend_kernel(order, n, offsets, lengths, bounds, core_ref, *refs):
    pieces = (refs[:n], refs[n : 2 * n])
    (
        x_own_ref,
        x_got_ref,
        bias_ref,
        up_own_ref,
        up_got_ref,
        qkv_ref,
        mixed_ref,
        spare_ref,
        low_ref,
        weights,
        down,
        sems,
    ) = refs[2 * n :]
    item = pl.program_id(0)
    core = core_ref[0]
    slot, width = mixed_ref.shape[1:]
    heads = width // 2

    @pl.when(item == 0)
    def _():
        wide = 3 * heads
        copies = weight_copies(order, offsets, pieces, weights, sems.at[0], [(0, 0, wide, 0), (1, 0, wide, wide)])
        downs = weight_copies(order, offsets, pieces, down, sems.at[1], [(0, wide, LANES, 0)])
        start_all(downs)
        start_all(copies)
        weights[width:] = jnp.zeros((2 * LANES, 6 * heads), BF16)
        up = ups((up_own_ref, up_got_ref), heads)
        weights[width : width + 2 * RANK] = up
        weights[width + LANES : width + LANES + 2 * RANK] = up
        wait_all(downs)
        wait_all(copies)

    x = jnp.concatenate([x_own_ref[0], x_got_ref[0]], axis=0)
    low = two_parts(mm(x, down[...]))
    low_ref[0] = low
    wide_x = jnp.concatenate([x, low], axis=1)
    for part in range(3):
        at = slice(part * width, (part + 1) * width)
        out = (mm(wide_x, weights[:, at]) + bias_ref[0:1, at]) * bias_ref[1:2, at]
        qkv_ref[0, :, at] = out.astype(BF16)

    lane, query_flags, key_flags = flags_of(core, lengths[item], bounds[item], slot)
    query_low = query_flags.astype(BF16)
    key_low = key_flags.astype(BF16)
    ones = jnp.where(lane == 0, 1.0, 0.0).astype(BF16)
    zero = jnp.zeros((slot, LANES), BF16)
    totals = jnp.ones((slot, LANES), F32)
    peaks = []
    for pair in range(width // LANES):
        at_query, at_key, at_value = pair_columns(pair, heads)
        query = qkv_ref[0, :, at_query : at_query + LANES]
        keys = jnp.concatenate([qkv_ref[0, :, at_key : at_key + LANES], key_low], axis=1)
        values = jnp.concatenate([qkv_ref[0, :, at_value : at_value + LANES], ones], axis=1)
        outs = []
        for side in range(2):
            inside = (lane < HEAD_DIM) if side == 0 else (lane >= HEAD_DIM)
            query_side = jnp.concatenate([jnp.where(inside, query, zero), query_low], axis=1)
            scores = mm_nt(keys, query_side)
            peak = jnp.max(scores, axis=0, keepdims=True)
            probs = jnp.exp(scores - peak).astype(BF16)
            out = mm_tn(probs, values)
            total = out[:, LANES : LANES + 1]
            outs.append(out[:, :LANES] * (1.0 / total))
            totals = jnp.where((lane & 15) == 2 * pair + side, total, totals)
            peaks.append(peak)
        mixed_ref[0, :, pair * LANES : (pair + 1) * LANES] = jnp.where(
            lane < HEAD_DIM, outs[0], outs[1]
        ).astype(BF16)
    peaks += [jnp.zeros((1, slot), F32)] * (16 - len(peaks))
    peaks = jnp.concatenate(peaks, axis=0)
    peaks = jnp.concatenate([peaks] * (LANES // 16), axis=0).T
    spare_ref[0] = (three_parts(peaks + jnp.log(totals), lane) + query_flags).astype(BF16)


def row_mean(value):
    return jnp.mean(value, axis=-1, keepdims=True)


def normalize(value):
    centre = value - row_mean(value)
    scale = lax.rsqrt(row_mean(centre * centre) + EPS)
    return centre * scale, scale


def normalize_back(grad, gain, normal, scale):
    grad = grad * gain
    return scale * (grad - row_mean(grad) - normal * row_mean(grad * normal))


def feed_kernel(orders, chunks, n, offsets, core_ref, *refs):
    pieces = (refs[:n], refs[n : 2 * n])
    pieces_last = (refs[2 * n : 3 * n], refs[3 * n : 4 * n])
    (
        x_own_ref,
        x_got_ref,
        mixed_ref,
        grad_own_ref,
        grad_got_ref,
        hidden_bias_ref,
        output_bias_ref,
        gain_ref,
        shift_ref,
        out_own_ref,
        out_got_ref,
        grad_hidden_ref,
        grad_mixed_ref,
        out_weights,
        in_weights,
        back_weights,
        slope,
        sems,
    ) = refs[4 * n :]
    slot, width = mixed_ref.shape[1:]
    half_slot = slot // 2
    heads = width // 2
    first, last = chunks
    size = width
    parts = list(range(0, 2 * (first + last), size))

    o = heads
    tail = 2 * first
    groups = [
        weight_copies(orders[0], offsets, pieces, out_weights, sems.at[0], [(0, 0, o, 0), (1, 0, o, o)]),
        weight_copies(orders[0], offsets, pieces, in_weights, sems.at[1], [(0, o, first, 0), (1, o, first, first)]),
        weight_copies(
            orders[0], offsets, pieces, back_weights, sems.at[2], [(0, o + first, first, 0), (1, o + first, first, first)]
        ),
        weight_copies(
            orders[1], offsets, pieces_last, in_weights, sems.at[3], [(0, 0, last, tail), (1, 0, last, tail + last)]
        ),
        weight_copies(
            orders[1], offsets, pieces_last, back_weights, sems.at[4], [(0, last, last, tail), (1, last, last, tail + last)]
        ),
    ]

    @pl.when(pl.program_id(0) == 0)
    def _():
        for group in groups:
            start_all(group)

    def arrived(*which):
        @pl.when(pl.program_id(0) == 0)
        def _():
            for index in which:
                wait_all(groups[index])

    arrived(0)
    x = jnp.concatenate([x_own_ref[0], x_got_ref[0]], axis=0).astype(F32)
    summed = x + output_bias_ref[0:1] + mm_nt(mixed_ref[0], out_weights[...])
    normal_in, scale_in = normalize(summed)
    normed = normal_in * gain_ref[0:1] + shift_ref[0:1]
    normed_low = normed.astype(BF16)
    total = normed + output_bias_ref[1:2]
    for at in parts:
        if at == 0:
            arrived(1)
        if at < tail < at + size or at == tail:
            arrived(3)
        pre = mm(normed_low, in_weights[:, at : at + size]) + hidden_bias_ref[:, at : at + size]
        share = 0.5 * (1.0 + lax.erf(pre * 0.7071067811865476))
        slope[:, at : at + size] = share + pre * jnp.exp(-0.5 * pre * pre) * 0.3989422804014327
        if at == 0:
            arrived(2)
        if at < tail < at + size or at == tail:
            arrived(4)
        total += mm_nt((pre * share).astype(BF16), back_weights[:, at : at + size])
    normal_out, scale_out = normalize(total)
    out = (normal_out * gain_ref[1:2] + shift_ref[1:2]).astype(BF16)
    out_own_ref[0] = out[:half_slot]
    out_got_ref[0] = out[half_slot:]
    grad = jnp.concatenate([grad_own_ref[0], grad_got_ref[0]], axis=0).astype(F32)
    grad_total = normalize_back(grad, gain_ref[1:2], normal_out, scale_out)
    grad_low = grad_total.astype(BF16)
    grad_normed = grad_total
    for at in parts:
        grad_pre = (mm(grad_low, back_weights[:, at : at + size]) * slope[:, at : at + size]).astype(BF16)
        grad_normed += mm_nt(grad_pre, in_weights[:, at : at + size])
    grad_hidden = normalize_back(grad_normed, gain_ref[0:1], normal_in, scale_in)
    grad_hidden_ref[0] = grad_hidden
    grad_mixed_ref[0] = mm(grad_hidden.astype(BF16), out_weights[...]).astype(BF16)


def attend_back_kernel(lengths, bounds, core_ref, *refs):
    (
        qkv_ref,
        mixed_ref,
        spare_ref,
        low_ref,
        grad_mixed_ref,
        grads_ref,
        adapter_ref,
    ) = refs
    item = pl.program_id(0)
    core = core_ref[0]
    slot, width = mixed_ref.shape[1:]
    heads = width // 2

    lane, _, key_flags = flags_of(core, lengths[item], bounds[item], slot)
    row = iota((width, LANES), 0)
    column = iota((width, LANES), 1)
    pick = jnp.where((row // HEAD_DIM == (column & 15)) & (column < 48), 1.0, 0.0).astype(BF16)
    product = grad_mixed_ref[0].astype(F32) * mixed_ref[0].astype(F32)
    high = product.astype(BF16)
    rest = (product - high.astype(F32)).astype(BF16)
    inner = three_parts(mm(high, pick) + mm(rest, pick), lane).astype(BF16)
    spare = spare_ref[0]
    zero = jnp.zeros((slot, LANES), BF16)
    for pair in range(width // LANES):
        at_query, at_key, at_value = pair_columns(pair, heads)
        query = qkv_ref[0, :, at_query : at_query + LANES]
        keys = qkv_ref[0, :, at_key : at_key + LANES]
        values = qkv_ref[0, :, at_value : at_value + LANES]
        grad = grad_mixed_ref[0, :, pair * LANES : (pair + 1) * LANES]
        total_query = jnp.zeros((slot, LANES), F32)
        total_key = jnp.zeros((slot, LANES), F32)
        total_value = jnp.zeros((slot, LANES), F32)
        for side in range(2):
            head = 2 * pair + side
            inside = (lane < HEAD_DIM) if side == 0 else (lane >= HEAD_DIM)
            mine = ((lane & 15) == head) & (lane < 48)
            query_side = jnp.where(inside, query, zero)
            key_side = jnp.where(inside, keys, zero)
            grad_side = jnp.where(inside, grad, zero)
            key_wide = jnp.concatenate([keys, jnp.where(mine, -1.0, key_flags).astype(BF16)], axis=1)
            value_wide = jnp.concatenate([values, jnp.where(mine, -1.0, 0.0).astype(BF16)], axis=1)
            probs = jnp.exp(mm_nt(key_wide, jnp.concatenate([query_side, spare], axis=1)))
            grad_probs = mm_nt(value_wide, jnp.concatenate([grad_side, inner], axis=1))
            grad_scores = (probs * grad_probs).astype(BF16)
            total_value += mm(probs.astype(BF16), grad_side)
            total_key += mm(grad_scores, query_side)
            total_query += mm_tn(grad_scores, key_side)
        grads_ref[0, :, at_query : at_query + LANES] = (total_query * 0.125).astype(BF16)
        grads_ref[0, :, at_key : at_key + LANES] = total_key.astype(BF16)
        grads_ref[0, :, at_value : at_value + LANES] = total_value.astype(BF16)

    update = 2.0 * mm_tn(low_ref[0], grads_ref[0])
    parts = []
    for half in range(2):
        at = half * 3 * heads
        of_query = update[:, at : at + heads]
        of_value = update[:, at + 2 * heads : at + 3 * heads]
        rows = [
            of_query[:RANK] + of_query[LANES : LANES + RANK],
            of_value[RANK : 2 * RANK] + of_value[LANES + RANK : LANES + 2 * RANK],
        ]
        parts.append(jnp.concatenate(rows, axis=0))
    part = jnp.concatenate(parts, axis=1)

    @pl.when(item == 0)
    def _():
        adapter_ref[...] = part

    @pl.when(item > 0)
    def _():
        adapter_ref[...] += part


def input_grad_kernel(order, n, offsets, core_ref, *refs):
    pieces = (refs[:n], refs[n : 2 * n])
    (
        grads_ref,
        grad_hidden_ref,
        up_own_ref,
        up_got_ref,
        own_ref,
        got_ref,
        weights,
        up,
        sems,
    ) = refs[2 * n :]
    slot, width = grad_hidden_ref.shape[1:]
    heads = width // 2

    @pl.when(pl.program_id(0) == 0)
    def _():
        copies = load_projections(order, offsets, pieces, weights, sems.at[0], heads, (6 * heads, 6 * heads + LANES))
        start_all(copies)
        up[...] = jnp.zeros_like(up)
        up[: 2 * RANK] = ups((up_own_ref, up_got_ref), heads)
        wait_all(copies)

    grads = grads_ref[0]
    small = two_parts(mm_nt(grads, up[...]))
    total = grad_hidden_ref[0] + mm_nt(jnp.concatenate([grads, small], axis=1), weights[...])
    own_ref[0] = total[: slot // 2]
    got_ref[0] = total[slot // 2 :]


def any_spec():
    return pl.BlockSpec(memory_space=pl.ANY)


def whole_spec(array):
    return pl.BlockSpec(array.shape, lambda i, *_: (0,) * array.ndim)


def item_spec(shape):
    return pl.BlockSpec((1, *shape[1:]), lambda i, *_: (i, 0, 0))


def shape_of(shape, dtype):
    return jax.ShapeDtypeStruct(shape, dtype)


def call(kernel, name, scalars, flat, args, outs, scratch, items, flops, moved):
    return pl.pallas_call(
        kernel,
        grid_spec=pltpu.PrefetchScalarGridSpec(
            num_scalar_prefetch=len(scalars),
            grid=(items,),
            in_specs=[any_spec()] * len(flat) + [spec for _, spec in args],
            out_specs=[spec for _, spec in outs],
            scratch_shapes=scratch,
        ),
        out_shape=[shape for shape, _ in outs],
        compiler_params=pltpu.CompilerParams(vmem_limit_bytes=VMEM_LIMIT),
        cost_estimate=pl.CostEstimate(flops=flops, bytes_accessed=moved, transcendentals=0),
        name=name,
    )(*scalars, *flat, *[array for array, _ in args])


def swap(array):
    return lax.ppermute(array, "tensor", [(0, 1), (1, 0)])


def after(value, *deps):
    return lax.optimization_barrier((value, *deps))[0]


def over_dp(count, array, target):
    return lax.ppermute(array, "dp", [(i, target(i)) for i in range(count)])


LINE_FIRST = ((4, 8, 1, 2), (8, 4, 2, 1))
PLANE_FIRST = ((1, 2, 4, 8), (2, 1, 8, 4))


def block_offsets(index, rows, flips):
    place = jnp.arange(16)
    flipped = sum(((place >> bit) & 1) * flips[bit] for bit in range(4))
    return ((index ^ flipped) * rows).astype(jnp.int32)


def local(
    inputs,
    lengths,
    bounds,
    query_matrix,
    key_matrix,
    value_matrix,
    query_value_bias,
    adapter_down_weight,
    adapter_up_weight,
    attention_output_weight,
    feedforward_input_weight,
    feedforward_input_bias,
    feedforward_output_weight,
    output_bias,
    layernorm_scale,
    layernorm_bias,
    output_gradient,
    *,
    count,
):
    micro, rows, width = inputs.shape
    mine = micro // 2
    slot = 2 * rows
    heads = width // 2
    core = lax.axis_index("tensor")
    shard_rows = query_matrix.shape[0]
    hidden = feedforward_input_weight.shape[1]
    last = hidden // 3 if count == 16 else hidden // 2
    first = hidden - last

    down = jnp.transpose(adapter_down_weight, (1, 0, 2)).reshape(shard_rows, 2 * RANK)
    down = jnp.pad(down, ((0, 0), (0, LANES - 2 * RANK)))
    shard = jnp.concatenate([query_matrix, key_matrix, value_matrix, down], axis=1)
    back = feedforward_output_weight.T
    shard_first = jnp.concatenate(
        [attention_output_weight.T, feedforward_input_weight[:, :first], back[:, :first]], axis=1
    )
    shard_last = jnp.concatenate([feedforward_input_weight[:, first:], back[:, first:]], axis=1)

    others = (1 - core) * mine
    x_got = swap(lax.dynamic_slice_in_dim(inputs, others, mine, 0))
    bias_got, up_got = swap(query_value_bias), swap(adapter_up_weight)

    if count == 16:
        index = lax.axis_index("dp")

        def tables(flips):
            mine_first = [jnp.where(core == 0, a, b) for a, b in zip(*flips, strict=True)]
            other_first = [jnp.where(core == 0, b, a) for a, b in zip(*flips, strict=True)]
            return [block_offsets(index, shard_rows, f) for f in (mine_first, other_first)]

        offsets = jnp.concatenate(tables(LINE_FIRST) + tables(PLANE_FIRST))
        order, order_last, n = ((0, 16), 8), ((32, 48), 8), 2

        def exchange(array, flips, step):
            pairs = [(2 * i + t, 2 * (i ^ flips[t][step]) + t) for i in range(count) for t in range(2)]
            return lax.ppermute(array, ("dp", "tensor"), pairs)

        def joined(*arrays):
            return jnp.concatenate(arrays, axis=0)

        line = joined(shard, exchange(shard, LINE_FIRST, 0))
        plane = joined(shard_last, exchange(shard_last, PLANE_FIRST, 0))
        line, plane = lax.optimization_barrier((line, plane))
        line = joined(line, exchange(line, LINE_FIRST, 1))
        plane = joined(plane, exchange(plane, PLANE_FIRST, 1))
        line, plane, x_got, bias_got, up_got, shard_first = lax.optimization_barrier(
            (line, plane, x_got, bias_got, up_got, shard_first)
        )
        line_first = joined(shard_first, exchange(shard_first, LINE_FIRST, 0))
        line = joined(line, exchange(line, LINE_FIRST, 2))
        line_first, line = lax.optimization_barrier((line_first, line))
        line_first = joined(line_first, exchange(line_first, LINE_FIRST, 1))
        own = [line, exchange(line, LINE_FIRST, 3)]
        swapped = [swap(line)]
        line_first, plane, own, swapped = lax.optimization_barrier((line_first, plane, own, swapped))
        swapped.append(swap(own[1]))
        line_first = joined(line_first, exchange(line_first, LINE_FIRST, 2))
        plane = joined(plane, exchange(plane, PLANE_FIRST, 2))
        plane, line_first, x_got, swapped = lax.optimization_barrier((plane, line_first, x_got, swapped))
        own_first = [line_first, exchange(line_first, LINE_FIRST, 3)]
        own_last = [plane, exchange(plane, PLANE_FIRST, 3)]
        got_first, got_last = [swap(line_first)], [swap(plane)]
    else:
        offsets = jnp.zeros((2,), jnp.int32)
        order = order_last = ((0, 0), 1)
        n = 1
        own, own_first, own_last = (
            [lax.all_gather(s, "dp", axis=0, tiled=True)] for s in (shard, shard_first, shard_last)
        )
        swapped, got_first, got_last = [swap(own[0])], [], []
    pieces = (*own, *swapped)

    first_item = core * mine
    my_lengths = lax.dynamic_slice_in_dim(lengths[:, 0], first_item, mine, 0)
    my_bounds = lax.dynamic_slice_in_dim(bounds[:, 0], first_item, mine, 0)
    core = core[None].astype(jnp.int32)

    blank = jnp.zeros((heads,), F32)
    ones = blank + 1
    both = [query_value_bias[0], blank, query_value_bias[1], bias_got[0], blank, bias_got[1]]
    scale = [ones * 0.125, ones, ones] * 2
    bias = jnp.stack([jnp.concatenate(both), jnp.concatenate(scale)])
    own_block = pl.BlockSpec((1, rows, width), lambda i, *s: (s[-1][0] * mine + i, 0, 0))
    got_block = pl.BlockSpec((1, rows, width), lambda i, *_: (i, 0, 0))
    item = (mine, slot, width)
    wide = (mine, slot, 3 * width)

    def out_item(shape, dtype):
        return shape_of(shape, dtype), item_spec(shape)

    def in_item(array):
        return array, item_spec(array.shape)

    def in_whole(array):
        return array, whole_spec(array)

    split_out = lambda dtype: [(shape_of(inputs.shape, dtype), own_block), (shape_of((mine, rows, width), dtype), got_block)]

    tokens = mine * slot
    qkv, mixed, spare, low = call(
        functools.partial(project_attend_kernel, order, n),
        "project_attend",
        (offsets, my_lengths, my_bounds, core),
        pieces,
        [(inputs, own_block), (x_got, got_block), in_whole(bias), in_whole(adapter_up_weight), in_whole(up_got)],
        [
            out_item(wide, BF16),
            out_item(item, BF16),
            out_item((mine, slot, LANES), BF16),
            out_item((mine, slot, 2 * LANES), BF16),
        ],
        [
            pltpu.VMEM((width + 2 * LANES, 3 * width), BF16),
            pltpu.VMEM((width, LANES), BF16),
            pltpu.SemaphoreType.DMA((2,)),
        ],
        mine,
        2 * tokens * width * (4 * width + 8 * slot),
        12 * tokens * width,
    )
    grad_got = swap(lax.dynamic_slice_in_dim(output_gradient, others, mine, 0))
    hidden_bias_got = swap(feedforward_input_bias)
    own_first, own_last = lax.optimization_barrier((own_first, own_last, mixed))[:2]
    got_first += map(swap, own_first[len(got_first) :])
    got_last += map(swap, own_last[len(got_last) :])
    hidden_bias = jnp.concatenate(
        [
            feedforward_input_bias[:first],
            hidden_bias_got[:first],
            feedforward_input_bias[first:],
            hidden_bias_got[first:],
        ]
    )[None]
    pieces_feed = (*own_first, *got_first, *own_last, *got_last)
    out, out_send, grad_hidden, grad_mixed = call(
        functools.partial(feed_kernel, (order, order_last), (first, last), n),
        "feed",
        (offsets, core),
        pieces_feed,
        [
            (inputs, own_block),
            (x_got, got_block),
            in_item(mixed),
            (output_gradient, own_block),
            (grad_got, got_block),
            *map(in_whole, (hidden_bias, output_bias, layernorm_scale, layernorm_bias)),
        ],
        [*split_out(BF16), out_item(item, F32), out_item(item, BF16)],
        [
            pltpu.VMEM((width, width), BF16),
            pltpu.VMEM((width, 2 * hidden), BF16),
            pltpu.VMEM((width, 2 * hidden), BF16),
            pltpu.VMEM((slot, 2 * hidden), F32),
            pltpu.SemaphoreType.DMA((5,)),
        ],
        mine,
        4 * tokens * width * (width + 4 * hidden),
        8 * width * hidden,
    )
    out_send = swap(out_send)
    adapter = (2 * RANK, width)
    grads, adapter = call(
        attend_back_kernel,
        "attend_back",
        (my_lengths, my_bounds, core),
        (),
        [*map(in_item, (qkv, mixed, spare, low, grad_mixed))],
        [out_item(wide, BF16), (shape_of(adapter, F32), pl.BlockSpec(adapter, lambda i, *_: (0, 0)))],
        [],
        mine,
        2 * tokens * width * 20 * slot,
        16 * tokens * width,
    )
    if count == 16:
        ways = [over_dp(count, adapter, lambda i, flip=flip: i ^ flip) for flip in (1, 2, 3)]
    total, total_send = call(
        functools.partial(input_grad_kernel, order, n),
        "input_grad",
        (offsets, core),
        pieces,
        [in_item(grads), in_item(grad_hidden), in_whole(adapter_up_weight), in_whole(up_got)],
        split_out(F32),
        [
            pltpu.VMEM((width, 3 * width + 2 * LANES), BF16),
            pltpu.VMEM((LANES, 3 * width), BF16),
            pltpu.SemaphoreType.DMA((1,)),
        ],
        mine,
        2 * tokens * width * 3 * width,
        12 * tokens * width,
    )
    if count == 16:
        *ways, total_send, out = lax.optimization_barrier((*ways, total_send, out))
        adapter = (adapter + ways[0]) + (ways[1] + ways[2])
        ways = [over_dp(count, adapter, lambda i, flip=flip: i ^ flip) for flip in (4, 8, 12)]
        input_grad = lax.dynamic_update_slice_in_dim(total, swap(total_send), others, 0)
        result = lax.dynamic_update_slice_in_dim(out, out_send, others, 0)
        *ways, input_grad, result = lax.optimization_barrier((*ways, input_grad, result))
        adapter = (adapter + ways[0]) + (ways[1] + ways[2])
    else:
        adapter = lax.psum(adapter, "dp")
        input_grad = lax.dynamic_update_slice_in_dim(total, swap(total_send), others, 0)
        result = lax.dynamic_update_slice_in_dim(out, out_send, others, 0)
    adapter = adapter[:, :heads] + swap(adapter[:, heads:])
    return result, input_grad, adapter.reshape(2, RANK, heads)


def solution(mesh):
    return jax.shard_map(
        functools.partial(local, count=mesh.shape["dp"]),
        mesh=mesh,
        in_specs=(
            P(None, ("dp", "tensor"), None),
            P(None, "dp"),
            P(None, "dp"),
            P("dp", "tensor"),
            P("dp", "tensor"),
            P("dp", "tensor"),
            P(None, "tensor"),
            P(None, "dp", None),
            P(None, None, "tensor"),
            P("tensor", "dp"),
            P("dp", "tensor"),
            P("tensor"),
            P("tensor", "dp"),
            P(),
            P(),
            P(),
            P(None, ("dp", "tensor"), None),
        ),
        out_specs=(
            P(None, ("dp", "tensor"), None),
            P(None, ("dp", "tensor"), None),
            P(None, None, "tensor"),
        ),
        check_vma=False,
    )
```

```python
import functools

import jax
import jax.numpy as jnp
from jax import lax
from jax.experimental import pallas as pl
from jax.experimental.pallas import tpu as pltpu
from jax.sharding import PartitionSpec as P

F32 = jnp.float32
BF16 = jnp.bfloat16
HEAD_DIM = 64
RANK = 8
LANES = 128
EPS = 1e-05
MASKED = -float(2**30)
SEG = 64
VMEM_LIMIT = 60 * 2**20

NT = (((1,), (1,)), ((), ()))
TN = (((0,), (0,)), ((), ()))


def mm(a, b):
    return jnp.dot(a, b, preferred_element_type=F32)


def mm_nt(a, b):
    return lax.dot_general(a, b, NT, preferred_element_type=F32)


def mm_tn(a, b):
    return lax.dot_general(a, b, TN, preferred_element_type=F32)


def iota(shape, dimension):
    return lax.broadcasted_iota(jnp.int32, shape, dimension)


def three_parts(value, lane):
    high = value.astype(BF16).astype(F32)
    rest = value - high
    middle = rest.astype(BF16).astype(F32)
    return jnp.where(lane < 16, high, jnp.where(lane < 32, middle, jnp.where(lane < 48, rest - middle, 0.0)))


def two_parts(value):
    high = value.astype(BF16)
    return jnp.concatenate([high, (value - high.astype(F32)).astype(BF16)], axis=1)


def weight_copies(order, offsets, pieces, target, sem, columns):
    firsts, blocks = order
    copies, waits = [], []
    for half, first, width, to in columns:
        for index, ref in enumerate(pieces[half]):
            rows = ref.shape[0] // blocks
            for place in range(blocks):
                start = offsets[firsts[half] + index * blocks + place]
                if rows % 16 == 0:
                    start = pl.multiple_of(start, 16)
                copies.append(
                    pltpu.make_async_copy(
                        ref.at[pl.ds(place * rows, rows), pl.ds(first, width)],
                        target.at[pl.ds(start, rows), pl.ds(to, width)],
                        sem,
                    )
                )
        filled = target.at[pl.ds(0, sum(ref.shape[0] for ref in pieces[half])), pl.ds(to, width)]
        waits.append(pltpu.make_async_copy(filled, filled, sem))
    return copies, waits


def start_all(group):
    for copy in group[0]:
        copy.start()


def wait_all(group):
    for copy in group[1]:
        copy.wait()


def places(core, shape, half_slot):
    row = iota(shape, 0)
    return jnp.where(row < half_slot, row + core * half_slot, row - core * half_slot)


def flags_of(core, length, bound, slot):
    lane = iota((slot, LANES), 1)
    place = places(core, (slot, LANES), slot // 2)
    second = place >= bound
    query = jnp.where(
        lane == SEG,
        jnp.where(second, 1.0, 0.0),
        jnp.where(lane == SEG + 1, jnp.where(second, 0.0, 1.0), jnp.where(lane == SEG + 2, 1.0, 0.0)),
    )
    key = jnp.where(
        lane == SEG,
        jnp.where(second, 0.0, MASKED),
        jnp.where(
            lane == SEG + 1,
            jnp.where(second, MASKED, 0.0),
            jnp.where((lane == SEG + 2) & (place >= length), MASKED, 0.0),
        ),
    )
    return lane, query, key


def pair_columns(pair, heads):
    per_half = heads // LANES
    base = (pair // per_half) * 3 * heads + (pair % per_half) * LANES
    return base, base + heads, base + 2 * heads


def load_projections(order, offsets, pieces, weights, sem, heads, downs):
    wide = 3 * heads
    columns = [(0, 0, wide, 0), (1, 0, wide, wide)]
    columns += [(0, wide, LANES, to) for to in downs]
    return weight_copies(order, offsets, pieces, weights, sem, columns)


def ups(up_refs, heads):
    blank = jnp.zeros((RANK, heads), BF16)
    parts = []
    for ref in up_refs:
        parts += [
            jnp.concatenate([ref[0] * 2, blank], axis=0),
            jnp.concatenate([blank, blank], axis=0),
            jnp.concatenate([blank, ref[1] * 2], axis=0),
        ]
    return jnp.concatenate(parts, axis=1)


def project_attend_kernel(order, n, offsets, lengths, bounds, core_ref, *refs):
    pieces = (refs[:n], refs[n : 2 * n])
    (
        x_own_ref,
        x_got_ref,
        bias_ref,
        up_own_ref,
        up_got_ref,
        qkv_ref,
        mixed_ref,
        spare_ref,
        low_ref,
        weights,
        down,
        sems,
    ) = refs[2 * n :]
    item = pl.program_id(0)
    core = core_ref[0]
    slot, width = mixed_ref.shape[1:]
    heads = width // 2

    @pl.when(item == 0)
    def _():
        wide = 3 * heads
        copies = weight_copies(order, offsets, pieces, weights, sems.at[0], [(0, 0, wide, 0), (1, 0, wide, wide)])
        downs = weight_copies(order, offsets, pieces, down, sems.at[1], [(0, wide, LANES, 0)])
        start_all(downs)
        start_all(copies)
        weights[width:] = jnp.zeros((2 * LANES, 6 * heads), BF16)
        up = ups((up_own_ref, up_got_ref), heads)
        weights[width : width + 2 * RANK] = up
        weights[width + LANES : width + LANES + 2 * RANK] = up
        wait_all(downs)
        wait_all(copies)

    x = jnp.concatenate([x_own_ref[0], x_got_ref[0]], axis=0)
    low = two_parts(mm(x, down[...]))
    low_ref[0] = low
    wide_x = jnp.concatenate([x, low], axis=1)
    for part in range(3):
        at = slice(part * width, (part + 1) * width)
        out = (mm(wide_x, weights[:, at]) + bias_ref[0:1, at]) * bias_ref[1:2, at]
        qkv_ref[0, :, at] = out.astype(BF16)

    lane, query_flags, key_flags = flags_of(core, lengths[item], bounds[item], slot)
    query_low = query_flags.astype(BF16)
    key_low = key_flags.astype(BF16)
    ones = jnp.where(lane == 0, 1.0, 0.0).astype(BF16)
    zero = jnp.zeros((slot, LANES), BF16)
    totals = jnp.ones((slot, LANES), F32)
    peaks = []
    for pair in range(width // LANES):
        at_query, at_key, at_value = pair_columns(pair, heads)
        query = qkv_ref[0, :, at_query : at_query + LANES]
        keys = jnp.concatenate([qkv_ref[0, :, at_key : at_key + LANES], key_low], axis=1)
        values = jnp.concatenate([qkv_ref[0, :, at_value : at_value + LANES], ones], axis=1)
        outs = []
        for side in range(2):
            inside = (lane < HEAD_DIM) if side == 0 else (lane >= HEAD_DIM)
            query_side = jnp.concatenate([jnp.where(inside, query, zero), query_low], axis=1)
            scores = mm_nt(keys, query_side)
            peak = jnp.max(scores, axis=0, keepdims=True)
            probs = jnp.exp(scores - peak).astype(BF16)
            out = mm_tn(probs, values)
            total = out[:, LANES : LANES + 1]
            outs.append(out[:, :LANES] * (1.0 / total))
            totals = jnp.where((lane & 15) == 2 * pair + side, total, totals)
            peaks.append(peak)
        mixed_ref[0, :, pair * LANES : (pair + 1) * LANES] = jnp.where(
            lane < HEAD_DIM, outs[0], outs[1]
        ).astype(BF16)
    peaks += [jnp.zeros((1, slot), F32)] * (16 - len(peaks))
    peaks = jnp.concatenate(peaks, axis=0)
    peaks = jnp.concatenate([peaks] * (LANES // 16), axis=0).T
    spare_ref[0] = (three_parts(peaks + jnp.log(totals), lane) + query_flags).astype(BF16)


def row_mean(value):
    return jnp.mean(value, axis=-1, keepdims=True)


def normalize(value):
    centre = value - row_mean(value)
    scale = lax.rsqrt(row_mean(centre * centre) + EPS)
    return centre * scale, scale


def normalize_back(grad, gain, normal, scale):
    grad = grad * gain
    return scale * (grad - row_mean(grad) - normal * row_mean(grad * normal))


def feed_kernel(orders, chunks, n, offsets, core_ref, *refs):
    pieces = (refs[:n], refs[n : 2 * n])
    pieces_last = (refs[2 * n : 3 * n], refs[3 * n : 4 * n])
    (
        x_own_ref,
        x_got_ref,
        mixed_ref,
        grad_own_ref,
        grad_got_ref,
        hidden_bias_ref,
        output_bias_ref,
        gain_ref,
        shift_ref,
        out_own_ref,
        out_got_ref,
        grad_hidden_ref,
        grad_mixed_ref,
        out_weights,
        in_weights,
        back_weights,
        slope,
        sems,
    ) = refs[4 * n :]
    slot, width = mixed_ref.shape[1:]
    half_slot = slot // 2
    heads = width // 2
    first, last = chunks
    size = width
    parts = list(range(0, 2 * (first + last), size))

    o = heads
    tail = 2 * first
    groups = [
        weight_copies(orders[0], offsets, pieces, out_weights, sems.at[0], [(0, 0, o, 0), (1, 0, o, o)]),
        weight_copies(orders[0], offsets, pieces, in_weights, sems.at[1], [(0, o, first, 0), (1, o, first, first)]),
        weight_copies(
            orders[0], offsets, pieces, back_weights, sems.at[2], [(0, o + first, first, 0), (1, o + first, first, first)]
        ),
        weight_copies(
            orders[1], offsets, pieces_last, in_weights, sems.at[3], [(0, 0, last, tail), (1, 0, last, tail + last)]
        ),
        weight_copies(
            orders[1], offsets, pieces_last, back_weights, sems.at[4], [(0, last, last, tail), (1, last, last, tail + last)]
        ),
    ]

    @pl.when(pl.program_id(0) == 0)
    def _():
        for group in groups:
            start_all(group)

    def arrived(*which):
        @pl.when(pl.program_id(0) == 0)
        def _():
            for index in which:
                wait_all(groups[index])

    arrived(0)
    x = jnp.concatenate([x_own_ref[0], x_got_ref[0]], axis=0).astype(F32)
    summed = x + output_bias_ref[0:1] + mm_nt(mixed_ref[0], out_weights[...])
    normal_in, scale_in = normalize(summed)
    normed = normal_in * gain_ref[0:1] + shift_ref[0:1]
    normed_low = normed.astype(BF16)
    total = normed + output_bias_ref[1:2]
    for at in parts:
        if at == 0:
            arrived(1)
        if at < tail < at + size or at == tail:
            arrived(3)
        pre = mm(normed_low, in_weights[:, at : at + size]) + hidden_bias_ref[:, at : at + size]
        share = 0.5 * (1.0 + lax.erf(pre * 0.7071067811865476))
        slope[:, at : at + size] = share + pre * jnp.exp(-0.5 * pre * pre) * 0.3989422804014327
        if at == 0:
            arrived(2)
        if at < tail < at + size or at == tail:
            arrived(4)
        total += mm_nt((pre * share).astype(BF16), back_weights[:, at : at + size])
    normal_out, scale_out = normalize(total)
    out = (normal_out * gain_ref[1:2] + shift_ref[1:2]).astype(BF16)
    out_own_ref[0] = out[:half_slot]
    out_got_ref[0] = out[half_slot:]
    grad = jnp.concatenate([grad_own_ref[0], grad_got_ref[0]], axis=0).astype(F32)
    grad_total = normalize_back(grad, gain_ref[1:2], normal_out, scale_out)
    grad_low = grad_total.astype(BF16)
    grad_normed = grad_total
    for at in parts:
        grad_pre = (mm(grad_low, back_weights[:, at : at + size]) * slope[:, at : at + size]).astype(BF16)
        grad_normed += mm_nt(grad_pre, in_weights[:, at : at + size])
    grad_hidden = normalize_back(grad_normed, gain_ref[0:1], normal_in, scale_in)
    grad_hidden_ref[0] = grad_hidden
    grad_mixed_ref[0] = mm(grad_hidden.astype(BF16), out_weights[...]).astype(BF16)


def attend_back_kernel(lengths, bounds, core_ref, *refs):
    (
        qkv_ref,
        mixed_ref,
        spare_ref,
        low_ref,
        grad_mixed_ref,
        grads_ref,
        adapter_ref,
    ) = refs
    item = pl.program_id(0)
    core = core_ref[0]
    slot, width = mixed_ref.shape[1:]
    heads = width // 2

    lane, _, key_flags = flags_of(core, lengths[item], bounds[item], slot)
    row = iota((width, LANES), 0)
    column = iota((width, LANES), 1)
    pick = jnp.where((row // HEAD_DIM == (column & 15)) & (column < 48), 1.0, 0.0).astype(BF16)
    product = grad_mixed_ref[0].astype(F32) * mixed_ref[0].astype(F32)
    high = product.astype(BF16)
    rest = (product - high.astype(F32)).astype(BF16)
    inner = three_parts(mm(high, pick) + mm(rest, pick), lane).astype(BF16)
    spare = spare_ref[0]
    zero = jnp.zeros((slot, LANES), BF16)
    per_half = heads // LANES

    def columns(first):
        return pl.ds(pl.multiple_of(first, LANES), LANES)

    def of_pair(pair):
        base = (pair // per_half) * 3 * heads + (pair % per_half) * LANES
        at_query, at_key, at_value = (columns(base + part * heads) for part in range(3))
        query = qkv_ref[0, :, at_query]
        keys = qkv_ref[0, :, at_key]
        values = qkv_ref[0, :, at_value]
        grad = grad_mixed_ref[0, :, columns(pair * LANES)]
        total_query = jnp.zeros((slot, LANES), F32)
        total_key = jnp.zeros((slot, LANES), F32)
        total_value = jnp.zeros((slot, LANES), F32)
        for side in range(2):
            head = 2 * pair + side
            inside = (lane < HEAD_DIM) if side == 0 else (lane >= HEAD_DIM)
            mine = ((lane & 15) == head) & (lane < 48)
            query_side = jnp.where(inside, query, zero)
            key_side = jnp.where(inside, keys, zero)
            grad_side = jnp.where(inside, grad, zero)
            key_wide = jnp.concatenate([keys, jnp.where(mine, -1.0, key_flags).astype(BF16)], axis=1)
            value_wide = jnp.concatenate([values, jnp.where(mine, -1.0, 0.0).astype(BF16)], axis=1)
            probs = jnp.exp(mm_nt(key_wide, jnp.concatenate([query_side, spare], axis=1)))
            grad_probs = mm_nt(value_wide, jnp.concatenate([grad_side, inner], axis=1))
            grad_scores = (probs * grad_probs).astype(BF16)
            total_value += mm(probs.astype(BF16), grad_side)
            total_key += mm(grad_scores, query_side)
            total_query += mm_tn(grad_scores, key_side)
        grads_ref[0, :, at_query] = (total_query * 0.125).astype(BF16)
        grads_ref[0, :, at_key] = total_key.astype(BF16)
        grads_ref[0, :, at_value] = total_value.astype(BF16)

    pairs = width // LANES
    group = 3 if pairs % 3 == 0 else 1

    @pl.loop(0, pairs // group)
    def _(step):
        for place in range(group):
            of_pair(step * group + place)

    update = 2.0 * mm_tn(low_ref[0], grads_ref[0])
    parts = []
    for half in range(2):
        at = half * 3 * heads
        of_query = update[:, at : at + heads]
        of_value = update[:, at + 2 * heads : at + 3 * heads]
        rows = [
            of_query[:RANK] + of_query[LANES : LANES + RANK],
            of_value[RANK : 2 * RANK] + of_value[LANES + RANK : LANES + 2 * RANK],
        ]
        parts.append(jnp.concatenate(rows, axis=0))
    part = jnp.concatenate(parts, axis=1)

    @pl.when(item == 0)
    def _():
        adapter_ref[...] = part

    @pl.when(item > 0)
    def _():
        adapter_ref[...] += part


def input_grad_kernel(order, n, offsets, core_ref, *refs):
    pieces = (refs[:n], refs[n : 2 * n])
    (
        grads_ref,
        grad_hidden_ref,
        up_own_ref,
        up_got_ref,
        own_ref,
        got_ref,
        weights,
        up,
        sems,
    ) = refs[2 * n :]
    slot, width = grad_hidden_ref.shape[1:]
    heads = width // 2

    @pl.when(pl.program_id(0) == 0)
    def _():
        copies = load_projections(order, offsets, pieces, weights, sems.at[0], heads, (6 * heads, 6 * heads + LANES))
        start_all(copies)
        up[...] = jnp.zeros_like(up)
        up[: 2 * RANK] = ups((up_own_ref, up_got_ref), heads)
        wait_all(copies)

    grads = grads_ref[0]
    small = two_parts(mm_nt(grads, up[...]))
    total = grad_hidden_ref[0] + mm_nt(jnp.concatenate([grads, small], axis=1), weights[...])
    own_ref[0] = total[: slot // 2]
    got_ref[0] = total[slot // 2 :]


def any_spec():
    return pl.BlockSpec(memory_space=pl.ANY)


def whole_spec(array):
    return pl.BlockSpec(array.shape, lambda i, *_: (0,) * array.ndim)


def item_spec(shape):
    return pl.BlockSpec((1, *shape[1:]), lambda i, *_: (i, 0, 0))


def shape_of(shape, dtype):
    return jax.ShapeDtypeStruct(shape, dtype)


def call(kernel, name, scalars, flat, args, outs, scratch, items, flops, moved):
    return pl.pallas_call(
        kernel,
        grid_spec=pltpu.PrefetchScalarGridSpec(
            num_scalar_prefetch=len(scalars),
            grid=(items,),
            in_specs=[any_spec()] * len(flat) + [spec for _, spec in args],
            out_specs=[spec for _, spec in outs],
            scratch_shapes=scratch,
        ),
        out_shape=[shape for shape, _ in outs],
        compiler_params=pltpu.CompilerParams(vmem_limit_bytes=VMEM_LIMIT),
        cost_estimate=pl.CostEstimate(flops=flops, bytes_accessed=moved, transcendentals=0),
        name=name,
    )(*scalars, *flat, *[array for array, _ in args])


def swap(array):
    return lax.ppermute(array, "tensor", [(0, 1), (1, 0)])


def after(value, *deps):
    return lax.optimization_barrier((value, *deps))[0]


def over_dp(count, array, target):
    return lax.ppermute(array, "dp", [(i, target(i)) for i in range(count)])


LINE_FIRST = ((4, 8, 1, 2), (8, 4, 2, 1))
PLANE_FIRST = ((1, 2, 4, 8), (2, 1, 8, 4))


def block_offsets(index, rows, flips):
    place = jnp.arange(16)
    flipped = sum(((place >> bit) & 1) * flips[bit] for bit in range(4))
    return ((index ^ flipped) * rows).astype(jnp.int32)


def local(
    inputs,
    lengths,
    bounds,
    query_matrix,
    key_matrix,
    value_matrix,
    query_value_bias,
    adapter_down_weight,
    adapter_up_weight,
    attention_output_weight,
    feedforward_input_weight,
    feedforward_input_bias,
    feedforward_output_weight,
    output_bias,
    layernorm_scale,
    layernorm_bias,
    output_gradient,
    *,
    count,
):
    micro, rows, width = inputs.shape
    mine = micro // 2
    slot = 2 * rows
    heads = width // 2
    core = lax.axis_index("tensor")
    shard_rows = query_matrix.shape[0]
    hidden = feedforward_input_weight.shape[1]
    last = hidden // 3 if count == 16 else hidden // 2
    first = hidden - last

    down = jnp.transpose(adapter_down_weight, (1, 0, 2)).reshape(shard_rows, 2 * RANK)
    down = jnp.pad(down, ((0, 0), (0, LANES - 2 * RANK)))
    shard = jnp.concatenate([query_matrix, key_matrix, value_matrix, down], axis=1)
    back = feedforward_output_weight.T
    shard_first = jnp.concatenate(
        [attention_output_weight.T, feedforward_input_weight[:, :first], back[:, :first]], axis=1
    )
    shard_last = jnp.concatenate([feedforward_input_weight[:, first:], back[:, first:]], axis=1)

    others = (1 - core) * mine
    x_got = swap(lax.dynamic_slice_in_dim(inputs, others, mine, 0))
    grad_got = swap(lax.dynamic_slice_in_dim(output_gradient, others, mine, 0))
    bias_got, up_got, hidden_bias_got = map(swap, (query_value_bias, adapter_up_weight, feedforward_input_bias))

    blank = jnp.zeros((heads,), F32)
    ones = blank + 1
    both = [query_value_bias[0], blank, query_value_bias[1], bias_got[0], blank, bias_got[1]]
    scale = [ones * 0.125, ones, ones] * 2
    bias = jnp.stack([jnp.concatenate(both), jnp.concatenate(scale)])

    if count == 16:
        index = lax.axis_index("dp")

        def tables(flips):
            mine_first = [jnp.where(core == 0, a, b) for a, b in zip(*flips, strict=True)]
            other_first = [jnp.where(core == 0, b, a) for a, b in zip(*flips, strict=True)]
            return [block_offsets(index, shard_rows, f) for f in (mine_first, other_first)]

        offsets = jnp.concatenate(tables(LINE_FIRST) + tables(PLANE_FIRST))
        order, order_last, n = ((0, 16), 8), ((32, 48), 8), 2

        def exchange(array, flips, step):
            pairs = [(2 * i + t, 2 * (i ^ flips[t][step]) + t) for i in range(count) for t in range(2)]
            return lax.ppermute(array, ("dp", "tensor"), pairs)

        def joined(*arrays):
            return jnp.concatenate(arrays, axis=0)

        line = joined(shard, exchange(shard, LINE_FIRST, 0))
        line, shard_last = lax.optimization_barrier((line, shard_last))
        plane = joined(shard_last, exchange(shard_last, PLANE_FIRST, 0))
        line = joined(line, exchange(line, LINE_FIRST, 1))
        line, plane, *early = lax.optimization_barrier((line, plane, x_got, up_got, grad_got, hidden_bias_got, offsets, bias))
        x_got, up_got, grad_got, hidden_bias_got, offsets, bias = early
        shard_first = after(shard_first, line)
        line_first = joined(shard_first, exchange(shard_first, LINE_FIRST, 0))
        plane = joined(plane, exchange(plane, PLANE_FIRST, 1))
        line = joined(line, exchange(line, LINE_FIRST, 2))
        line, plane, line_first = lax.optimization_barrier((line, plane, line_first))
        line_first = joined(line_first, exchange(line_first, LINE_FIRST, 1))
        own = [line, exchange(line, LINE_FIRST, 3)]
        swapped = [swap(line)]
        line_first, plane, own, swapped = lax.optimization_barrier((line_first, plane, own, swapped))
        swapped.append(swap(own[1]))
        line_first = joined(line_first, exchange(line_first, LINE_FIRST, 2))
        plane = joined(plane, exchange(plane, PLANE_FIRST, 2))
        plane, line_first, x_got, swapped = lax.optimization_barrier((plane, line_first, x_got, swapped))
        own_first = [line_first, exchange(line_first, LINE_FIRST, 3)]
        own_last = [plane, exchange(plane, PLANE_FIRST, 3)]
        got_first, got_last = [swap(line_first)], [swap(plane)]
    else:
        offsets = jnp.zeros((2,), jnp.int32)
        order = order_last = ((0, 0), 1)
        n = 1
        own, own_first, own_last = (
            [lax.all_gather(s, "dp", axis=0, tiled=True)] for s in (shard, shard_first, shard_last)
        )
        swapped, got_first, got_last = [swap(own[0])], [], []
    pieces = (*own, *swapped)

    first_item = core * mine
    my_lengths = lax.dynamic_slice_in_dim(lengths[:, 0], first_item, mine, 0)
    my_bounds = lax.dynamic_slice_in_dim(bounds[:, 0], first_item, mine, 0)
    core = core[None].astype(jnp.int32)

    own_block = pl.BlockSpec((1, rows, width), lambda i, *s: (s[-1][0] * mine + i, 0, 0))
    got_block = pl.BlockSpec((1, rows, width), lambda i, *_: (i, 0, 0))
    item = (mine, slot, width)
    wide = (mine, slot, 3 * width)

    def out_item(shape, dtype):
        return shape_of(shape, dtype), item_spec(shape)

    def in_item(array):
        return array, item_spec(array.shape)

    def in_whole(array):
        return array, whole_spec(array)

    split_out = lambda dtype: [(shape_of(inputs.shape, dtype), own_block), (shape_of((mine, rows, width), dtype), got_block)]

    tokens = mine * slot
    qkv, mixed, spare, low = call(
        functools.partial(project_attend_kernel, order, n),
        "project_attend",
        (offsets, my_lengths, my_bounds, core),
        pieces,
        [(inputs, own_block), (x_got, got_block), in_whole(bias), in_whole(adapter_up_weight), in_whole(up_got)],
        [
            out_item(wide, BF16),
            out_item(item, BF16),
            out_item((mine, slot, LANES), BF16),
            out_item((mine, slot, 2 * LANES), BF16),
        ],
        [
            pltpu.VMEM((width + 2 * LANES, 3 * width), BF16),
            pltpu.VMEM((width, LANES), BF16),
            pltpu.SemaphoreType.DMA((2,)),
        ],
        mine,
        2 * tokens * width * (4 * width + 8 * slot),
        12 * tokens * width,
    )
    own_first, own_last = lax.optimization_barrier((own_first, own_last, mixed))[:2]
    got_first += map(swap, own_first[len(got_first) :])
    got_last += map(swap, own_last[len(got_last) :])
    hidden_bias = jnp.concatenate(
        [
            feedforward_input_bias[:first],
            hidden_bias_got[:first],
            feedforward_input_bias[first:],
            hidden_bias_got[first:],
        ]
    )[None]
    pieces_feed = (*own_first, *got_first, *own_last, *got_last)
    out, out_send, grad_hidden, grad_mixed = call(
        functools.partial(feed_kernel, (order, order_last), (first, last), n),
        "feed",
        (offsets, core),
        pieces_feed,
        [
            (inputs, own_block),
            (x_got, got_block),
            in_item(mixed),
            (output_gradient, own_block),
            (grad_got, got_block),
            *map(in_whole, (hidden_bias, output_bias, layernorm_scale, layernorm_bias)),
        ],
        [*split_out(BF16), out_item(item, F32), out_item(item, BF16)],
        [
            pltpu.VMEM((width, width), BF16),
            pltpu.VMEM((width, 2 * hidden), BF16),
            pltpu.VMEM((width, 2 * hidden), BF16),
            pltpu.VMEM((slot, 2 * hidden), F32),
            pltpu.SemaphoreType.DMA((5,)),
        ],
        mine,
        4 * tokens * width * (width + 4 * hidden),
        8 * width * hidden,
    )
    out_send = swap(out_send)
    adapter = (2 * RANK, width)
    grads, adapter = call(
        attend_back_kernel,
        "attend_back",
        (my_lengths, my_bounds, core),
        (),
        [*map(in_item, (qkv, mixed, spare, low, grad_mixed))],
        [out_item(wide, BF16), (shape_of(adapter, F32), pl.BlockSpec(adapter, lambda i, *_: (0, 0)))],
        [],
        mine,
        2 * tokens * width * 20 * slot,
        16 * tokens * width,
    )
    if count == 16:
        ways = [over_dp(count, adapter, lambda i, flip=flip: i ^ flip) for flip in (4, 8, 12)]
    total, total_send = call(
        functools.partial(input_grad_kernel, order, n),
        "input_grad",
        (offsets, core),
        pieces,
        [in_item(grads), in_item(grad_hidden), in_whole(adapter_up_weight), in_whole(up_got)],
        split_out(F32),
        [
            pltpu.VMEM((width, 3 * width + 2 * LANES), BF16),
            pltpu.VMEM((LANES, 3 * width), BF16),
            pltpu.SemaphoreType.DMA((1,)),
        ],
        mine,
        2 * tokens * width * 3 * width,
        12 * tokens * width,
    )
    if count == 16:
        *ways, total_send, out = lax.optimization_barrier((*ways, total_send, out))
        adapter = (adapter + ways[0]) + (ways[1] + ways[2])
        ways = [over_dp(count, adapter, lambda i, flip=flip: i ^ flip) for flip in (1, 2, 3)]
        input_grad = lax.dynamic_update_slice_in_dim(total, swap(total_send), others, 0)
        result = lax.dynamic_update_slice_in_dim(out, out_send, others, 0)
        *ways, input_grad, result = lax.optimization_barrier((*ways, input_grad, result))
        adapter = (adapter + ways[0]) + (ways[1] + ways[2])
    else:
        adapter = lax.psum(adapter, "dp")
        input_grad = lax.dynamic_update_slice_in_dim(total, swap(total_send), others, 0)
        result = lax.dynamic_update_slice_in_dim(out, out_send, others, 0)
    adapter = adapter[:, :heads] + swap(adapter[:, heads:])
    return result, input_grad, adapter.reshape(2, RANK, heads)


def solution(mesh):
    return jax.shard_map(
        functools.partial(local, count=mesh.shape["dp"]),
        mesh=mesh,
        in_specs=(
            P(None, ("dp", "tensor"), None),
            P(None, "dp"),
            P(None, "dp"),
            P("dp", "tensor"),
            P("dp", "tensor"),
            P("dp", "tensor"),
            P(None, "tensor"),
            P(None, "dp", None),
            P(None, None, "tensor"),
            P("tensor", "dp"),
            P("dp", "tensor"),
            P("tensor"),
            P("tensor", "dp"),
            P(),
            P(),
            P(),
            P(None, ("dp", "tensor"), None),
        ),
        out_specs=(
            P(None, ("dp", "tensor"), None),
            P(None, ("dp", "tensor"), None),
            P(None, None, "tensor"),
        ),
        check_vma=False,
    )
```

```python
import functools

import jax
import jax.numpy as jnp
from jax import lax
from jax.experimental import pallas as pl
from jax.experimental.pallas import tpu as pltpu
from jax.sharding import PartitionSpec as P

F32 = jnp.float32
BF16 = jnp.bfloat16
HEAD_DIM = 64
RANK = 8
LANES = 128
EPS = 1e-05
MASKED = -float(2**30)
SEG = 64
VMEM_LIMIT = 60 * 2**20

NT = (((1,), (1,)), ((), ()))
TN = (((0,), (0,)), ((), ()))


def mm(a, b):
    return jnp.dot(a, b, preferred_element_type=F32)


def mm_nt(a, b):
    return lax.dot_general(a, b, NT, preferred_element_type=F32)


def mm_tn(a, b):
    return lax.dot_general(a, b, TN, preferred_element_type=F32)


def iota(shape, dimension):
    return lax.broadcasted_iota(jnp.int32, shape, dimension)


def three_parts(value, lane):
    high = value.astype(BF16).astype(F32)
    rest = value - high
    middle = rest.astype(BF16).astype(F32)
    return jnp.where(lane < 16, high, jnp.where(lane < 32, middle, jnp.where(lane < 48, rest - middle, 0.0)))


def two_parts(value):
    high = value.astype(BF16)
    return jnp.concatenate([high, (value - high.astype(F32)).astype(BF16)], axis=1)


def weight_copies(order, offsets, pieces, target, sem, columns):
    firsts, blocks = order
    copies, waits = [], []
    for half, first, width, to in columns:
        for index, ref in enumerate(pieces[half]):
            rows = ref.shape[0] // blocks
            for place in range(blocks):
                start = offsets[firsts[half] + index * blocks + place]
                if rows % 16 == 0:
                    start = pl.multiple_of(start, 16)
                copies.append(
                    pltpu.make_async_copy(
                        ref.at[pl.ds(place * rows, rows), pl.ds(first, width)],
                        target.at[pl.ds(start, rows), pl.ds(to, width)],
                        sem,
                    )
                )
        filled = target.at[pl.ds(0, sum(ref.shape[0] for ref in pieces[half])), pl.ds(to, width)]
        waits.append(pltpu.make_async_copy(filled, filled, sem))
    return copies, waits


def start_all(group):
    for copy in group[0]:
        copy.start()


def wait_all(group):
    for copy in group[1]:
        copy.wait()


def places(core, shape, half_slot):
    row = iota(shape, 0)
    return jnp.where(row < half_slot, row + core * half_slot, row - core * half_slot)


def flags_of(core, length, bound, slot):
    lane = iota((slot, LANES), 1)
    place = places(core, (slot, LANES), slot // 2)
    second = place >= bound
    query = jnp.where(
        lane == SEG,
        jnp.where(second, 1.0, 0.0),
        jnp.where(lane == SEG + 1, jnp.where(second, 0.0, 1.0), jnp.where(lane == SEG + 2, 1.0, 0.0)),
    )
    key = jnp.where(
        lane == SEG,
        jnp.where(second, 0.0, MASKED),
        jnp.where(
            lane == SEG + 1,
            jnp.where(second, MASKED, 0.0),
            jnp.where((lane == SEG + 2) & (place >= length), MASKED, 0.0),
        ),
    )
    return lane, query, key


def pair_columns(pair, heads):
    per_half = heads // LANES
    base = (pair // per_half) * 3 * heads + (pair % per_half) * LANES
    return base, base + heads, base + 2 * heads


def load_projections(order, offsets, pieces, weights, sem, heads, downs):
    wide = 3 * heads
    columns = [(0, 0, wide, 0), (1, 0, wide, wide)]
    columns += [(0, wide, LANES, to) for to in downs]
    return weight_copies(order, offsets, pieces, weights, sem, columns)


def ups(up_refs, heads):
    blank = jnp.zeros((RANK, heads), BF16)
    parts = []
    for ref in up_refs:
        parts += [
            jnp.concatenate([ref[0] * 2, blank], axis=0),
            jnp.concatenate([blank, blank], axis=0),
            jnp.concatenate([blank, ref[1] * 2], axis=0),
        ]
    return jnp.concatenate(parts, axis=1)


def project_attend_kernel(order, n, offsets, lengths, bounds, core_ref, *refs):
    pieces = (refs[:n], refs[n : 2 * n])
    (
        x_own_ref,
        x_got_ref,
        bias_ref,
        up_own_ref,
        up_got_ref,
        qkv_ref,
        mixed_ref,
        spare_ref,
        low_ref,
        weights,
        down,
        sems,
    ) = refs[2 * n :]
    item = pl.program_id(0)
    core = core_ref[0]
    slot, width = mixed_ref.shape[1:]
    heads = width // 2

    @pl.when(item == 0)
    def _():
        wide = 3 * heads
        copies = weight_copies(order, offsets, pieces, weights, sems.at[0], [(0, 0, wide, 0), (1, 0, wide, wide)])
        downs = weight_copies(order, offsets, pieces, down, sems.at[1], [(0, wide, LANES, 0)])
        start_all(downs)
        start_all(copies)
        weights[width:] = jnp.zeros((2 * LANES, 6 * heads), BF16)
        up = ups((up_own_ref, up_got_ref), heads)
        weights[width : width + 2 * RANK] = up
        weights[width + LANES : width + LANES + 2 * RANK] = up
        wait_all(downs)
        wait_all(copies)

    x = jnp.concatenate([x_own_ref[0], x_got_ref[0]], axis=0)
    low = two_parts(mm(x, down[...]))
    low_ref[0] = low
    wide_x = jnp.concatenate([x, low], axis=1)
    for part in range(3):
        at = slice(part * width, (part + 1) * width)
        out = (mm(wide_x, weights[:, at]) + bias_ref[0:1, at]) * bias_ref[1:2, at]
        qkv_ref[0, :, at] = out.astype(BF16)

    lane, query_flags, key_flags = flags_of(core, lengths[item], bounds[item], slot)
    query_low = query_flags.astype(BF16)
    key_low = key_flags.astype(BF16)
    ones = jnp.where(lane == 0, 1.0, 0.0).astype(BF16)
    zero = jnp.zeros((slot, LANES), BF16)
    totals = jnp.ones((slot, LANES), F32)
    peaks = []
    for pair in range(width // LANES):
        at_query, at_key, at_value = pair_columns(pair, heads)
        query = qkv_ref[0, :, at_query : at_query + LANES]
        keys = jnp.concatenate([qkv_ref[0, :, at_key : at_key + LANES], key_low], axis=1)
        values = jnp.concatenate([qkv_ref[0, :, at_value : at_value + LANES], ones], axis=1)
        outs = []
        for side in range(2):
            inside = (lane < HEAD_DIM) if side == 0 else (lane >= HEAD_DIM)
            query_side = jnp.concatenate([jnp.where(inside, query, zero), query_low], axis=1)
            scores = mm_nt(keys, query_side)
            peak = jnp.max(scores, axis=0, keepdims=True)
            probs = jnp.exp(scores - peak).astype(BF16)
            out = mm_tn(probs, values)
            total = out[:, LANES : LANES + 1]
            outs.append(out[:, :LANES] * (1.0 / total))
            totals = jnp.where((lane & 15) == 2 * pair + side, total, totals)
            peaks.append(peak)
        mixed_ref[0, :, pair * LANES : (pair + 1) * LANES] = jnp.where(
            lane < HEAD_DIM, outs[0], outs[1]
        ).astype(BF16)
    peaks += [jnp.zeros((1, slot), F32)] * (16 - len(peaks))
    peaks = jnp.concatenate(peaks, axis=0)
    peaks = jnp.concatenate([peaks] * (LANES // 16), axis=0).T
    spare_ref[0] = (three_parts(peaks + jnp.log(totals), lane) + query_flags).astype(BF16)


def row_mean(value):
    return jnp.mean(value, axis=-1, keepdims=True)


def normalize(value):
    centre = value - row_mean(value)
    scale = lax.rsqrt(row_mean(centre * centre) + EPS)
    return centre * scale, scale


def normalize_back(grad, gain, normal, scale):
    grad = grad * gain
    return scale * (grad - row_mean(grad) - normal * row_mean(grad * normal))


def feed_kernel(orders, chunks, n, offsets, core_ref, *refs):
    pieces = (refs[:n], refs[n : 2 * n])
    pieces_last = (refs[2 * n : 3 * n], refs[3 * n : 4 * n])
    (
        x_own_ref,
        x_got_ref,
        mixed_ref,
        grad_own_ref,
        grad_got_ref,
        hidden_bias_ref,
        output_bias_ref,
        gain_ref,
        shift_ref,
        out_own_ref,
        out_got_ref,
        grad_hidden_ref,
        grad_mixed_ref,
        out_weights,
        in_weights,
        back_weights,
        slope,
        sems,
    ) = refs[4 * n :]
    slot, width = mixed_ref.shape[1:]
    half_slot = slot // 2
    heads = width // 2
    first, last = chunks
    size = width
    parts = list(range(0, 2 * (first + last), size))

    o = heads
    tail = 2 * first
    groups = [
        weight_copies(orders[0], offsets, pieces, out_weights, sems.at[0], [(0, 0, o, 0), (1, 0, o, o)]),
        weight_copies(orders[0], offsets, pieces, in_weights, sems.at[1], [(0, o, first, 0), (1, o, first, first)]),
        weight_copies(
            orders[0], offsets, pieces, back_weights, sems.at[2], [(0, o + first, first, 0), (1, o + first, first, first)]
        ),
        weight_copies(
            orders[1], offsets, pieces_last, in_weights, sems.at[3], [(0, 0, last, tail), (1, 0, last, tail + last)]
        ),
        weight_copies(
            orders[1], offsets, pieces_last, back_weights, sems.at[4], [(0, last, last, tail), (1, last, last, tail + last)]
        ),
    ]

    @pl.when(pl.program_id(0) == 0)
    def _():
        for group in groups:
            start_all(group)

    def arrived(*which):
        @pl.when(pl.program_id(0) == 0)
        def _():
            for index in which:
                wait_all(groups[index])

    arrived(0)
    x = jnp.concatenate([x_own_ref[0], x_got_ref[0]], axis=0).astype(F32)
    summed = x + output_bias_ref[0:1] + mm_nt(mixed_ref[0], out_weights[...])
    normal_in, scale_in = normalize(summed)
    normed = normal_in * gain_ref[0:1] + shift_ref[0:1]
    normed_low = normed.astype(BF16)
    total = normed + output_bias_ref[1:2]
    for at in parts:
        if at == 0:
            arrived(1)
        if at < tail < at + size or at == tail:
            arrived(3)
        pre = mm(normed_low, in_weights[:, at : at + size]) + hidden_bias_ref[:, at : at + size]
        share = 0.5 * (1.0 + lax.erf(pre * 0.7071067811865476))
        slope[:, at : at + size] = share + pre * jnp.exp(-0.5 * pre * pre) * 0.3989422804014327
        if at == 0:
            arrived(2)
        if at < tail < at + size or at == tail:
            arrived(4)
        total += mm_nt((pre * share).astype(BF16), back_weights[:, at : at + size])
    normal_out, scale_out = normalize(total)
    out = (normal_out * gain_ref[1:2] + shift_ref[1:2]).astype(BF16)
    out_own_ref[0] = out[:half_slot]
    out_got_ref[0] = out[half_slot:]
    grad = jnp.concatenate([grad_own_ref[0], grad_got_ref[0]], axis=0).astype(F32)
    grad_total = normalize_back(grad, gain_ref[1:2], normal_out, scale_out)
    grad_low = grad_total.astype(BF16)
    grad_normed = grad_total
    for at in parts:
        grad_pre = (mm(grad_low, back_weights[:, at : at + size]) * slope[:, at : at + size]).astype(BF16)
        grad_normed += mm_nt(grad_pre, in_weights[:, at : at + size])
    grad_hidden = normalize_back(grad_normed, gain_ref[0:1], normal_in, scale_in)
    grad_hidden_ref[0] = grad_hidden
    grad_mixed_ref[0] = mm(grad_hidden.astype(BF16), out_weights[...]).astype(BF16)


def attend_back_kernel(lengths, bounds, core_ref, *refs):
    (
        qkv_ref,
        mixed_ref,
        spare_ref,
        low_ref,
        grad_mixed_ref,
        grads_ref,
        adapter_ref,
    ) = refs
    item = pl.program_id(0)
    core = core_ref[0]
    slot, width = mixed_ref.shape[1:]
    heads = width // 2

    lane, _, key_flags = flags_of(core, lengths[item], bounds[item], slot)
    row = iota((width, LANES), 0)
    column = iota((width, LANES), 1)
    pick = jnp.where((row // HEAD_DIM == (column & 15)) & (column < 48), 1.0, 0.0).astype(BF16)
    product = grad_mixed_ref[0].astype(F32) * mixed_ref[0].astype(F32)
    high = product.astype(BF16)
    rest = (product - high.astype(F32)).astype(BF16)
    inner = three_parts(mm(high, pick) + mm(rest, pick), lane).astype(BF16)
    spare = spare_ref[0]
    zero = jnp.zeros((slot, LANES), BF16)
    per_half = heads // LANES

    def columns(first):
        return pl.ds(pl.multiple_of(first, LANES), LANES)

    def of_pair(pair):
        base = (pair // per_half) * 3 * heads + (pair % per_half) * LANES
        at_query, at_key, at_value = (columns(base + part * heads) for part in range(3))
        query = qkv_ref[0, :, at_query]
        keys = qkv_ref[0, :, at_key]
        values = qkv_ref[0, :, at_value]
        grad = grad_mixed_ref[0, :, columns(pair * LANES)]
        total_query = jnp.zeros((slot, LANES), F32)
        total_key = jnp.zeros((slot, LANES), F32)
        total_value = jnp.zeros((slot, LANES), F32)
        for side in range(2):
            head = 2 * pair + side
            inside = (lane < HEAD_DIM) if side == 0 else (lane >= HEAD_DIM)
            mine = ((lane & 15) == head) & (lane < 48)
            query_side = jnp.where(inside, query, zero)
            key_side = jnp.where(inside, keys, zero)
            grad_side = jnp.where(inside, grad, zero)
            key_wide = jnp.concatenate([keys, jnp.where(mine, -1.0, key_flags).astype(BF16)], axis=1)
            value_wide = jnp.concatenate([values, jnp.where(mine, -1.0, 0.0).astype(BF16)], axis=1)
            probs = jnp.exp(mm_nt(key_wide, jnp.concatenate([query_side, spare], axis=1)))
            grad_probs = mm_nt(value_wide, jnp.concatenate([grad_side, inner], axis=1))
            grad_scores = (probs * grad_probs).astype(BF16)
            total_value += mm(probs.astype(BF16), grad_side)
            total_key += mm(grad_scores, query_side)
            total_query += mm_tn(grad_scores, key_side)
        grads_ref[0, :, at_query] = (total_query * 0.125).astype(BF16)
        grads_ref[0, :, at_key] = total_key.astype(BF16)
        grads_ref[0, :, at_value] = total_value.astype(BF16)

    pairs = width // LANES
    group = 3 if pairs % 3 == 0 else 1

    @pl.loop(0, pairs // group)
    def _(step):
        for place in range(group):
            of_pair(step * group + place)

    update = 2.0 * mm_tn(low_ref[0], grads_ref[0])
    parts = []
    for half in range(2):
        at = half * 3 * heads
        of_query = update[:, at : at + heads]
        of_value = update[:, at + 2 * heads : at + 3 * heads]
        rows = [
            of_query[:RANK] + of_query[LANES : LANES + RANK],
            of_value[RANK : 2 * RANK] + of_value[LANES + RANK : LANES + 2 * RANK],
        ]
        parts.append(jnp.concatenate(rows, axis=0))
    part = jnp.concatenate(parts, axis=1)

    @pl.when(item == 0)
    def _():
        adapter_ref[...] = part

    @pl.when(item > 0)
    def _():
        adapter_ref[...] += part


def input_grad_kernel(order, n, offsets, core_ref, *refs):
    pieces = (refs[:n], refs[n : 2 * n])
    (
        grads_ref,
        grad_hidden_ref,
        up_own_ref,
        up_got_ref,
        own_ref,
        got_ref,
        weights,
        up,
        sems,
    ) = refs[2 * n :]
    slot, width = grad_hidden_ref.shape[1:]
    heads = width // 2

    @pl.when(pl.program_id(0) == 0)
    def _():
        copies = load_projections(order, offsets, pieces, weights, sems.at[0], heads, (6 * heads, 6 * heads + LANES))
        start_all(copies)
        up[...] = jnp.zeros_like(up)
        up[: 2 * RANK] = ups((up_own_ref, up_got_ref), heads)
        wait_all(copies)

    grads = grads_ref[0]
    small = two_parts(mm_nt(grads, up[...]))
    total = grad_hidden_ref[0] + mm_nt(jnp.concatenate([grads, small], axis=1), weights[...])
    own_ref[0] = total[: slot // 2]
    got_ref[0] = total[slot // 2 :]


def any_spec():
    return pl.BlockSpec(memory_space=pl.ANY)


def whole_spec(array):
    return pl.BlockSpec(array.shape, lambda i, *_: (0,) * array.ndim)


def item_spec(shape):
    return pl.BlockSpec((1, *shape[1:]), lambda i, *_: (i, 0, 0))


def shape_of(shape, dtype):
    return jax.ShapeDtypeStruct(shape, dtype)


def call(kernel, name, scalars, flat, args, outs, scratch, items, flops, moved):
    return pl.pallas_call(
        kernel,
        grid_spec=pltpu.PrefetchScalarGridSpec(
            num_scalar_prefetch=len(scalars),
            grid=(items,),
            in_specs=[any_spec()] * len(flat) + [spec for _, spec in args],
            out_specs=[spec for _, spec in outs],
            scratch_shapes=scratch,
        ),
        out_shape=[shape for shape, _ in outs],
        compiler_params=pltpu.CompilerParams(vmem_limit_bytes=VMEM_LIMIT),
        cost_estimate=pl.CostEstimate(flops=flops, bytes_accessed=moved, transcendentals=0),
        name=name,
    )(*scalars, *flat, *[array for array, _ in args])


def swap(array):
    return lax.ppermute(array, "tensor", [(0, 1), (1, 0)])


def after(value, *deps):
    return lax.optimization_barrier((value, *deps))[0]


def over_dp(count, array, target):
    return lax.ppermute(array, "dp", [(i, target(i)) for i in range(count)])


LINE_FIRST = ((4, 8, 1, 2), (8, 4, 2, 1))
PLANE_FIRST = ((1, 2, 4, 8), (2, 1, 8, 4))


def block_offsets(index, rows, flips):
    place = jnp.arange(16)
    flipped = sum(((place >> bit) & 1) * flips[bit] for bit in range(4))
    return ((index ^ flipped) * rows).astype(jnp.int32)


def local(
    inputs,
    lengths,
    bounds,
    query_matrix,
    key_matrix,
    value_matrix,
    query_value_bias,
    adapter_down_weight,
    adapter_up_weight,
    attention_output_weight,
    feedforward_input_weight,
    feedforward_input_bias,
    feedforward_output_weight,
    output_bias,
    layernorm_scale,
    layernorm_bias,
    output_gradient,
    *,
    count,
):
    micro, rows, width = inputs.shape
    mine = micro // 2
    slot = 2 * rows
    heads = width // 2
    core = lax.axis_index("tensor")
    shard_rows = query_matrix.shape[0]
    hidden = feedforward_input_weight.shape[1]
    last = hidden // 3 if count == 16 else hidden // 2
    first = hidden - last

    blank = jnp.zeros((shard_rows, LANES - 2 * RANK), BF16)
    down = [adapter_down_weight[0], adapter_down_weight[1], blank]
    shard = jnp.concatenate([query_matrix, key_matrix, value_matrix, *down], axis=1)
    back = feedforward_output_weight.T
    shard_first = jnp.concatenate(
        [attention_output_weight.T, feedforward_input_weight[:, :first], back[:, :first]], axis=1
    )
    shard_last = jnp.concatenate([feedforward_input_weight[:, first:], back[:, first:]], axis=1)

    others = (1 - core) * mine
    x_got = swap(lax.dynamic_slice_in_dim(inputs, others, mine, 0))
    grad_got = swap(lax.dynamic_slice_in_dim(output_gradient, others, mine, 0))
    bias_got, up_got, hidden_bias_got = map(swap, (query_value_bias, adapter_up_weight, feedforward_input_bias))

    blank = jnp.zeros((heads,), F32)
    ones = blank + 1
    both = [query_value_bias[0], blank, query_value_bias[1], bias_got[0], blank, bias_got[1]]
    scale = [ones * 0.125, ones, ones] * 2
    bias = jnp.stack([jnp.concatenate(both), jnp.concatenate(scale)])

    if count == 16:
        index = lax.axis_index("dp")

        def tables(flips):
            mine_first = [jnp.where(core == 0, a, b) for a, b in zip(*flips, strict=True)]
            other_first = [jnp.where(core == 0, b, a) for a, b in zip(*flips, strict=True)]
            return [block_offsets(index, shard_rows, f) for f in (mine_first, other_first)]

        offsets = jnp.concatenate(tables(LINE_FIRST) + tables(PLANE_FIRST))
        order, order_last, n = ((0, 16), 8), ((32, 48), 8), 2

        def exchange(array, flips, step):
            pairs = [(2 * i + t, 2 * (i ^ flips[t][step]) + t) for i in range(count) for t in range(2)]
            return lax.ppermute(array, ("dp", "tensor"), pairs)

        def joined(*arrays):
            return jnp.concatenate(arrays, axis=0)

        shard, shard_last = lax.optimization_barrier((shard, after(shard_last, shard)))
        line = joined(shard, exchange(shard, LINE_FIRST, 0))
        plane = joined(shard_last, exchange(shard_last, PLANE_FIRST, 0))
        line = joined(line, exchange(line, LINE_FIRST, 1))
        plane = joined(plane, exchange(plane, PLANE_FIRST, 1))
        line, plane, *early = lax.optimization_barrier((line, plane, x_got, up_got, grad_got, hidden_bias_got, offsets, bias))
        x_got, up_got, grad_got, hidden_bias_got, offsets, bias = early
        shard_first = after(shard_first, line)
        line_first = joined(shard_first, exchange(shard_first, LINE_FIRST, 0))
        line = joined(line, exchange(line, LINE_FIRST, 2))
        line_first = after(line_first, line)
        line_first = joined(line_first, exchange(line_first, LINE_FIRST, 1))
        own = [line, exchange(line, LINE_FIRST, 3)]
        swapped = [swap(line)]
        line_first, plane, own, swapped = lax.optimization_barrier((line_first, plane, own, swapped))
        swapped.append(swap(own[1]))
        line_first = joined(line_first, exchange(line_first, LINE_FIRST, 2))
        plane = joined(plane, exchange(plane, PLANE_FIRST, 2))
        plane, line_first, x_got = lax.optimization_barrier((plane, line_first, x_got))
        own_first = [line_first, exchange(line_first, LINE_FIRST, 3)]
        own_last = [plane, exchange(plane, PLANE_FIRST, 3)]
        got_first, got_last = [swap(line_first)], [swap(plane)]
    else:
        offsets = jnp.zeros((2,), jnp.int32)
        order = order_last = ((0, 0), 1)
        n = 1
        own, own_first, own_last = (
            [lax.all_gather(s, "dp", axis=0, tiled=True)] for s in (shard, shard_first, shard_last)
        )
        swapped, got_first, got_last = [swap(own[0])], [], []
    pieces = (*own, *swapped)

    first_item = core * mine
    my_lengths = lax.dynamic_slice_in_dim(lengths[:, 0], first_item, mine, 0)
    my_bounds = lax.dynamic_slice_in_dim(bounds[:, 0], first_item, mine, 0)
    core = core[None].astype(jnp.int32)

    own_block = pl.BlockSpec((1, rows, width), lambda i, *s: (s[-1][0] * mine + i, 0, 0))
    got_block = pl.BlockSpec((1, rows, width), lambda i, *_: (i, 0, 0))
    item = (mine, slot, width)
    wide = (mine, slot, 3 * width)

    def out_item(shape, dtype):
        return shape_of(shape, dtype), item_spec(shape)

    def in_item(array):
        return array, item_spec(array.shape)

    def in_whole(array):
        return array, whole_spec(array)

    split_out = lambda dtype: [(shape_of(inputs.shape, dtype), own_block), (shape_of((mine, rows, width), dtype), got_block)]

    tokens = mine * slot
    qkv, mixed, spare, low = call(
        functools.partial(project_attend_kernel, order, n),
        "project_attend",
        (offsets, my_lengths, my_bounds, core),
        pieces,
        [(inputs, own_block), (x_got, got_block), in_whole(bias), in_whole(adapter_up_weight), in_whole(up_got)],
        [
            out_item(wide, BF16),
            out_item(item, BF16),
            out_item((mine, slot, LANES), BF16),
            out_item((mine, slot, 2 * LANES), BF16),
        ],
        [
            pltpu.VMEM((width + 2 * LANES, 3 * width), BF16),
            pltpu.VMEM((width, LANES), BF16),
            pltpu.SemaphoreType.DMA((2,)),
        ],
        mine,
        2 * tokens * width * (4 * width + 8 * slot),
        12 * tokens * width,
    )
    own_first, own_last = lax.optimization_barrier((own_first, own_last, mixed))[:2]
    got_first += map(swap, own_first[len(got_first) :])
    got_last += map(swap, own_last[len(got_last) :])
    hidden_bias = jnp.concatenate(
        [
            feedforward_input_bias[:first],
            hidden_bias_got[:first],
            feedforward_input_bias[first:],
            hidden_bias_got[first:],
        ]
    )[None]
    pieces_feed = (*own_first, *got_first, *own_last, *got_last)
    out, out_send, grad_hidden, grad_mixed = call(
        functools.partial(feed_kernel, (order, order_last), (first, last), n),
        "feed",
        (offsets, core),
        pieces_feed,
        [
            (inputs, own_block),
            (x_got, got_block),
            in_item(mixed),
            (output_gradient, own_block),
            (grad_got, got_block),
            *map(in_whole, (hidden_bias, output_bias, layernorm_scale, layernorm_bias)),
        ],
        [*split_out(BF16), out_item(item, F32), out_item(item, BF16)],
        [
            pltpu.VMEM((width, width), BF16),
            pltpu.VMEM((width, 2 * hidden), BF16),
            pltpu.VMEM((width, 2 * hidden), BF16),
            pltpu.VMEM((slot, 2 * hidden), F32),
            pltpu.SemaphoreType.DMA((5,)),
        ],
        mine,
        4 * tokens * width * (width + 4 * hidden),
        8 * width * hidden,
    )
    out_send = swap(out_send)
    adapter = (2 * RANK, width)
    grads, adapter = call(
        attend_back_kernel,
        "attend_back",
        (my_lengths, my_bounds, core),
        (),
        [*map(in_item, (qkv, mixed, spare, low, grad_mixed))],
        [out_item(wide, BF16), (shape_of(adapter, F32), pl.BlockSpec(adapter, lambda i, *_: (0, 0)))],
        [],
        mine,
        2 * tokens * width * 20 * slot,
        16 * tokens * width,
    )
    if count == 16:
        ways = [over_dp(count, adapter, lambda i, flip=flip: i ^ flip) for flip in (4, 8, 12)]
    total, total_send = call(
        functools.partial(input_grad_kernel, order, n),
        "input_grad",
        (offsets, core),
        pieces,
        [in_item(grads), in_item(grad_hidden), in_whole(adapter_up_weight), in_whole(up_got)],
        split_out(F32),
        [
            pltpu.VMEM((width, 3 * width + 2 * LANES), BF16),
            pltpu.VMEM((LANES, 3 * width), BF16),
            pltpu.SemaphoreType.DMA((1,)),
        ],
        mine,
        2 * tokens * width * 3 * width,
        12 * tokens * width,
    )
    if count == 16:
        *ways, total_send, out = lax.optimization_barrier((*ways, total_send, out))
        adapter = (adapter + ways[0]) + (ways[1] + ways[2])
        ways = [over_dp(count, adapter, lambda i, flip=flip: i ^ flip) for flip in (1, 2, 3)]
        input_grad = lax.dynamic_update_slice_in_dim(total, swap(total_send), others, 0)
        result = lax.dynamic_update_slice_in_dim(out, out_send, others, 0)
        *ways, input_grad, result = lax.optimization_barrier((*ways, input_grad, result))
        adapter = (adapter + ways[0]) + (ways[1] + ways[2])
    else:
        adapter = lax.psum(adapter, "dp")
        input_grad = lax.dynamic_update_slice_in_dim(total, swap(total_send), others, 0)
        result = lax.dynamic_update_slice_in_dim(out, out_send, others, 0)
    adapter = adapter[:, :heads] + swap(adapter[:, heads:])
    return result, input_grad, adapter.reshape(2, RANK, heads)


def solution(mesh):
    return jax.shard_map(
        functools.partial(local, count=mesh.shape["dp"]),
        mesh=mesh,
        in_specs=(
            P(None, ("dp", "tensor"), None),
            P(None, "dp"),
            P(None, "dp"),
            P("dp", "tensor"),
            P("dp", "tensor"),
            P("dp", "tensor"),
            P(None, "tensor"),
            P(None, "dp", None),
            P(None, None, "tensor"),
            P("tensor", "dp"),
            P("dp", "tensor"),
            P("tensor"),
            P("tensor", "dp"),
            P(),
            P(),
            P(),
            P(None, ("dp", "tensor"), None),
        ),
        out_specs=(
            P(None, ("dp", "tensor"), None),
            P(None, ("dp", "tensor"), None),
            P(None, None, "tensor"),
        ),
        check_vma=False,
    )
```

```python
import functools

import jax
import jax.numpy as jnp
from jax import lax
from jax.experimental import pallas as pl
from jax.experimental.pallas import tpu as pltpu
from jax.sharding import PartitionSpec as P

F32 = jnp.float32
BF16 = jnp.bfloat16
HEAD_DIM = 64
RANK = 8
LANES = 128
EPS = 1e-05
MASKED = -float(2**30)
SEG = 64
VMEM_LIMIT = 60 * 2**20

NT = (((1,), (1,)), ((), ()))
TN = (((0,), (0,)), ((), ()))


def mm(a, b):
    return jnp.dot(a, b, preferred_element_type=F32)


def mm_nt(a, b):
    return lax.dot_general(a, b, NT, preferred_element_type=F32)


def mm_tn(a, b):
    return lax.dot_general(a, b, TN, preferred_element_type=F32)


def iota(shape, dimension):
    return lax.broadcasted_iota(jnp.int32, shape, dimension)


def three_parts(value, lane):
    high = value.astype(BF16).astype(F32)
    rest = value - high
    middle = rest.astype(BF16).astype(F32)
    return jnp.where(lane < 16, high, jnp.where(lane < 32, middle, jnp.where(lane < 48, rest - middle, 0.0)))


def two_parts(value):
    high = value.astype(BF16)
    return jnp.concatenate([high, (value - high.astype(F32)).astype(BF16)], axis=1)


def weight_copies(order, offsets, pieces, target, sem, columns):
    firsts, blocks = order
    copies, waits = [], []
    for half, first, width, to in columns:
        for index, ref in enumerate(pieces[half]):
            rows = ref.shape[0] // blocks
            for place in range(blocks):
                start = offsets[firsts[half] + index * blocks + place]
                if rows % 16 == 0:
                    start = pl.multiple_of(start, 16)
                copies.append(
                    pltpu.make_async_copy(
                        ref.at[pl.ds(place * rows, rows), pl.ds(first, width)],
                        target.at[pl.ds(start, rows), pl.ds(to, width)],
                        sem,
                    )
                )
        filled = target.at[pl.ds(0, sum(ref.shape[0] for ref in pieces[half])), pl.ds(to, width)]
        waits.append(pltpu.make_async_copy(filled, filled, sem))
    return copies, waits


def start_all(group):
    for copy in group[0]:
        copy.start()


def wait_all(group):
    for copy in group[1]:
        copy.wait()


def places(core, shape, half_slot):
    row = iota(shape, 0)
    return jnp.where(row < half_slot, row + core * half_slot, row - core * half_slot)


def flags_of(core, length, bound, slot):
    lane = iota((slot, LANES), 1)
    place = places(core, (slot, LANES), slot // 2)
    second = place >= bound
    query = jnp.where(
        lane == SEG,
        jnp.where(second, 1.0, 0.0),
        jnp.where(lane == SEG + 1, jnp.where(second, 0.0, 1.0), jnp.where(lane == SEG + 2, 1.0, 0.0)),
    )
    key = jnp.where(
        lane == SEG,
        jnp.where(second, 0.0, MASKED),
        jnp.where(
            lane == SEG + 1,
            jnp.where(second, MASKED, 0.0),
            jnp.where((lane == SEG + 2) & (place >= length), MASKED, 0.0),
        ),
    )
    return lane, query, key


def pair_columns(pair, heads):
    per_half = heads // LANES
    base = (pair // per_half) * 3 * heads + (pair % per_half) * LANES
    return base, base + heads, base + 2 * heads


def load_projections(order, offsets, pieces, weights, sem, heads, downs):
    wide = 3 * heads
    columns = [(0, 0, wide, 0), (1, 0, wide, wide)]
    columns += [(0, wide, LANES, to) for to in downs]
    return weight_copies(order, offsets, pieces, weights, sem, columns)


def ups(up_refs, heads):
    blank = jnp.zeros((RANK, heads), BF16)
    parts = []
    for ref in up_refs:
        parts += [
            jnp.concatenate([ref[0] * 2, blank], axis=0),
            jnp.concatenate([blank, blank], axis=0),
            jnp.concatenate([blank, ref[1] * 2], axis=0),
        ]
    return jnp.concatenate(parts, axis=1)


def project_attend_kernel(order, n, offsets, lengths, bounds, core_ref, *refs):
    pieces = (refs[:n], refs[n : 2 * n])
    (
        x_own_ref,
        x_got_ref,
        bias_ref,
        up_own_ref,
        up_got_ref,
        qkv_ref,
        mixed_ref,
        spare_ref,
        low_ref,
        weights,
        down,
        sems,
    ) = refs[2 * n :]
    item = pl.program_id(0)
    core = core_ref[0]
    slot, width = mixed_ref.shape[1:]
    heads = width // 2

    @pl.when(item == 0)
    def _():
        wide = 3 * heads
        copies = weight_copies(order, offsets, pieces, weights, sems.at[0], [(0, 0, wide, 0), (1, 0, wide, wide)])
        downs = weight_copies(order, offsets, pieces, down, sems.at[1], [(0, wide, LANES, 0)])
        start_all(downs)
        start_all(copies)
        weights[width:] = jnp.zeros((2 * LANES, 6 * heads), BF16)
        up = ups((up_own_ref, up_got_ref), heads)
        weights[width : width + 2 * RANK] = up
        weights[width + LANES : width + LANES + 2 * RANK] = up
        wait_all(downs)
        wait_all(copies)

    x = jnp.concatenate([x_own_ref[0], x_got_ref[0]], axis=0)
    low = two_parts(mm(x, down[...]))
    low_ref[0] = low
    wide_x = jnp.concatenate([x, low], axis=1)
    for part in range(3):
        at = slice(part * width, (part + 1) * width)
        out = (mm(wide_x, weights[:, at]) + bias_ref[0:1, at]) * bias_ref[1:2, at]
        qkv_ref[0, :, at] = out.astype(BF16)

    lane, query_flags, key_flags = flags_of(core, lengths[item], bounds[item], slot)
    query_low = query_flags.astype(BF16)
    key_low = key_flags.astype(BF16)
    ones = jnp.where(lane == 0, 1.0, 0.0).astype(BF16)
    zero = jnp.zeros((slot, LANES), BF16)
    totals = jnp.ones((slot, LANES), F32)
    peaks = []
    for pair in range(width // LANES):
        at_query, at_key, at_value = pair_columns(pair, heads)
        query = qkv_ref[0, :, at_query : at_query + LANES]
        keys = jnp.concatenate([qkv_ref[0, :, at_key : at_key + LANES], key_low], axis=1)
        values = jnp.concatenate([qkv_ref[0, :, at_value : at_value + LANES], ones], axis=1)
        outs = []
        for side in range(2):
            inside = (lane < HEAD_DIM) if side == 0 else (lane >= HEAD_DIM)
            query_side = jnp.concatenate([jnp.where(inside, query, zero), query_low], axis=1)
            scores = mm_nt(keys, query_side)
            peak = jnp.max(scores, axis=0, keepdims=True)
            probs = jnp.exp(scores - peak).astype(BF16)
            out = mm_tn(probs, values)
            total = out[:, LANES : LANES + 1]
            outs.append(out[:, :LANES] * (1.0 / total))
            totals = jnp.where((lane & 15) == 2 * pair + side, total, totals)
            peaks.append(peak)
        mixed_ref[0, :, pair * LANES : (pair + 1) * LANES] = jnp.where(
            lane < HEAD_DIM, outs[0], outs[1]
        ).astype(BF16)
    peaks += [jnp.zeros((1, slot), F32)] * (16 - len(peaks))
    peaks = jnp.concatenate(peaks, axis=0)
    peaks = jnp.concatenate([peaks] * (LANES // 16), axis=0).T
    spare_ref[0] = (three_parts(peaks + jnp.log(totals), lane) + query_flags).astype(BF16)


def row_mean(value):
    return jnp.mean(value, axis=-1, keepdims=True)


def normalize(value):
    centre = value - row_mean(value)
    scale = lax.rsqrt(row_mean(centre * centre) + EPS)
    return centre * scale, scale


def normalize_back(grad, gain, normal, scale):
    grad = grad * gain
    return scale * (grad - row_mean(grad) - normal * row_mean(grad * normal))


def feed_kernel(orders, chunks, n, offsets, core_ref, *refs):
    pieces = (refs[:n], refs[n : 2 * n])
    pieces_last = (refs[2 * n : 3 * n], refs[3 * n : 4 * n])
    (
        x_own_ref,
        x_got_ref,
        mixed_ref,
        grad_own_ref,
        grad_got_ref,
        hidden_bias_ref,
        output_bias_ref,
        gain_ref,
        shift_ref,
        out_own_ref,
        out_got_ref,
        grad_hidden_ref,
        grad_mixed_ref,
        out_weights,
        in_weights,
        back_weights,
        slope,
        sems,
    ) = refs[4 * n :]
    slot, width = mixed_ref.shape[1:]
    half_slot = slot // 2
    heads = width // 2
    first, last = chunks
    size = width
    parts = list(range(0, 2 * (first + last), size))

    o = heads
    tail = 2 * first
    groups = [
        weight_copies(orders[0], offsets, pieces, out_weights, sems.at[0], [(0, 0, o, 0), (1, 0, o, o)]),
        weight_copies(orders[0], offsets, pieces, in_weights, sems.at[1], [(0, o, first, 0), (1, o, first, first)]),
        weight_copies(
            orders[0], offsets, pieces, back_weights, sems.at[2], [(0, o + first, first, 0), (1, o + first, first, first)]
        ),
        weight_copies(
            orders[1], offsets, pieces_last, in_weights, sems.at[3], [(0, 0, last, tail), (1, 0, last, tail + last)]
        ),
        weight_copies(
            orders[1], offsets, pieces_last, back_weights, sems.at[4], [(0, last, last, tail), (1, last, last, tail + last)]
        ),
    ]

    @pl.when(pl.program_id(0) == 0)
    def _():
        for group in groups:
            start_all(group)

    def arrived(*which):
        @pl.when(pl.program_id(0) == 0)
        def _():
            for index in which:
                wait_all(groups[index])

    arrived(0)
    x = jnp.concatenate([x_own_ref[0], x_got_ref[0]], axis=0).astype(F32)
    summed = x + output_bias_ref[0:1] + mm_nt(mixed_ref[0], out_weights[...])
    normal_in, scale_in = normalize(summed)
    normed = normal_in * gain_ref[0:1] + shift_ref[0:1]
    normed_low = normed.astype(BF16)
    total = normed + output_bias_ref[1:2]
    for at in parts:
        if at == 0:
            arrived(1)
        if at < tail < at + size or at == tail:
            arrived(3)
        pre = mm(normed_low, in_weights[:, at : at + size]) + hidden_bias_ref[:, at : at + size]
        share = 0.5 * (1.0 + lax.erf(pre * 0.7071067811865476))
        slope[:, at : at + size] = share + pre * jnp.exp(-0.5 * pre * pre) * 0.3989422804014327
        if at == 0:
            arrived(2)
        if at < tail < at + size or at == tail:
            arrived(4)
        total += mm_nt((pre * share).astype(BF16), back_weights[:, at : at + size])
    normal_out, scale_out = normalize(total)
    out = (normal_out * gain_ref[1:2] + shift_ref[1:2]).astype(BF16)
    out_own_ref[0] = out[:half_slot]
    out_got_ref[0] = out[half_slot:]
    grad = jnp.concatenate([grad_own_ref[0], grad_got_ref[0]], axis=0).astype(F32)
    grad_total = normalize_back(grad, gain_ref[1:2], normal_out, scale_out)
    grad_low = grad_total.astype(BF16)
    grad_normed = grad_total
    for at in parts:
        grad_pre = (mm(grad_low, back_weights[:, at : at + size]) * slope[:, at : at + size]).astype(BF16)
        grad_normed += mm_nt(grad_pre, in_weights[:, at : at + size])
    grad_hidden = normalize_back(grad_normed, gain_ref[0:1], normal_in, scale_in)
    grad_hidden_ref[0] = grad_hidden
    grad_mixed_ref[0] = mm(grad_hidden.astype(BF16), out_weights[...]).astype(BF16)


def attend_back_kernel(lengths, bounds, core_ref, *refs):
    (
        qkv_ref,
        mixed_ref,
        spare_ref,
        low_ref,
        grad_mixed_ref,
        grads_ref,
        adapter_ref,
    ) = refs
    item = pl.program_id(0)
    core = core_ref[0]
    slot, width = mixed_ref.shape[1:]
    heads = width // 2

    lane, _, key_flags = flags_of(core, lengths[item], bounds[item], slot)
    row = iota((width, LANES), 0)
    column = iota((width, LANES), 1)
    pick = jnp.where((row // HEAD_DIM == (column & 15)) & (column < 48), 1.0, 0.0).astype(BF16)
    product = grad_mixed_ref[0].astype(F32) * mixed_ref[0].astype(F32)
    high = product.astype(BF16)
    rest = (product - high.astype(F32)).astype(BF16)
    inner = three_parts(mm(high, pick) + mm(rest, pick), lane).astype(BF16)
    spare = spare_ref[0]
    zero = jnp.zeros((slot, LANES), BF16)
    per_half = heads // LANES

    def columns(first):
        return pl.ds(pl.multiple_of(first, LANES), LANES)

    def of_pair(pair):
        base = (pair // per_half) * 3 * heads + (pair % per_half) * LANES
        at_query, at_key, at_value = (columns(base + part * heads) for part in range(3))
        query = qkv_ref[0, :, at_query]
        keys = qkv_ref[0, :, at_key]
        values = qkv_ref[0, :, at_value]
        grad = grad_mixed_ref[0, :, columns(pair * LANES)]
        total_query = jnp.zeros((slot, LANES), F32)
        total_key = jnp.zeros((slot, LANES), F32)
        total_value = jnp.zeros((slot, LANES), F32)
        for side in range(2):
            head = 2 * pair + side
            inside = (lane < HEAD_DIM) if side == 0 else (lane >= HEAD_DIM)
            mine = ((lane & 15) == head) & (lane < 48)
            query_side = jnp.where(inside, query, zero)
            key_side = jnp.where(inside, keys, zero)
            grad_side = jnp.where(inside, grad, zero)
            key_wide = jnp.concatenate([keys, jnp.where(mine, -1.0, key_flags).astype(BF16)], axis=1)
            value_wide = jnp.concatenate([values, jnp.where(mine, -1.0, 0.0).astype(BF16)], axis=1)
            probs = jnp.exp(mm_nt(key_wide, jnp.concatenate([query_side, spare], axis=1)))
            grad_probs = mm_nt(value_wide, jnp.concatenate([grad_side, inner], axis=1))
            grad_scores = (probs * grad_probs).astype(BF16)
            total_value += mm(probs.astype(BF16), grad_side)
            total_key += mm(grad_scores, query_side)
            total_query += mm_tn(grad_scores, key_side)
        grads_ref[0, :, at_query] = (total_query * 0.125).astype(BF16)
        grads_ref[0, :, at_key] = total_key.astype(BF16)
        grads_ref[0, :, at_value] = total_value.astype(BF16)

    pairs = width // LANES
    group = 3 if pairs % 3 == 0 else 1

    @pl.loop(0, pairs // group)
    def _(step):
        for place in range(group):
            of_pair(step * group + place)

    update = 2.0 * mm_tn(low_ref[0], grads_ref[0])
    parts = []
    for half in range(2):
        at = half * 3 * heads
        of_query = update[:, at : at + heads]
        of_value = update[:, at + 2 * heads : at + 3 * heads]
        rows = [
            of_query[:RANK] + of_query[LANES : LANES + RANK],
            of_value[RANK : 2 * RANK] + of_value[LANES + RANK : LANES + 2 * RANK],
        ]
        parts.append(jnp.concatenate(rows, axis=0))
    part = jnp.concatenate(parts, axis=1)

    @pl.when(item == 0)
    def _():
        adapter_ref[...] = part

    @pl.when(item > 0)
    def _():
        adapter_ref[...] += part


def input_grad_kernel(order, n, offsets, core_ref, *refs):
    pieces = (refs[:n], refs[n : 2 * n])
    (
        grads_ref,
        grad_hidden_ref,
        up_own_ref,
        up_got_ref,
        own_ref,
        got_ref,
        weights,
        up,
        sems,
    ) = refs[2 * n :]
    slot, width = grad_hidden_ref.shape[1:]
    heads = width // 2

    @pl.when(pl.program_id(0) == 0)
    def _():
        copies = load_projections(order, offsets, pieces, weights, sems.at[0], heads, (6 * heads, 6 * heads + LANES))
        start_all(copies)
        up[...] = jnp.zeros_like(up)
        up[: 2 * RANK] = ups((up_own_ref, up_got_ref), heads)
        wait_all(copies)

    grads = grads_ref[0]
    small = two_parts(mm_nt(grads, up[...]))
    total = grad_hidden_ref[0] + mm_nt(jnp.concatenate([grads, small], axis=1), weights[...])
    own_ref[0] = total[: slot // 2]
    got_ref[0] = total[slot // 2 :]


def any_spec():
    return pl.BlockSpec(memory_space=pl.ANY)


def whole_spec(array):
    return pl.BlockSpec(array.shape, lambda i, *_: (0,) * array.ndim)


def item_spec(shape):
    return pl.BlockSpec((1, *shape[1:]), lambda i, *_: (i, 0, 0))


def shape_of(shape, dtype):
    return jax.ShapeDtypeStruct(shape, dtype)


def call(kernel, name, scalars, flat, args, outs, scratch, items, flops, moved):
    return pl.pallas_call(
        kernel,
        grid_spec=pltpu.PrefetchScalarGridSpec(
            num_scalar_prefetch=len(scalars),
            grid=(items,),
            in_specs=[any_spec()] * len(flat) + [spec for _, spec in args],
            out_specs=[spec for _, spec in outs],
            scratch_shapes=scratch,
        ),
        out_shape=[shape for shape, _ in outs],
        compiler_params=pltpu.CompilerParams(vmem_limit_bytes=VMEM_LIMIT),
        cost_estimate=pl.CostEstimate(flops=flops, bytes_accessed=moved, transcendentals=0),
        name=name,
    )(*scalars, *flat, *[array for array, _ in args])


def swap(array):
    return lax.ppermute(array, "tensor", [(0, 1), (1, 0)])


def after(value, *deps):
    return lax.optimization_barrier((value, *deps))[0]


def over_dp(count, array, target):
    return lax.ppermute(array, "dp", [(i, target(i)) for i in range(count)])


LINE_FIRST = ((4, 8, 1, 2), (8, 4, 2, 1))
PLANE_FIRST = ((1, 2, 4, 8), (2, 1, 8, 4))


def block_offsets(index, rows, flips):
    place = jnp.arange(16)
    flipped = sum(((place >> bit) & 1) * flips[bit] for bit in range(4))
    return ((index ^ flipped) * rows).astype(jnp.int32)


def local(
    inputs,
    lengths,
    bounds,
    query_matrix,
    key_matrix,
    value_matrix,
    query_value_bias,
    adapter_down_weight,
    adapter_up_weight,
    attention_output_weight,
    feedforward_input_weight,
    feedforward_input_bias,
    feedforward_output_weight,
    output_bias,
    layernorm_scale,
    layernorm_bias,
    output_gradient,
    *,
    count,
):
    micro, rows, width = inputs.shape
    mine = micro // 2
    slot = 2 * rows
    heads = width // 2
    core = lax.axis_index("tensor")
    shard_rows = query_matrix.shape[0]
    hidden = feedforward_input_weight.shape[1]
    last = hidden // 3 if count == 16 else hidden // 2
    first = hidden - last

    blank = jnp.zeros((shard_rows, LANES - 2 * RANK), BF16)
    down = [adapter_down_weight[0], adapter_down_weight[1], blank]
    shard = jnp.concatenate([query_matrix, key_matrix, value_matrix, *down], axis=1)
    back = feedforward_output_weight.T
    shard_first = jnp.concatenate(
        [attention_output_weight.T, feedforward_input_weight[:, :first], back[:, :first]], axis=1
    )
    shard_last = jnp.concatenate([feedforward_input_weight[:, first:], back[:, first:]], axis=1)

    others = (1 - core) * mine
    x_send = lax.dynamic_slice_in_dim(inputs, others, mine, 0)
    x_got = swap(x_send)
    grad_got = swap(lax.dynamic_slice_in_dim(output_gradient, others, mine, 0))
    bias_got, up_got, hidden_bias_got = map(swap, (query_value_bias, adapter_up_weight, feedforward_input_bias))

    blank = jnp.zeros((heads,), F32)
    ones = blank + 1
    both = [query_value_bias[0], blank, query_value_bias[1], bias_got[0], blank, bias_got[1]]
    scale = [ones * 0.125, ones, ones] * 2
    bias = jnp.stack([jnp.concatenate(both), jnp.concatenate(scale)])

    if count == 16:
        index = lax.axis_index("dp")

        def tables(flips):
            mine_first = [jnp.where(core == 0, a, b) for a, b in zip(*flips, strict=True)]
            other_first = [jnp.where(core == 0, b, a) for a, b in zip(*flips, strict=True)]
            return [block_offsets(index, shard_rows, f) for f in (mine_first, other_first)]

        offsets = jnp.concatenate(tables(LINE_FIRST) + tables(PLANE_FIRST))
        order, order_last, n = ((0, 16), 8), ((32, 48), 8), 2

        def exchange(array, flips, step):
            pairs = [(2 * i + t, 2 * (i ^ flips[t][step]) + t) for i in range(count) for t in range(2)]
            return lax.ppermute(array, ("dp", "tensor"), pairs)

        def joined(*arrays):
            return jnp.concatenate(arrays, axis=0)

        shard_last = after(shard_last, x_send)
        line = line_start = joined(shard, exchange(shard, LINE_FIRST, 0))
        plane = joined(shard_last, exchange(shard_last, PLANE_FIRST, 0))
        line = joined(line, exchange(line, LINE_FIRST, 1))
        plane = after(plane, line_start)
        plane = joined(plane, exchange(plane, PLANE_FIRST, 1))
        line, plane, *early = lax.optimization_barrier((line, plane, x_got, up_got, grad_got, hidden_bias_got, offsets, bias))
        x_got, up_got, grad_got, hidden_bias_got, offsets, bias = early
        shard_first = after(shard_first, line)
        line_first = joined(shard_first, exchange(shard_first, LINE_FIRST, 0))
        line = joined(line, exchange(line, LINE_FIRST, 2))
        line_first = after(line_first, line)
        line_first = joined(line_first, exchange(line_first, LINE_FIRST, 1))
        own = [line, exchange(line, LINE_FIRST, 3)]
        swapped = [swap(line)]
        line_first, plane, own, swapped = lax.optimization_barrier((line_first, plane, own, swapped))
        swapped.append(swap(own[1]))
        line_first = joined(line_first, exchange(line_first, LINE_FIRST, 2))
        plane = joined(plane, exchange(plane, PLANE_FIRST, 2))
        plane, line_first, x_got = lax.optimization_barrier((plane, line_first, x_got))
        own_first = [line_first, exchange(line_first, LINE_FIRST, 3)]
        own_last = [plane, exchange(plane, PLANE_FIRST, 3)]
        got_first, got_last = [swap(line_first)], [swap(plane)]
    else:
        offsets = jnp.zeros((2,), jnp.int32)
        order = order_last = ((0, 0), 1)
        n = 1
        own, own_first, own_last = (
            [lax.all_gather(s, "dp", axis=0, tiled=True)] for s in (shard, shard_first, shard_last)
        )
        swapped, got_first, got_last = [swap(own[0])], [], []
    pieces = (*own, *swapped)

    first_item = core * mine
    my_lengths = lax.dynamic_slice_in_dim(lengths[:, 0], first_item, mine, 0)
    my_bounds = lax.dynamic_slice_in_dim(bounds[:, 0], first_item, mine, 0)
    core = core[None].astype(jnp.int32)

    own_block = pl.BlockSpec((1, rows, width), lambda i, *s: (s[-1][0] * mine + i, 0, 0))
    got_block = pl.BlockSpec((1, rows, width), lambda i, *_: (i, 0, 0))
    item = (mine, slot, width)
    wide = (mine, slot, 3 * width)

    def out_item(shape, dtype):
        return shape_of(shape, dtype), item_spec(shape)

    def in_item(array):
        return array, item_spec(array.shape)

    def in_whole(array):
        return array, whole_spec(array)

    split_out = lambda dtype: [(shape_of(inputs.shape, dtype), own_block), (shape_of((mine, rows, width), dtype), got_block)]

    tokens = mine * slot
    qkv, mixed, spare, low = call(
        functools.partial(project_attend_kernel, order, n),
        "project_attend",
        (offsets, my_lengths, my_bounds, core),
        pieces,
        [(inputs, own_block), (x_got, got_block), in_whole(bias), in_whole(adapter_up_weight), in_whole(up_got)],
        [
            out_item(wide, BF16),
            out_item(item, BF16),
            out_item((mine, slot, LANES), BF16),
            out_item((mine, slot, 2 * LANES), BF16),
        ],
        [
            pltpu.VMEM((width + 2 * LANES, 3 * width), BF16),
            pltpu.VMEM((width, LANES), BF16),
            pltpu.SemaphoreType.DMA((2,)),
        ],
        mine,
        2 * tokens * width * (4 * width + 8 * slot),
        12 * tokens * width,
    )
    own_first, own_last = lax.optimization_barrier((own_first, own_last, mixed))[:2]
    got_first += map(swap, own_first[len(got_first) :])
    got_last += map(swap, own_last[len(got_last) :])
    hidden_bias = jnp.concatenate(
        [
            feedforward_input_bias[:first],
            hidden_bias_got[:first],
            feedforward_input_bias[first:],
            hidden_bias_got[first:],
        ]
    )[None]
    pieces_feed = (*own_first, *got_first, *own_last, *got_last)
    out, out_send, grad_hidden, grad_mixed = call(
        functools.partial(feed_kernel, (order, order_last), (first, last), n),
        "feed",
        (offsets, core),
        pieces_feed,
        [
            (inputs, own_block),
            (x_got, got_block),
            in_item(mixed),
            (output_gradient, own_block),
            (grad_got, got_block),
            *map(in_whole, (hidden_bias, output_bias, layernorm_scale, layernorm_bias)),
        ],
        [*split_out(BF16), out_item(item, F32), out_item(item, BF16)],
        [
            pltpu.VMEM((width, width), BF16),
            pltpu.VMEM((width, 2 * hidden), BF16),
            pltpu.VMEM((width, 2 * hidden), BF16),
            pltpu.VMEM((slot, 2 * hidden), F32),
            pltpu.SemaphoreType.DMA((5,)),
        ],
        mine,
        4 * tokens * width * (width + 4 * hidden),
        8 * width * hidden,
    )
    out_got = swap(out_send)
    adapter = (2 * RANK, width)
    grads, adapter = call(
        attend_back_kernel,
        "attend_back",
        (my_lengths, my_bounds, core),
        (),
        [*map(in_item, (qkv, mixed, spare, low, grad_mixed))],
        [out_item(wide, BF16), (shape_of(adapter, F32), pl.BlockSpec(adapter, lambda i, *_: (0, 0)))],
        [],
        mine,
        2 * tokens * width * 20 * slot,
        16 * tokens * width,
    )
    grads, out_got = lax.optimization_barrier((grads, out_got))
    if count == 16:
        ways = [over_dp(count, adapter, lambda i, flip=flip: i ^ flip) for flip in (4, 8, 12)]
    total, total_send = call(
        functools.partial(input_grad_kernel, order, n),
        "input_grad",
        (offsets, core),
        pieces,
        [in_item(grads), in_item(grad_hidden), in_whole(adapter_up_weight), in_whole(up_got)],
        split_out(F32),
        [
            pltpu.VMEM((width, 3 * width + 2 * LANES), BF16),
            pltpu.VMEM((LANES, 3 * width), BF16),
            pltpu.SemaphoreType.DMA((1,)),
        ],
        mine,
        2 * tokens * width * 3 * width,
        12 * tokens * width,
    )
    if count == 16:
        *ways, total_send, out = lax.optimization_barrier((*ways, total_send, out))
        adapter = (adapter + ways[0]) + (ways[1] + ways[2])
        ways = [over_dp(count, adapter, lambda i, flip=flip: i ^ flip) for flip in (1, 2, 3)]
        input_grad = lax.dynamic_update_slice_in_dim(total, swap(total_send), others, 0)
        result = lax.dynamic_update_slice_in_dim(out, out_got, others, 0)
        *ways, input_grad, result = lax.optimization_barrier((*ways, input_grad, result))
        adapter = (adapter + ways[0]) + (ways[1] + ways[2])
    else:
        adapter = lax.psum(adapter, "dp")
        input_grad = lax.dynamic_update_slice_in_dim(total, swap(total_send), others, 0)
        result = lax.dynamic_update_slice_in_dim(out, out_got, others, 0)
    adapter = adapter[:, :heads] + swap(adapter[:, heads:])
    return result, input_grad, adapter.reshape(2, RANK, heads)


def solution(mesh):
    return jax.shard_map(
        functools.partial(local, count=mesh.shape["dp"]),
        mesh=mesh,
        in_specs=(
            P(None, ("dp", "tensor"), None),
            P(None, "dp"),
            P(None, "dp"),
            P("dp", "tensor"),
            P("dp", "tensor"),
            P("dp", "tensor"),
            P(None, "tensor"),
            P(None, "dp", None),
            P(None, None, "tensor"),
            P("tensor", "dp"),
            P("dp", "tensor"),
            P("tensor"),
            P("tensor", "dp"),
            P(),
            P(),
            P(),
            P(None, ("dp", "tensor"), None),
        ),
        out_specs=(
            P(None, ("dp", "tensor"), None),
            P(None, ("dp", "tensor"), None),
            P(None, None, "tensor"),
        ),
        check_vma=False,
    )
```

```python
import functools

import jax
import jax.numpy as jnp
from jax import lax
from jax.experimental import pallas as pl
from jax.experimental.pallas import tpu as pltpu
from jax.sharding import PartitionSpec as P

F32 = jnp.float32
BF16 = jnp.bfloat16
HEAD_DIM = 64
RANK = 8
LANES = 128
EPS = 1e-05
MASKED = -float(2**30)
SEG = 64
VMEM_LIMIT = 60 * 2**20

NT = (((1,), (1,)), ((), ()))
TN = (((0,), (0,)), ((), ()))


def mm(a, b):
    return jnp.dot(a, b, preferred_element_type=F32)


def mm_nt(a, b):
    return lax.dot_general(a, b, NT, preferred_element_type=F32)


def mm_tn(a, b):
    return lax.dot_general(a, b, TN, preferred_element_type=F32)


def iota(shape, dimension):
    return lax.broadcasted_iota(jnp.int32, shape, dimension)


def three_parts(value, lane):
    high = value.astype(BF16).astype(F32)
    rest = value - high
    middle = rest.astype(BF16).astype(F32)
    return jnp.where(lane < 16, high, jnp.where(lane < 32, middle, jnp.where(lane < 48, rest - middle, 0.0)))


def two_parts(value):
    high = value.astype(BF16)
    return jnp.concatenate([high, (value - high.astype(F32)).astype(BF16)], axis=1)


def weight_copies(order, offsets, pieces, target, sem, columns):
    firsts, blocks = order
    copies, waits = [], []
    for half, first, width, to in columns:
        for index, ref in enumerate(pieces[half]):
            rows = ref.shape[0] // blocks
            for place in range(blocks):
                start = offsets[firsts[half] + index * blocks + place]
                if rows % 16 == 0:
                    start = pl.multiple_of(start, 16)
                copies.append(
                    pltpu.make_async_copy(
                        ref.at[pl.ds(place * rows, rows), pl.ds(first, width)],
                        target.at[pl.ds(start, rows), pl.ds(to, width)],
                        sem,
                    )
                )
        filled = target.at[pl.ds(0, sum(ref.shape[0] for ref in pieces[half])), pl.ds(to, width)]
        waits.append(pltpu.make_async_copy(filled, filled, sem))
    return copies, waits


def start_all(group):
    for copy in group[0]:
        copy.start()


def wait_all(group):
    for copy in group[1]:
        copy.wait()


def places(core, shape, half_slot):
    row = iota(shape, 0)
    return jnp.where(row < half_slot, row + core * half_slot, row - core * half_slot)


def flags_of(core, length, bound, slot):
    lane = iota((slot, LANES), 1)
    place = places(core, (slot, LANES), slot // 2)
    second = place >= bound
    query = jnp.where(
        lane == SEG,
        jnp.where(second, 1.0, 0.0),
        jnp.where(lane == SEG + 1, jnp.where(second, 0.0, 1.0), jnp.where(lane == SEG + 2, 1.0, 0.0)),
    )
    key = jnp.where(
        lane == SEG,
        jnp.where(second, 0.0, MASKED),
        jnp.where(
            lane == SEG + 1,
            jnp.where(second, MASKED, 0.0),
            jnp.where((lane == SEG + 2) & (place >= length), MASKED, 0.0),
        ),
    )
    return lane, query, key


def pair_columns(pair, heads):
    per_half = heads // LANES
    base = (pair // per_half) * 3 * heads + (pair % per_half) * LANES
    return base, base + heads, base + 2 * heads


def load_projections(order, offsets, pieces, weights, sem, heads, downs):
    wide = 3 * heads
    columns = [(0, 0, wide, 0), (1, 0, wide, wide)]
    columns += [(0, wide, LANES, to) for to in downs]
    return weight_copies(order, offsets, pieces, weights, sem, columns)


def ups(up_refs, heads):
    blank = jnp.zeros((RANK, heads), BF16)
    parts = []
    for ref in up_refs:
        parts += [
            jnp.concatenate([ref[0] * 2, blank], axis=0),
            jnp.concatenate([blank, blank], axis=0),
            jnp.concatenate([blank, ref[1] * 2], axis=0),
        ]
    return jnp.concatenate(parts, axis=1)


def project_attend_kernel(order, n, offsets, lengths, bounds, core_ref, *refs):
    pieces = (refs[:n], refs[n : 2 * n])
    (
        x_own_ref,
        x_got_ref,
        bias_ref,
        up_own_ref,
        up_got_ref,
        qkv_ref,
        mixed_ref,
        spare_ref,
        low_ref,
        weights,
        down,
        sems,
    ) = refs[2 * n :]
    item = pl.program_id(0)
    core = core_ref[0]
    slot, width = mixed_ref.shape[1:]
    heads = width // 2

    @pl.when(item == 0)
    def _():
        wide = 3 * heads
        copies = weight_copies(order, offsets, pieces, weights, sems.at[0], [(0, 0, wide, 0), (1, 0, wide, wide)])
        downs = weight_copies(order, offsets, pieces, down, sems.at[1], [(0, wide, LANES, 0)])
        start_all(downs)
        start_all(copies)
        weights[width:] = jnp.zeros((2 * LANES, 6 * heads), BF16)
        up = ups((up_own_ref, up_got_ref), heads)
        weights[width : width + 2 * RANK] = up
        weights[width + LANES : width + LANES + 2 * RANK] = up
        wait_all(downs)
        wait_all(copies)

    x = jnp.concatenate([x_own_ref[0], x_got_ref[0]], axis=0)
    low = two_parts(mm(x, down[...]))
    low_ref[0] = low
    wide_x = jnp.concatenate([x, low], axis=1)
    for part in range(3):
        at = slice(part * width, (part + 1) * width)
        out = (mm(wide_x, weights[:, at]) + bias_ref[0:1, at]) * bias_ref[1:2, at]
        qkv_ref[0, :, at] = out.astype(BF16)

    lane, query_flags, key_flags = flags_of(core, lengths[item], bounds[item], slot)
    query_low = query_flags.astype(BF16)
    key_low = key_flags.astype(BF16)
    ones = jnp.where(lane == 0, 1.0, 0.0).astype(BF16)
    zero = jnp.zeros((slot, LANES), BF16)
    totals = jnp.ones((slot, LANES), F32)
    peaks = []
    for pair in range(width // LANES):
        at_query, at_key, at_value = pair_columns(pair, heads)
        query = qkv_ref[0, :, at_query : at_query + LANES]
        keys = jnp.concatenate([qkv_ref[0, :, at_key : at_key + LANES], key_low], axis=1)
        values = jnp.concatenate([qkv_ref[0, :, at_value : at_value + LANES], ones], axis=1)
        outs = []
        for side in range(2):
            inside = (lane < HEAD_DIM) if side == 0 else (lane >= HEAD_DIM)
            query_side = jnp.concatenate([jnp.where(inside, query, zero), query_low], axis=1)
            scores = mm_nt(keys, query_side)
            peak = jnp.max(scores, axis=0, keepdims=True)
            probs = jnp.exp(scores - peak).astype(BF16)
            out = mm_tn(probs, values)
            total = out[:, LANES : LANES + 1]
            outs.append(out[:, :LANES] * (1.0 / total))
            totals = jnp.where((lane & 15) == 2 * pair + side, total, totals)
            peaks.append(peak)
        mixed_ref[0, :, pair * LANES : (pair + 1) * LANES] = jnp.where(
            lane < HEAD_DIM, outs[0], outs[1]
        ).astype(BF16)
    peaks += [jnp.zeros((1, slot), F32)] * (16 - len(peaks))
    peaks = jnp.concatenate(peaks, axis=0)
    peaks = jnp.concatenate([peaks] * (LANES // 16), axis=0).T
    spare_ref[0] = (three_parts(peaks + jnp.log(totals), lane) + query_flags).astype(BF16)


def row_mean(value):
    return jnp.mean(value, axis=-1, keepdims=True)


def normalize(value):
    centre = value - row_mean(value)
    scale = lax.rsqrt(row_mean(centre * centre) + EPS)
    return centre * scale, scale


def normalize_back(grad, gain, normal, scale):
    grad = grad * gain
    return scale * (grad - row_mean(grad) - normal * row_mean(grad * normal))


def feed_kernel(orders, chunks, n, offsets, core_ref, *refs):
    pieces = (refs[:n], refs[n : 2 * n])
    pieces_last = (refs[2 * n : 3 * n], refs[3 * n : 4 * n])
    (
        x_own_ref,
        x_got_ref,
        mixed_ref,
        grad_own_ref,
        grad_got_ref,
        hidden_bias_ref,
        output_bias_ref,
        gain_ref,
        shift_ref,
        out_own_ref,
        out_got_ref,
        grad_hidden_ref,
        grad_mixed_ref,
        out_weights,
        in_weights,
        back_weights,
        slope,
        sems,
    ) = refs[4 * n :]
    slot, width = mixed_ref.shape[1:]
    half_slot = slot // 2
    heads = width // 2
    first, last = chunks
    size = width
    parts = list(range(0, 2 * (first + last), size))

    o = heads
    tail = 2 * first
    groups = [
        weight_copies(orders[0], offsets, pieces, out_weights, sems.at[0], [(0, 0, o, 0), (1, 0, o, o)]),
        weight_copies(orders[0], offsets, pieces, in_weights, sems.at[1], [(0, o, first, 0), (1, o, first, first)]),
        weight_copies(
            orders[0], offsets, pieces, back_weights, sems.at[2], [(0, o + first, first, 0), (1, o + first, first, first)]
        ),
        weight_copies(
            orders[1], offsets, pieces_last, in_weights, sems.at[3], [(0, 0, last, tail), (1, 0, last, tail + last)]
        ),
        weight_copies(
            orders[1], offsets, pieces_last, back_weights, sems.at[4], [(0, last, last, tail), (1, last, last, tail + last)]
        ),
    ]

    @pl.when(pl.program_id(0) == 0)
    def _():
        for group in groups:
            start_all(group)

    def arrived(*which):
        @pl.when(pl.program_id(0) == 0)
        def _():
            for index in which:
                wait_all(groups[index])

    arrived(0)
    x = jnp.concatenate([x_own_ref[0], x_got_ref[0]], axis=0).astype(F32)
    summed = x + output_bias_ref[0:1] + mm_nt(mixed_ref[0], out_weights[...])
    normal_in, scale_in = normalize(summed)
    normed = normal_in * gain_ref[0:1] + shift_ref[0:1]
    normed_low = normed.astype(BF16)
    total = normed + output_bias_ref[1:2]
    for at in parts:
        if at == 0:
            arrived(1)
        if at < tail < at + size or at == tail:
            arrived(3)
        pre = mm(normed_low, in_weights[:, at : at + size]) + hidden_bias_ref[:, at : at + size]
        share = 0.5 * (1.0 + lax.erf(pre * 0.7071067811865476))
        slope[:, at : at + size] = share + pre * jnp.exp(-0.5 * pre * pre) * 0.3989422804014327
        if at == 0:
            arrived(2)
        if at < tail < at + size or at == tail:
            arrived(4)
        total += mm_nt((pre * share).astype(BF16), back_weights[:, at : at + size])
    normal_out, scale_out = normalize(total)
    out = (normal_out * gain_ref[1:2] + shift_ref[1:2]).astype(BF16)
    out_own_ref[0] = out[:half_slot]
    out_got_ref[0] = out[half_slot:]
    grad = jnp.concatenate([grad_own_ref[0], grad_got_ref[0]], axis=0).astype(F32)
    grad_total = normalize_back(grad, gain_ref[1:2], normal_out, scale_out)
    grad_low = grad_total.astype(BF16)
    grad_normed = grad_total
    for at in parts:
        grad_pre = (mm(grad_low, back_weights[:, at : at + size]) * slope[:, at : at + size]).astype(BF16)
        grad_normed += mm_nt(grad_pre, in_weights[:, at : at + size])
    grad_hidden = normalize_back(grad_normed, gain_ref[0:1], normal_in, scale_in)
    grad_hidden_ref[0] = grad_hidden
    grad_mixed_ref[0] = mm(grad_hidden.astype(BF16), out_weights[...]).astype(BF16)


def attend_back_kernel(lengths, bounds, core_ref, *refs):
    (
        qkv_ref,
        mixed_ref,
        spare_ref,
        low_ref,
        grad_mixed_ref,
        grads_ref,
        adapter_ref,
    ) = refs
    item = pl.program_id(0)
    core = core_ref[0]
    slot, width = mixed_ref.shape[1:]
    heads = width // 2

    lane, _, key_flags = flags_of(core, lengths[item], bounds[item], slot)
    row = iota((width, LANES), 0)
    column = iota((width, LANES), 1)
    pick = jnp.where((row // HEAD_DIM == (column & 15)) & (column < 48), 1.0, 0.0).astype(BF16)
    product = grad_mixed_ref[0].astype(F32) * mixed_ref[0].astype(F32)
    high = product.astype(BF16)
    rest = (product - high.astype(F32)).astype(BF16)
    inner = three_parts(mm(high, pick) + mm(rest, pick), lane).astype(BF16)
    spare = spare_ref[0]
    zero = jnp.zeros((slot, LANES), BF16)
    per_half = heads // LANES

    def columns(first):
        return pl.ds(pl.multiple_of(first, LANES), LANES)

    def of_pair(pair):
        base = (pair // per_half) * 3 * heads + (pair % per_half) * LANES
        at_query, at_key, at_value = (columns(base + part * heads) for part in range(3))
        query = qkv_ref[0, :, at_query]
        keys = qkv_ref[0, :, at_key]
        values = qkv_ref[0, :, at_value]
        grad = grad_mixed_ref[0, :, columns(pair * LANES)]
        total_query = jnp.zeros((slot, LANES), F32)
        total_key = jnp.zeros((slot, LANES), F32)
        total_value = jnp.zeros((slot, LANES), F32)
        for side in range(2):
            head = 2 * pair + side
            inside = (lane < HEAD_DIM) if side == 0 else (lane >= HEAD_DIM)
            mine = ((lane & 15) == head) & (lane < 48)
            query_side = jnp.where(inside, query, zero)
            key_side = jnp.where(inside, keys, zero)
            grad_side = jnp.where(inside, grad, zero)
            key_wide = jnp.concatenate([keys, jnp.where(mine, -1.0, key_flags).astype(BF16)], axis=1)
            value_wide = jnp.concatenate([values, jnp.where(mine, -1.0, 0.0).astype(BF16)], axis=1)
            probs = jnp.exp(mm_nt(key_wide, jnp.concatenate([query_side, spare], axis=1)))
            grad_probs = mm_nt(value_wide, jnp.concatenate([grad_side, inner], axis=1))
            grad_scores = (probs * grad_probs).astype(BF16)
            total_value += mm(probs.astype(BF16), grad_side)
            total_key += mm(grad_scores, query_side)
            total_query += mm_tn(grad_scores, key_side)
        grads_ref[0, :, at_query] = (total_query * 0.125).astype(BF16)
        grads_ref[0, :, at_key] = total_key.astype(BF16)
        grads_ref[0, :, at_value] = total_value.astype(BF16)

    pairs = width // LANES
    group = 3 if pairs % 3 == 0 else 1

    @pl.loop(0, pairs // group)
    def _(step):
        for place in range(group):
            of_pair(step * group + place)

    update = 2.0 * mm_tn(low_ref[0], grads_ref[0])
    parts = []
    for half in range(2):
        at = half * 3 * heads
        of_query = update[:, at : at + heads]
        of_value = update[:, at + 2 * heads : at + 3 * heads]
        rows = [
            of_query[:RANK] + of_query[LANES : LANES + RANK],
            of_value[RANK : 2 * RANK] + of_value[LANES + RANK : LANES + 2 * RANK],
        ]
        parts.append(jnp.concatenate(rows, axis=0))
    part = jnp.concatenate(parts, axis=1)

    @pl.when(item == 0)
    def _():
        adapter_ref[...] = part

    @pl.when(item > 0)
    def _():
        adapter_ref[...] += part


def input_grad_kernel(order, n, offsets, core_ref, *refs):
    pieces = (refs[:n], refs[n : 2 * n])
    (
        grads_ref,
        grad_hidden_ref,
        up_own_ref,
        up_got_ref,
        own_ref,
        got_ref,
        weights,
        up,
        sems,
    ) = refs[2 * n :]
    slot, width = grad_hidden_ref.shape[1:]
    heads = width // 2

    @pl.when(pl.program_id(0) == 0)
    def _():
        copies = load_projections(order, offsets, pieces, weights, sems.at[0], heads, (6 * heads, 6 * heads + LANES))
        start_all(copies)
        up[...] = jnp.zeros_like(up)
        up[: 2 * RANK] = ups((up_own_ref, up_got_ref), heads)
        wait_all(copies)

    grads = grads_ref[0]
    small = two_parts(mm_nt(grads, up[...]))
    total = grad_hidden_ref[0] + mm_nt(jnp.concatenate([grads, small], axis=1), weights[...])
    own_ref[0] = total[: slot // 2]
    got_ref[0] = total[slot // 2 :]


def any_spec():
    return pl.BlockSpec(memory_space=pl.ANY)


def whole_spec(array):
    return pl.BlockSpec(array.shape, lambda i, *_: (0,) * array.ndim)


def item_spec(shape):
    return pl.BlockSpec((1, *shape[1:]), lambda i, *_: (i, 0, 0))


def shape_of(shape, dtype):
    return jax.ShapeDtypeStruct(shape, dtype)


def call(kernel, name, scalars, flat, args, outs, scratch, items, flops, moved):
    return pl.pallas_call(
        kernel,
        grid_spec=pltpu.PrefetchScalarGridSpec(
            num_scalar_prefetch=len(scalars),
            grid=(items,),
            in_specs=[any_spec()] * len(flat) + [spec for _, spec in args],
            out_specs=[spec for _, spec in outs],
            scratch_shapes=scratch,
        ),
        out_shape=[shape for shape, _ in outs],
        compiler_params=pltpu.CompilerParams(vmem_limit_bytes=VMEM_LIMIT),
        cost_estimate=pl.CostEstimate(flops=flops, bytes_accessed=moved, transcendentals=0),
        name=name,
    )(*scalars, *flat, *[array for array, _ in args])


def swap(array):
    return lax.ppermute(array, "tensor", [(0, 1), (1, 0)])


def after(value, *deps):
    return lax.optimization_barrier((value, *deps))[0]


def over_dp(count, array, target):
    return lax.ppermute(array, "dp", [(i, target(i)) for i in range(count)])


LINE_FIRST = ((4, 8, 1, 2), (8, 4, 2, 1))
PLANE_FIRST = ((1, 2, 4, 8), (2, 1, 8, 4))


def block_offsets(index, rows, flips):
    place = jnp.arange(16)
    flipped = sum(((place >> bit) & 1) * flips[bit] for bit in range(4))
    return ((index ^ flipped) * rows).astype(jnp.int32)


def local(
    inputs,
    lengths,
    bounds,
    query_matrix,
    key_matrix,
    value_matrix,
    query_value_bias,
    adapter_down_weight,
    adapter_up_weight,
    attention_output_weight,
    feedforward_input_weight,
    feedforward_input_bias,
    feedforward_output_weight,
    output_bias,
    layernorm_scale,
    layernorm_bias,
    output_gradient,
    *,
    count,
):
    micro, rows, width = inputs.shape
    mine = micro // 2
    slot = 2 * rows
    heads = width // 2
    core = lax.axis_index("tensor")
    shard_rows = query_matrix.shape[0]
    hidden = feedforward_input_weight.shape[1]
    last = hidden // 3 if count == 16 else hidden // 2
    first = hidden - last

    blank = jnp.zeros((shard_rows, LANES - 2 * RANK), BF16)
    down = [adapter_down_weight[0], adapter_down_weight[1], blank]
    shard = jnp.concatenate([query_matrix, key_matrix, value_matrix, *down], axis=1)
    back = feedforward_output_weight.T
    shard_first = jnp.concatenate(
        [attention_output_weight.T, feedforward_input_weight[:, :first], back[:, :first]], axis=1
    )
    shard_last = jnp.concatenate([feedforward_input_weight[:, first:], back[:, first:]], axis=1)

    others = (1 - core) * mine
    x_send = lax.dynamic_slice_in_dim(inputs, others, mine, 0)
    x_got = swap(x_send)
    grad_got = swap(lax.dynamic_slice_in_dim(output_gradient, others, mine, 0))
    bias_got, up_got, hidden_bias_got = map(swap, (query_value_bias, adapter_up_weight, feedforward_input_bias))

    first_item = core * mine
    my_lengths = lax.dynamic_slice_in_dim(lengths[:, 0], first_item, mine, 0)
    my_bounds = lax.dynamic_slice_in_dim(bounds[:, 0], first_item, mine, 0)
    blank = jnp.zeros((heads,), F32)
    ones = blank + 1
    both = [query_value_bias[0], blank, query_value_bias[1], bias_got[0], blank, bias_got[1]]
    scale = [ones * 0.125, ones, ones] * 2
    bias = jnp.stack([jnp.concatenate(both), jnp.concatenate(scale)])

    if count == 16:
        index = lax.axis_index("dp")

        def tables(flips):
            mine_first = [jnp.where(core == 0, a, b) for a, b in zip(*flips, strict=True)]
            other_first = [jnp.where(core == 0, b, a) for a, b in zip(*flips, strict=True)]
            return [block_offsets(index, shard_rows, f) for f in (mine_first, other_first)]

        offsets = jnp.concatenate(tables(LINE_FIRST) + tables(PLANE_FIRST))
        order, order_last, n = ((0, 16), 8), ((32, 48), 8), 2

        def exchange(array, flips, step):
            pairs = [(2 * i + t, 2 * (i ^ flips[t][step]) + t) for i in range(count) for t in range(2)]
            return lax.ppermute(array, ("dp", "tensor"), pairs)

        def joined(*arrays):
            return jnp.concatenate(arrays, axis=0)

        shard_last = after(shard_last, x_send)
        line = line_start = joined(shard, exchange(shard, LINE_FIRST, 0))
        plane = joined(shard_last, exchange(shard_last, PLANE_FIRST, 0))
        line = joined(line, exchange(line, LINE_FIRST, 1))
        plane = after(plane, line_start)
        plane = joined(plane, exchange(plane, PLANE_FIRST, 1))
        line, plane, *early = lax.optimization_barrier((line, plane, x_got, up_got, grad_got, hidden_bias_got, offsets, bias))
        x_got, up_got, grad_got, hidden_bias_got, offsets, bias = early
        shard_first = after(shard_first, line)
        line_first = joined(shard_first, exchange(shard_first, LINE_FIRST, 0))
        line = joined(line, exchange(line, LINE_FIRST, 2))
        line_first = after(line_first, line)
        line_first = joined(line_first, exchange(line_first, LINE_FIRST, 1))
        own = [line, exchange(line, LINE_FIRST, 3)]
        swapped = [swap(line)]
        line_first, plane, own, swapped, my_lengths, my_bounds = lax.optimization_barrier(
            (line_first, plane, own, swapped, my_lengths, my_bounds)
        )
        swapped.append(swap(own[1]))
        line_first = joined(line_first, exchange(line_first, LINE_FIRST, 2))
        plane = joined(plane, exchange(plane, PLANE_FIRST, 2))
        got_last = [swap(plane)]
        plane, line_first, x_got = lax.optimization_barrier((plane, line_first, x_got))
        own_first = [line_first, exchange(line_first, LINE_FIRST, 3)]
        own_last = [plane, exchange(plane, PLANE_FIRST, 3)]
        got_first = [swap(line_first)]
        got_last, x_got = lax.optimization_barrier((got_last, x_got))
    else:
        offsets = jnp.zeros((2,), jnp.int32)
        order = order_last = ((0, 0), 1)
        n = 1
        own, own_first, own_last = (
            [lax.all_gather(s, "dp", axis=0, tiled=True)] for s in (shard, shard_first, shard_last)
        )
        swapped, got_first, got_last = [swap(own[0])], [], []
    pieces = (*own, *swapped)

    core = core[None].astype(jnp.int32)

    own_block = pl.BlockSpec((1, rows, width), lambda i, *s: (s[-1][0] * mine + i, 0, 0))
    got_block = pl.BlockSpec((1, rows, width), lambda i, *_: (i, 0, 0))
    item = (mine, slot, width)
    wide = (mine, slot, 3 * width)

    def out_item(shape, dtype):
        return shape_of(shape, dtype), item_spec(shape)

    def in_item(array):
        return array, item_spec(array.shape)

    def in_whole(array):
        return array, whole_spec(array)

    split_out = lambda dtype: [(shape_of(inputs.shape, dtype), own_block), (shape_of((mine, rows, width), dtype), got_block)]

    tokens = mine * slot
    qkv, mixed, spare, low = call(
        functools.partial(project_attend_kernel, order, n),
        "project_attend",
        (offsets, my_lengths, my_bounds, core),
        pieces,
        [(inputs, own_block), (x_got, got_block), in_whole(bias), in_whole(adapter_up_weight), in_whole(up_got)],
        [
            out_item(wide, BF16),
            out_item(item, BF16),
            out_item((mine, slot, LANES), BF16),
            out_item((mine, slot, 2 * LANES), BF16),
        ],
        [
            pltpu.VMEM((width + 2 * LANES, 3 * width), BF16),
            pltpu.VMEM((width, LANES), BF16),
            pltpu.SemaphoreType.DMA((2,)),
        ],
        mine,
        2 * tokens * width * (4 * width + 8 * slot),
        12 * tokens * width,
    )
    own_first, own_last = lax.optimization_barrier((own_first, own_last, mixed))[:2]
    got_first += map(swap, own_first[len(got_first) :])
    got_last += map(swap, own_last[len(got_last) :])
    hidden_bias = jnp.concatenate(
        [
            feedforward_input_bias[:first],
            hidden_bias_got[:first],
            feedforward_input_bias[first:],
            hidden_bias_got[first:],
        ]
    )[None]
    pieces_feed = (*own_first, *got_first, *own_last, *got_last)
    out, out_send, grad_hidden, grad_mixed = call(
        functools.partial(feed_kernel, (order, order_last), (first, last), n),
        "feed",
        (offsets, core),
        pieces_feed,
        [
            (inputs, own_block),
            (x_got, got_block),
            in_item(mixed),
            (output_gradient, own_block),
            (grad_got, got_block),
            *map(in_whole, (hidden_bias, output_bias, layernorm_scale, layernorm_bias)),
        ],
        [*split_out(BF16), out_item(item, F32), out_item(item, BF16)],
        [
            pltpu.VMEM((width, width), BF16),
            pltpu.VMEM((width, 2 * hidden), BF16),
            pltpu.VMEM((width, 2 * hidden), BF16),
            pltpu.VMEM((slot, 2 * hidden), F32),
            pltpu.SemaphoreType.DMA((5,)),
        ],
        mine,
        4 * tokens * width * (width + 4 * hidden),
        8 * width * hidden,
    )
    out_got = swap(out_send)
    adapter = (2 * RANK, width)
    grads, adapter = call(
        attend_back_kernel,
        "attend_back",
        (my_lengths, my_bounds, core),
        (),
        [*map(in_item, (qkv, mixed, spare, low, grad_mixed))],
        [out_item(wide, BF16), (shape_of(adapter, F32), pl.BlockSpec(adapter, lambda i, *_: (0, 0)))],
        [],
        mine,
        2 * tokens * width * 20 * slot,
        16 * tokens * width,
    )
    grads, out_got = lax.optimization_barrier((grads, out_got))
    if count == 16:
        ways = [over_dp(count, adapter, lambda i, flip=flip: i ^ flip) for flip in (4, 8, 12)]
    total, total_send = call(
        functools.partial(input_grad_kernel, order, n),
        "input_grad",
        (offsets, core),
        pieces,
        [in_item(grads), in_item(grad_hidden), in_whole(adapter_up_weight), in_whole(up_got)],
        split_out(F32),
        [
            pltpu.VMEM((width, 3 * width + 2 * LANES), BF16),
            pltpu.VMEM((LANES, 3 * width), BF16),
            pltpu.SemaphoreType.DMA((1,)),
        ],
        mine,
        2 * tokens * width * 3 * width,
        12 * tokens * width,
    )
    if count == 16:
        *ways, total_send, out = lax.optimization_barrier((*ways, total_send, out))
        adapter = (adapter + ways[0]) + (ways[1] + ways[2])
        ways = [over_dp(count, adapter, lambda i, flip=flip: i ^ flip) for flip in (1, 2, 3)]
        input_grad = lax.dynamic_update_slice_in_dim(total, swap(total_send), others, 0)
        result = lax.dynamic_update_slice_in_dim(out, out_got, others, 0)
        *ways, input_grad, result = lax.optimization_barrier((*ways, input_grad, result))
        adapter = (adapter + ways[0]) + (ways[1] + ways[2])
    else:
        adapter = lax.psum(adapter, "dp")
        input_grad = lax.dynamic_update_slice_in_dim(total, swap(total_send), others, 0)
        result = lax.dynamic_update_slice_in_dim(out, out_got, others, 0)
    adapter = adapter[:, :heads] + swap(adapter[:, heads:])
    return result, input_grad, adapter.reshape(2, RANK, heads)


def solution(mesh):
    return jax.shard_map(
        functools.partial(local, count=mesh.shape["dp"]),
        mesh=mesh,
        in_specs=(
            P(None, ("dp", "tensor"), None),
            P(None, "dp"),
            P(None, "dp"),
            P("dp", "tensor"),
            P("dp", "tensor"),
            P("dp", "tensor"),
            P(None, "tensor"),
            P(None, "dp", None),
            P(None, None, "tensor"),
            P("tensor", "dp"),
            P("dp", "tensor"),
            P("tensor"),
            P("tensor", "dp"),
            P(),
            P(),
            P(),
            P(None, ("dp", "tensor"), None),
        ),
        out_specs=(
            P(None, ("dp", "tensor"), None),
            P(None, ("dp", "tensor"), None),
            P(None, None, "tensor"),
        ),
        check_vma=False,
    )
```
